128 devices in a mesh: chain: 32 (over x_hi, y, z), group: 4 (over x_lo, core).
Axes of the slice: x: 4 (x_hi: 2, x_lo: 2; x = x_hi * 2 + x_lo), y: 4, z: 4, core: 2. Of those that a mesh axis runs over, the one named last changes fastest.
Arguments:
- site_tensors: bfloat16 [4, 32, 16, 256, 2, 256], P('group', 'chain')
- bond_weights: float32 [4, 32, 16, 256], P('group', 'chain'), may hold values from 0.5 to 1.5
- sector_sizes: int32 [4, 32, 16], P('group', 'chain'), may hold values from 192 to 256, as said below
- kept_ranks: int32 [4, 32, 16], P('group', 'chain'), may hold values from 128 to 256, as said below
- sketches: bfloat16 [16, 512, 256], replicated, may hold values from -6 to 6
- gate_ends: float32 [2], replicated, may hold values from 0.5 to 1.5
- gate_pair: float32 [3], replicated, may hold values from -0.4 to 0.4
Outputs:
- updated_sites: bfloat16 [4, 32, 16, 256, 2, 256], P('group', 'chain')
The draws below stay inside these ranges and needn't reach their ends.
Inputs may be any that keep to these rules, and one draw needn't show every extreme that they name: `sector_sizes`: every bond has one charge sector, the same for all bonds of a draw, of size 256. `kept_ranks`: A kept rank of sector q of bond n is at most the size of sector q of bonds n - 1, n and n + 1 (bonds outside the MPS count as 256); in the sector of size 256 it equals 256.
All inputs are finite; a program needn't handle non-finite values.
Results may differ from the reference program's by a relative error of at most 0.0088.
Values may be sent and summed in bfloat16 or wider, within the bound.
No kernel may reach another device: no remote copies, remote signals or barrier semaphores. Data moves between devices by JAX's collectives and lax.ppermute only.
A program may use at most 192 MiB of HBM per device.

```python
import math
import jax
import jax.numpy as jnp
from jax import lax

NQ = 16
B = 256
SEGMENTS = 4
CHAIN_DEV = 32


def sector_plan(key):
    seeded = jax.random.fold_in(key, 4099)
    site_count = SEGMENTS * CHAIN_DEV
    sector_dims = jax.random.randint(jax.random.fold_in(seeded, 1), (site_count, NQ), 3 * B // 4, B + 1)
    full_sector = jax.random.randint(jax.random.fold_in(seeded, 2), (), 0, NQ)
    column = lax.broadcasted_iota(jnp.int32, (site_count, NQ), 1)
    sector_dims = jnp.where(column == full_sector, B, sector_dims)
    boundary = jnp.full((1, NQ), B, jnp.int32)
    earlier = jnp.concatenate([boundary, sector_dims[:-1]], axis=0)
    later_dims = jnp.concatenate([sector_dims[1:], boundary], axis=0)
    picked = jax.random.randint(jax.random.fold_in(seeded, 3), (site_count, NQ), B // 2, B + 1)
    kept = jnp.minimum(jnp.minimum(picked, sector_dims), jnp.minimum(earlier, later_dims))
    kept = jnp.where(column == full_sector, B, kept)
    return (sector_dims.reshape(SEGMENTS, CHAIN_DEV, NQ), kept.reshape(SEGMENTS, CHAIN_DEV, NQ))


def draw_sector_sizes(key, part):
    return sector_plan(key)[0]


def draw_kept_ranks(key, part):
    return sector_plan(key)[1]


def draw_site_tensors(key, part):
    shape = (SEGMENTS, CHAIN_DEV, NQ, B, 2, B)
    noise = jax.random.normal(jax.random.fold_in(key, 11), shape, jnp.float32)
    noise = noise * (0.8 / B ** 0.5)
    diagonal = jax.random.uniform(jax.random.fold_in(key, 12), (SEGMENTS, CHAIN_DEV, NQ, 1, 2, B), jnp.float32, 1.0, 2.0)
    rows = lax.broadcasted_iota(jnp.int32, (1, 1, 1, B, 1, B), 3)
    cols = lax.broadcasted_iota(jnp.int32, (1, 1, 1, B, 1, B), 5)
    identity = (rows == cols).astype(jnp.float32)
    return (noise + diagonal * identity).astype(jnp.bfloat16)


def level_of(own_key, shape, cuts, least, high):
    level = 1.0
    for position, shards_of in cuts:
        steps = jax.random.uniform(jax.random.fold_in(jax.random.fold_in(own_key, 6), position), (shards_of,), jnp.float32, least / len(cuts), high / len(cuts))
        level = level * jnp.repeat(jnp.exp(steps), shape[position] // shards_of).reshape((-1,) + (1,) * (len(shape) - 1 - position))
    return level


def gaussian(key, extent, scale, reach, held_as=jnp.bfloat16):
    return jnp.clip(scale * jax.random.normal(key, extent, jnp.float32), -reach, reach).astype(held_as)


def setup_inputs(seed: int = 0) -> dict:
    keys = jax.random.split(jax.random.key(seed), 8)
    site_tensors = draw_site_tensors(jax.random.fold_in(keys[7], 71), 0)
    bond_weights = jnp.clip(jnp.exp(math.log(1.5) - 1.0986123 * jax.random.uniform(keys[1], (SEGMENTS, CHAIN_DEV, NQ, B), jnp.float32) ** level_of(keys[1], (SEGMENTS, CHAIN_DEV, NQ, B), ((0, 4), (1, 32)), -0.2, 0.2)), 0.5, 1.5)
    sector_sizes = draw_sector_sizes(jax.random.fold_in(keys[7], 71), 0)
    kept_ranks = draw_kept_ranks(jax.random.fold_in(keys[7], 71), 0)
    sketches = gaussian(keys[4], (NQ, 2 * B, B), 1.0, 6.0)
    gate_ends = jnp.clip(jnp.exp(jax.random.uniform(keys[5], (2,), jnp.float32, math.log(0.5), math.log(1.5))), 0.5, 1.5)
    gate_pair = jnp.clip(jax.random.uniform(keys[6], (3,), jnp.float32, -0.4, 0.4), -0.4, 0.4)
    return dict(site_tensors=site_tensors, bond_weights=bond_weights, sector_sizes=sector_sizes, kept_ranks=kept_ranks, sketches=sketches, gate_ends=gate_ends, gate_pair=gate_pair)


def shift_next(values):
    return jnp.concatenate([values[1:], jnp.zeros_like(values[:1])], axis=0)

def shift_prev(values):
    return jnp.concatenate([jnp.zeros_like(values[:1]), values[:-1]], axis=0)

def weigh_tensor(tensor, row_lam, col_lam):
    col_scale = jnp.stack([col_lam, shift_next(col_lam)], axis=1)
    scaled = tensor.astype(jnp.float32) * row_lam[:, :, None, None]
    return (scaled * col_scale[:, None, :, :]).astype(jnp.bfloat16)

def truncate_bond(two_site, kept_mask, sketch_win, gate_ends, gate_pair):
    middle = two_site[1:-1]
    block_zz = gate_ends[0] * middle[:, 0, :, 0, :]
    block_oo = gate_ends[1] * middle[:, 1, :, 1, :]
    block_zo = (1.0 + gate_pair[0]) * middle[:, 0, :, 1, :] + gate_pair[2] * two_site[2:, 1, :, 0, :]
    block_oz = gate_pair[2] * two_site[:-2, 0, :, 1, :] + (1.0 + gate_pair[1]) * middle[:, 1, :, 0, :]
    upper = jnp.concatenate([block_zz, block_zo], axis=-1)
    lower = jnp.concatenate([block_oz, block_oo], axis=-1)
    mixed = jnp.concatenate([upper, lower], axis=1).astype(jnp.bfloat16)
    block_size = kept_mask.shape[1]
    sketch_cols = sketch_win * kept_mask[:, None, :]
    sampled = jnp.einsum('mij,mjk->mik', mixed.astype(jnp.float32), sketch_cols.astype(jnp.float32), precision=lax.Precision.HIGHEST)
    gram_matrix = jnp.einsum('mik,mil->mkl', sampled, sampled, precision=lax.Precision.HIGHEST)
    shift_amount = 0.01 * lax.optimization_barrier(jnp.sum(sampled * sampled, axis=(1, 2))) / block_size
    diag_add = 1.0 - kept_mask.astype(jnp.float32) + shift_amount[:, None]
    gram_matrix = gram_matrix + diag_add[:, :, None] * jnp.eye(block_size, dtype=jnp.float32)[None]
    lower_factor = jnp.linalg.cholesky(gram_matrix)
    factor_t = jax.scipy.linalg.solve_triangular(lower_factor, jnp.swapaxes(sampled, 1, 2), lower=True)
    scaled = (factor_t * math.sqrt(block_size)).astype(jnp.bfloat16)
    right_part = jnp.einsum('mki,mij->mkj', scaled.astype(jnp.float32), mixed.astype(jnp.float32), precision=lax.Precision.HIGHEST)
    right_part = (right_part / block_size).astype(jnp.bfloat16)
    return (scaled, right_part)

def left_from_factor(scaled):
    block_size = scaled.shape[1]
    columns = jnp.swapaxes(scaled, 1, 2)
    upper = columns[:, :block_size, :]
    lower = shift_next(columns[:, block_size:, :])
    return jnp.stack([upper, lower], axis=2)

def reference(site_tensors, bond_weights, sector_sizes, kept_ranks, sketches, gate_ends, gate_pair):
    site_count = SEGMENTS * CHAIN_DEV
    pair_count = site_count // 2
    column = lax.broadcasted_iota(jnp.int32, (NQ, B), 1)
    sites = site_tensors.reshape(site_count, NQ, B, 2, B)
    lam = bond_weights.reshape(site_count, NQ, B) * (column[None] < sector_sizes.reshape(site_count, NQ)[:, :, None]).astype(jnp.float32)
    kept_mask = (column[None] < kept_ranks.reshape(site_count, NQ)[:, :, None]).astype(jnp.bfloat16)
    lam_left = jnp.concatenate([jnp.ones((1, NQ, B), jnp.float32), lam[:-1]], axis=0)

    def one_pair(pair_inputs):
        pair_sites, pair_lam, left_lam, pair_kept = pair_inputs
        left_w = weigh_tensor(pair_sites[0], left_lam[0], jnp.ones((NQ, B), jnp.float32))
        right_w = weigh_tensor(pair_sites[1], left_lam[1], pair_lam[1])
        left_block = jnp.concatenate([left_w[:, :, 0, :], shift_prev(left_w[:, :, 1, :])], axis=1)
        right_block = right_w.reshape(NQ, B, 2 * B)
        two_site = jnp.einsum('mik,mkj->mij', left_block.astype(jnp.float32), right_block.astype(jnp.float32), precision=lax.Precision.HIGHEST)
        two_site = two_site.reshape(NQ, 2, B, 2, B)
        zero_sector = jnp.zeros((1, 2, B, 2, B), jnp.float32)
        two_site = jnp.concatenate([zero_sector, two_site, zero_sector], axis=0)
        scaled, right_part = truncate_bond(two_site, pair_kept[0], sketches, gate_ends, gate_pair)
        return jnp.stack([left_from_factor(scaled), right_part.reshape(NQ, B, 2, B)], axis=0)
    updated = lax.map(one_pair, (sites.reshape(pair_count, 2, NQ, B, 2, B), lam.reshape(pair_count, 2, NQ, B), lam_left.reshape(pair_count, 2, NQ, B), kept_mask.reshape(pair_count, 2, NQ, B)))
    return updated.reshape(SEGMENTS, CHAIN_DEV, NQ, B, 2, B)
```

```python
import functools

import jax
import jax.numpy as jnp
from jax import lax
from jax.experimental import pallas as pl
from jax.experimental.pallas import tpu as pltpu
from jax.sharding import PartitionSpec as P

f32 = jnp.float32
bf16 = jnp.bfloat16


BATCH = 4
LEAF = 32
PANELS = 8
LANES = 128
SIZE = 256


def split(x):
    high = x.astype(bf16)
    return high, (x - high.astype(f32)).astype(bf16)


def invert_leaf(d):
    lane = lax.broadcasted_iota(jnp.int32, (8, LANES), 1)
    sub = lax.broadcasted_iota(jnp.int32, (8, LANES), 0)
    segment = (lane // LEAF) * LEAF
    tiles = LEAF // 8
    rows = [d[8 * t : 8 * t + 8, :] for t in range(tiles)]
    cols = [
        [
            jnp.take_along_axis(rows[t], segment + j, axis=1) if t >= j // 8 else None
            for t in range(tiles)
        ]
        for j in range(LEAF)
    ]
    inverse = [((lane - segment) == (sub + 8 * t)).astype(f32) for t in range(tiles)]
    pivots = [jnp.ones((8, LANES), f32) for _ in range(tiles)]

    def row(v, r):
        return jnp.broadcast_to(v[r : r + 1, :], (8, LANES))

    for j in range(LEAF):
        top, r = j // 8, j % 8
        pivot = row(cols[j][top], r)
        reciprocal = 1.0 / pivot
        pivots[top] = jnp.where(sub == r, pivot, pivots[top])
        scaled = {t: cols[j][t] * reciprocal for t in range(top, tiles)}
        for i in range(j + 1, LEAF):
            factor = row(scaled[i // 8], i % 8)
            for t in range(i // 8, tiles):
                cols[i][t] = cols[i][t] - factor * cols[j][t]
        source = row(inverse[top], r)
        for t in range(top, tiles):
            factor = jnp.where(sub > r, scaled[t], 0.0) if t == top else scaled[t]
            inverse[t] = inverse[t] - factor * source
    return jnp.concatenate([inverse[t] * lax.rsqrt(pivots[t]) for t in range(tiles)], axis=0)


def times_blocks(x_split, y):
    r = lax.broadcasted_iota(jnp.int32, (LANES, LANES), 0) // LEAF
    c = lax.broadcasted_iota(jnp.int32, (LANES, LANES), 1) // LEAF
    blocks = jnp.where(r == c, jnp.concatenate([y] * BATCH, axis=0), 0.0)
    high, low = split(blocks)
    weights = jnp.concatenate(
        [
            jnp.concatenate([high, high], axis=1),
            jnp.concatenate([low, jnp.zeros_like(low)], axis=1),
        ],
        axis=0,
    )
    out = lax.dot_general(
        x_split, weights, (((1,), (1,)), ((), ())), preferred_element_type=f32
    )
    return out[:, :LANES] + out[:, LANES:]


def invert_factor(x_ref):
    lane = lax.broadcasted_iota(jnp.int32, (LEAF, LANES), 1)
    sub = lax.broadcasted_iota(jnp.int32, (LEAF, LANES), 0)
    eye = ((lane % LEAF) == sub).astype(f32)

    def step(j, carry):
        first = pl.multiple_of(j * LEAF, LEAF)
        inverse = invert_leaf(x_ref[j, pl.ds(first, LEAF), :])
        for k in range(PANELS):
            x_ref[k, pl.ds(first, LEAF), :] = jnp.zeros((LEAF, LANES), f32)
        x_ref[j, pl.ds(first, LEAF), :] = eye
        panel = times_blocks(jnp.concatenate(split(x_ref[j]), axis=1), inverse)
        x_ref[j] = panel
        panel_split = jnp.concatenate(split(panel), axis=1)
        for k in range(1, PANELS):
            y = x_ref[j, pl.ds(k * LEAF, LEAF), :] * (k > j).astype(f32)
            x_ref[k] = x_ref[k] - times_blocks(panel_split, y)
        return carry

    lax.fori_loop(0, PANELS, step, 0)


def compute_kernel(second, *refs):
    if second:
        (role, gates, kept, own, got, got_b, half, scale, sketch, carry) = refs[:10]
        refs = refs[10:]
        (msg, mine, merge), refs = refs[:3], refs[3:]
    else:
        (role, gates, kept, own, got, scale, sketch) = refs[:7]
        refs = refs[7:]
        (msg, mine, carry_out), refs = refs[:3], refs[3:]
    left_w, right_w, mixed, samp, gram, x_ref, scaled_ref, wide_t, wide_p = refs
    is_right = role[0] == 1
    first = role[1]
    g0, g1, p0, p1, p2 = [gates[i] for i in range(5)]

    def received(t):
        if not second:
            return got.at[t] if t < 5 else got.at[0]
        return [None, got_b.at[0], got_b.at[1], got_b.at[2], got.at[0], got.at[1]][t]

    def row_scale(which, q):
        line = scale[which, q + 1]
        return jnp.transpose(jnp.broadcast_to(line, (LANES, SIZE)))

    for t in range(6):
        q = first - 1 + t
        mine_at = jnp.clip(q, 0, 15)
        for left in (True, False):
            if left and t == 5:
                continue
            own_here = jnp.logical_not(is_right) if left else is_right
            halved = second and t == 0

            @pl.when(own_here)
            def _():
                wide_t[...] = own[mine_at].astype(f32)

            if halved:

                @pl.when(jnp.logical_not(own_here))
                def _():
                    for jb in range(2):
                        wide_t[pl.ds(2 * jb, SIZE, stride=4), :] = jnp.zeros((SIZE, LANES), f32)
                        wide_t[pl.ds(2 * jb + 1, SIZE, stride=4), :] = half[
                            :, jb * LANES : (jb + 1) * LANES
                        ].astype(f32)

            else:

                @pl.when(jnp.logical_not(own_here))
                def _():
                    wide_t[...] = received(t)[...].astype(f32)

            rows = row_scale(0 if left else 1, q)
            for s in range(2):
                if not left and ((t == 0 and s == 0) or (t == 5 and s == 1)):
                    continue
                for jb in range(2):
                    value = wide_t[pl.ds(2 * jb + s, SIZE, stride=4), :] * rows
                    lanes = slice(jb * LANES, (jb + 1) * LANES)
                    if left:
                        left_w[t, s, :, lanes] = value.astype(bf16)
                    else:
                        col = scale[2, q + s + 1][:, lanes]
                        right_w[t, s, :, lanes] = (value * col).astype(bf16)

    def dot(a, b):
        return jnp.dot(a, b, preferred_element_type=f32)

    lane256 = lax.broadcasted_iota(jnp.int32, (1, SIZE), 1)
    eye = lax.broadcasted_iota(jnp.int32, (SIZE, SIZE), 0) == lax.broadcasted_iota(
        jnp.int32, (SIZE, SIZE), 1
    )
    half_rows = (slice(0, SIZE), slice(SIZE, 2 * SIZE))

    for b in range(BATCH):
        t = b + 1
        m = first + b
        mixed[b, half_rows[0], half_rows[0]] = (g0 * dot(left_w[t, 0], right_w[t, 0])).astype(bf16)
        mixed[b, half_rows[0], half_rows[1]] = (
            p0 * dot(left_w[t, 0], right_w[t, 1]) + p2 * dot(left_w[t, 1], right_w[t + 1, 0])
        ).astype(bf16)
        mixed[b, half_rows[1], half_rows[0]] = (
            p2 * dot(left_w[t - 1, 0], right_w[t - 1, 1]) + p1 * dot(left_w[t - 1, 1], right_w[t, 0])
        ).astype(bf16)
        mixed[b, half_rows[1], half_rows[1]] = (
            g1 * dot(left_w[t - 1, 1], right_w[t, 1])
        ).astype(bf16)
        keep = lane256 < kept[m]
        sampled = jnp.where(keep, dot(mixed[b], sketch[m]), 0.0)
        high, low = split(sampled)
        samp[b, 0] = high
        samp[b, 1] = low
        shift = 0.01 * jnp.sum(sampled * sampled) / SIZE
        contract = (((0,), (0,)), ((), ()))
        high = samp[b, 0]
        low = samp[b, 1]
        hh = lax.dot_general(high, high, contract, preferred_element_type=f32)
        hl = lax.dot_general(high, low, contract, preferred_element_type=f32)
        added = jnp.where(keep, 0.0, 1.0) + shift
        gram[b] = (hh + (hl + jnp.transpose(hl))) + jnp.where(eye, added, 0.0)

    segment = lax.broadcasted_iota(jnp.int32, (1, LANES), 1) // LEAF

    def gather_lanes(pieces):
        out = pieces[0]
        for i in range(1, BATCH):
            out = jnp.where(segment == i, pieces[i], out)
        return out

    def rolled(value, segments):
        shift = (segments * LEAF) % LANES
        return pltpu.roll(value, shift, axis=1) if shift else value

    for k in range(PANELS):
        rows = slice(k * LEAF, SIZE)
        lanes = slice((k // 4) * LANES, (k // 4 + 1) * LANES)
        x_ref[k, rows, :] = gather_lanes(
            [rolled(gram[b, rows, lanes], b - k % 4) for b in range(BATCH)]
        )
        if k:
            x_ref[k, : k * LEAF, :] = jnp.zeros((k * LEAF, LANES), f32)

    invert_factor(x_ref)

    for b in range(BATCH):
        factor = jnp.concatenate(
            [
                gather_lanes([rolled(x_ref[4 * g + i], i - b) for i in range(BATCH)])
                for g in range(2)
            ],
            axis=1,
        )
        high, low = split(factor)
        solved = dot(samp[b, 0], high) + (dot(samp[b, 0], low) + dot(samp[b, 1], high))
        scaled_ref[b] = (solved * 16.0).astype(bf16)

    if not second:
        carry_out[...] = scaled_ref[0, half_rows[1], :]

    for b in range(BATCH):
        right_part = lax.dot_general(
            scaled_ref[b], mixed[b], (((0,), (0,)), ((), ())), preferred_element_type=f32
        ) * (1.0 / SIZE)
        for s in range(2):
            if s == 0:
                half_t = scaled_ref[b, half_rows[0], :]
            elif b + 1 < BATCH:
                half_t = scaled_ref[b + 1, half_rows[1], :]
            elif second:
                half_t = carry[...]
            else:
                half_t = jnp.zeros((SIZE, SIZE), bf16)
            for jb in range(2):
                rows = pl.ds(2 * jb + s, SIZE, stride=4)
                wide_t[rows, :] = half_t[:, jb * LANES : (jb + 1) * LANES].astype(f32)
                start = s * SIZE + jb * LANES
                wide_p[rows, :] = right_part[:, start : start + LANES]

        @pl.when(is_right)
        def _():
            msg[b] = wide_t[...].astype(bf16)
            mine[b] = wide_p[...].astype(bf16)

        @pl.when(jnp.logical_not(is_right))
        def _():
            msg[b] = wide_p[...].astype(bf16)
            mine[b] = wide_t[...].astype(bf16)

    if second:
        used = jnp.where(is_right, 0.0, 1.0)
        for jb in range(2):
            lower = scaled_ref[0, half_rows[1], jb * LANES : (jb + 1) * LANES].astype(f32)
            wide_t[pl.ds(2 * jb, SIZE, stride=4), :] = jnp.zeros((SIZE, LANES), f32)
            wide_t[pl.ds(2 * jb + 1, SIZE, stride=4), :] = lower * used
        merge[...] = wide_t[...].astype(bf16)


def compute(second, role, gates, kept, own, got, scale, sketch, got_b=None, half=None, carry=None):
    smem = pl.BlockSpec(memory_space=pltpu.SMEM)
    vmem = pl.BlockSpec(memory_space=pltpu.VMEM)
    if second:
        operands = (role, gates, kept, own, got, got_b, half, scale, sketch, carry)
        third = jax.ShapeDtypeStruct((4 * SIZE, LANES), bf16)
    else:
        operands = (role, gates, kept, own, got, scale, sketch)
        third = jax.ShapeDtypeStruct((SIZE, SIZE), bf16)
    part = jax.ShapeDtypeStruct((BATCH, 4 * SIZE, LANES), bf16)
    return pl.pallas_call(
        functools.partial(compute_kernel, second),
        out_shape=(part, part, third),
        in_specs=[smem] * 3 + [vmem] * (len(operands) - 3),
        out_specs=(vmem, vmem, vmem),
        scratch_shapes=[
            pltpu.VMEM((5, 2, SIZE, SIZE), bf16),
            pltpu.VMEM((6, 2, SIZE, SIZE), bf16),
            pltpu.VMEM((BATCH, 2 * SIZE, 2 * SIZE), bf16),
            pltpu.VMEM((BATCH, 2, 2 * SIZE, SIZE), bf16),
            pltpu.VMEM((BATCH, SIZE, SIZE), f32),
            pltpu.VMEM((PANELS, SIZE, LANES), f32),
            pltpu.VMEM((BATCH, 2 * SIZE, SIZE), bf16),
            pltpu.VMEM((4 * SIZE, LANES), f32),
            pltpu.VMEM((4 * SIZE, LANES), f32),
        ],
        compiler_params=pltpu.CompilerParams(vmem_limit_bytes=40 * 2**20),
        cost_estimate=pl.CostEstimate(
            flops=20_000_000_000, bytes_accessed=8_000_000, transcendentals=0
        ),
        name="second_half" if second else "first_half",
    )(*operands)


def to_lines(x):
    n = x.shape[0]
    return x.reshape(n, SIZE, 2, 2, LANES).transpose(0, 1, 3, 2, 4).reshape(n, 4 * SIZE, LANES)


def from_lines(x):
    n = x.shape[0]
    return x.reshape(n, SIZE, 2, 2, LANES).transpose(0, 1, 3, 2, 4).reshape(n, SIZE, 2, SIZE)


def shards(site_tensors, bond_weights, sector_sizes, kept_ranks, sketches, gate_ends, gate_pair):
    chain = lax.axis_size("chain")
    count = lax.axis_size("group") * chain
    site = lax.axis_index("group") * chain + lax.axis_index("chain")
    is_right = site % 2 == 1

    def swapped(value):
        return lax.ppermute(value, "chain", [(i, i ^ 1) for i in range(chain)])

    def onward(value, by):
        def place(n):
            return n % chain * (count // chain) + n // chain

        pairs = [(place(i), place(i + by)) for i in range(1, count, 2) if i + by < count]
        return lax.ppermute(value, ("chain", "group"), pairs)

    own = to_lines(site_tensors[0, 0])
    sectors = own.shape[0]
    got_a = swapped(lax.dynamic_slice_in_dim(own, jnp.where(is_right, 11, 3), 5, 0))

    column = lax.broadcasted_iota(jnp.int32, (sectors, SIZE), 1)
    lam = bond_weights[0, 0] * (column < sector_sizes[0, 0][:, None]).astype(f32)
    kept_line = jnp.pad(kept_ranks[0, 0].astype(f32)[None, :], ((0, 7), (0, SIZE - sectors)))
    packed = jnp.concatenate([lam, kept_line], axis=0)
    other = swapped(packed)
    before_left = onward(lam, 1)
    before_right = onward(lam, 2)

    got_b = swapped(lax.dynamic_slice_in_dim(own, jnp.where(is_right, 8, 0), 3, 0))
    half = lax.ppermute(
        site_tensors[0, 0, 7, :, 1, :], "chain", [(i, i - 1) for i in range(1, chain, 2)]
    )

    lam_prev = jnp.where(is_right, before_right, before_left)
    lam_prev = jnp.where(site < 2, jnp.ones_like(lam), lam_prev)
    lam_mid = jnp.where(is_right, other[:sectors], lam)
    lam_next = jnp.where(is_right, lam, other[:sectors])
    scale = jnp.pad(jnp.stack([lam_prev, lam_mid, lam_next]), ((0, 0), (1, 7), (0, 0)))
    scale = scale[:, :, None, :]
    kept = jnp.where(is_right, other[sectors, :sectors], kept_line[0, :sectors]).astype(jnp.int32)
    gates = jnp.concatenate([gate_ends, 1.0 + gate_pair[:2], gate_pair[2:]])
    flag = is_right.astype(jnp.int32)
    role_a = jnp.stack([flag, 12 - 8 * flag])
    role_b = jnp.stack([flag, 8 - 8 * flag])

    msg_a, mine_a, carry = compute(False, role_a, gates, kept, own, got_a, scale, sketches)
    back_a = swapped(from_lines(msg_a))
    msg_b, mine_b, merge = compute(
        True, role_b, gates, kept, own, got_a, scale, sketches, got_b, half, carry
    )
    back_b = swapped(from_lines(msg_b))

    mine_at = 8 - 8 * flag
    back_at = 8 * flag
    out = jnp.zeros((sectors, SIZE, 2, SIZE), bf16)
    out = lax.dynamic_update_slice_in_dim(out, from_lines(mine_a), mine_at + 4, 0)
    out = lax.dynamic_update_slice_in_dim(out, from_lines(mine_b), mine_at, 0)
    out = lax.dynamic_update_slice_in_dim(out, back_a, back_at + 4, 0)
    out = lax.dynamic_update_slice_in_dim(out, back_a[3:] + from_lines(merge[None]), back_at + 7, 0)
    out = lax.dynamic_update_slice_in_dim(out, back_b, back_at, 0)
    return out[None, None]


def solution(mesh):
    return jax.shard_map(
        shards,
        mesh=mesh,
        in_specs=(
            P("group", "chain", None, None, None, None),
            P("group", "chain", None, None),
            P("group", "chain", None),
            P("group", "chain", None),
            P(),
            P(),
            P(),
        ),
        out_specs=P("group", "chain", None, None, None, None),
        check_vma=False,
    )
```

```python
import functools

import jax
import jax.numpy as jnp
from jax import lax
from jax.experimental import pallas as pl
from jax.experimental.pallas import tpu as pltpu
from jax.sharding import PartitionSpec as P

f32 = jnp.float32
bf16 = jnp.bfloat16


BATCH = 4
LEAF = 32
PANELS = 8
LANES = 128
SIZE = 256


def split(x):
    high = x.astype(bf16)
    return high, (x - high.astype(f32)).astype(bf16)


def invert_leaf(d):
    lane = lax.broadcasted_iota(jnp.int32, (8, LANES), 1)
    sub = lax.broadcasted_iota(jnp.int32, (8, LANES), 0)
    segment = (lane // LEAF) * LEAF
    tiles = LEAF // 8
    rows = [d[8 * t : 8 * t + 8, :] for t in range(tiles)]
    cols = [
        [
            jnp.take_along_axis(rows[t], segment + j, axis=1) if t >= j // 8 else None
            for t in range(tiles)
        ]
        for j in range(LEAF)
    ]
    inverse = [((lane - segment) == (sub + 8 * t)).astype(f32) for t in range(tiles)]
    pivots = [jnp.ones((8, LANES), f32) for _ in range(tiles)]

    def row(v, r):
        return jnp.broadcast_to(v[r : r + 1, :], (8, LANES))

    for j in range(LEAF):
        top, r = j // 8, j % 8
        pivot = row(cols[j][top], r)
        reciprocal = 1.0 / pivot
        pivots[top] = jnp.where(sub == r, pivot, pivots[top])
        scaled = {t: cols[j][t] * reciprocal for t in range(top, tiles)}
        for i in range(j + 1, LEAF):
            factor = row(scaled[i // 8], i % 8)
            for t in range(i // 8, tiles):
                cols[i][t] = cols[i][t] - factor * cols[j][t]
        source = row(inverse[top], r)
        for t in range(top, tiles):
            factor = jnp.where(sub > r, scaled[t], 0.0) if t == top else scaled[t]
            inverse[t] = inverse[t] - factor * source
    return jnp.concatenate([inverse[t] * lax.rsqrt(pivots[t]) for t in range(tiles)], axis=0)


def block_weights(high, low, masks):
    high = jnp.concatenate([high * mask for mask in masks], axis=0)
    low = jnp.concatenate([low * mask for mask in masks], axis=0)
    upper = jnp.concatenate([high, high], axis=1)
    lower = jnp.concatenate([low, jnp.zeros_like(low)], axis=1)
    return jnp.concatenate([upper, lower], axis=0)


def times_transposed(x, weights):
    out = lax.dot_general(x, weights, (((1,), (1,)), ((), ())), preferred_element_type=f32)
    return out[:, :LANES] + out[:, LANES:]


def invert_factor(a_ref, x_ref):
    lane = lax.broadcasted_iota(jnp.int32, (LEAF, LANES), 1)
    sub = lax.broadcasted_iota(jnp.int32, (LEAF, LANES), 0)
    eye = ((lane % LEAF) == sub).astype(f32)
    masks = [((lane // LEAF) == b).astype(f32).astype(bf16) for b in range(BATCH)]
    for j in range(PANELS):
        start = j * LEAF
        block = slice(start, start + LEAF)
        col = a_ref[j]
        if j:
            weights = [
                block_weights(
                    x_ref[block, k * SIZE : k * SIZE + LANES],
                    x_ref[block, k * SIZE + LANES : (k + 1) * SIZE],
                    masks,
                )
                for k in range(j)
            ]
            col = col - times_transposed(x_ref[:, : j * SIZE], jnp.concatenate(weights, axis=1))
            x_ref[block, : j * SIZE] = jnp.zeros((LEAF, j * SIZE), bf16)
        inverse = invert_leaf(col[block])
        col = jnp.concatenate(
            [part for part in (col[:start], eye, col[start + LEAF :]) if part.shape[0]], axis=0
        )
        col = times_transposed(
            jnp.concatenate(split(col), axis=1), block_weights(*split(inverse), masks)
        )
        x_ref[:, j * SIZE : (j + 1) * SIZE] = jnp.concatenate(split(col), axis=1)


def compute_kernel(second, *refs):
    if second:
        (role, gates, kept, own, got, got_b, half, scale, sketches, carry) = refs[:10]
        (msg, out, merge), refs = refs[11:14], refs[14:]
    else:
        (role, gates, kept, own, got, scale, sketches) = refs[:7]
        (msg, out, carry_out), refs = refs[7:10], refs[10:]
    left_w, right_w, mixed, samp, gram, a_ref, x_ref, scaled_ref, wide_t, wide_p = refs[:10]
    own_win, got_win, sketch, mine, own_sem, got_sem, sketch_sem, mine_sem = refs[10:]
    is_right = role[0] == 1
    first = role[1]
    g0, g1, p0, p1, p2 = [gates[i] for i in range(5)]

    def own_copy(t):
        at = jnp.clip(first - 1 + t, 0, 15)
        return pltpu.make_async_copy(own.at[at], own_win.at[t], own_sem.at[t])

    def got_copy(t, source):
        return pltpu.make_async_copy(source, got_win.at[t], got_sem.at[t])

    if second:
        sources = [None, got_b.at[0], got_b.at[1], got_b.at[2], got.at[0], got.at[1]]
    else:
        sources = [got.at[t] for t in range(5)] + [got.at[0]]
    sketch_copy = pltpu.make_async_copy(sketches.at[pl.ds(first, BATCH)], sketch, sketch_sem)
    for t in range(6):
        own_copy(t).start()
        if sources[t] is not None:
            got_copy(t, sources[t]).start()
    sketch_copy.start()
    if second:
        for jb in range(2):
            wide_t[pl.ds(2 * jb, SIZE, stride=4), :] = jnp.zeros((SIZE, LANES), f32)
            wide_t[pl.ds(2 * jb + 1, SIZE, stride=4), :] = half[
                :, jb * LANES : (jb + 1) * LANES
            ].astype(f32)
        got_win[0] = wide_t[...].astype(bf16)

    def row_scale(which, q):
        line = scale[which, q + 1]
        return jnp.transpose(jnp.broadcast_to(line, (LANES, SIZE)))

    def weigh(t, loop):
        q = first - 1 + t
        own_copy(t).wait()

        @pl.when(t >= (1 if second else 0))
        def _():
            got_copy(t, got.at[0]).wait()

        own_wide = own_win[t].astype(f32)
        got_wide = got_win[t].astype(f32)
        wide_t[...] = jnp.where(is_right, got_wide, own_wide)
        wide_p[...] = jnp.where(is_right, own_wide, got_wide)
        left_rows = row_scale(0, q)
        right_rows = row_scale(1, q)
        for s in range(2):
            col = scale[2, q + s + 1]
            for jb in range(2):
                lines = pl.ds(2 * jb + s, SIZE, stride=4)
                lanes = slice(jb * LANES, (jb + 1) * LANES)
                left_w[t, s, :, lanes] = (wide_t[lines, :] * left_rows).astype(bf16)
                value = (wide_p[lines, :] * right_rows) * col[:, lanes]
                right_w[t, s, :, lanes] = value.astype(bf16)
        return loop

    lax.fori_loop(0, 6, weigh, 0)

    def dot(a, b):
        return jnp.dot(a, b, preferred_element_type=f32)

    lane256 = lax.broadcasted_iota(jnp.int32, (1, SIZE), 1)
    eye = lax.broadcasted_iota(jnp.int32, (SIZE, SIZE), 0) == lax.broadcasted_iota(
        jnp.int32, (SIZE, SIZE), 1
    )
    upper, lower = slice(0, SIZE), slice(SIZE, 2 * SIZE)
    contract_rows = (((0,), (0,)), ((), ()))
    sketch_copy.wait()

    def sample(b, loop):
        t = b + 1
        left = [left_w[t, 0], left_w[t, 1], left_w[b, 0], left_w[b, 1]]
        right = [right_w[t, 0], right_w[t, 1]]
        mixed[b, upper, upper] = (g0 * dot(left[0], right[0])).astype(bf16)
        mixed[b, upper, lower] = (
            p0 * dot(left[0], right[1]) + p2 * dot(left[1], right_w[t + 1, 0])
        ).astype(bf16)
        mixed[b, lower, upper] = (
            p2 * dot(left[2], right_w[b, 1]) + p1 * dot(left[3], right[0])
        ).astype(bf16)
        mixed[b, lower, lower] = (g1 * dot(left[3], right[1])).astype(bf16)
        keep = lane256 < kept[first + b]
        sampled = jnp.where(keep, dot(mixed[b], sketch[b]), 0.0)
        high, low = split(sampled)
        samp[b, 0] = high
        samp[b, 1] = low
        shift = 0.01 * jnp.sum(sampled * sampled) / SIZE
        hh = lax.dot_general(high, high, contract_rows, preferred_element_type=f32)
        hl = lax.dot_general(high, low, contract_rows, preferred_element_type=f32)
        added = jnp.where(keep, 0.0, 1.0) + shift
        gram[b] = (hh + (hl + jnp.transpose(hl))) + jnp.where(eye, added, 0.0)
        return loop

    lax.fori_loop(0, BATCH, sample, 0)

    segment = lax.broadcasted_iota(jnp.int32, (1, LANES), 1) // LEAF

    def gather_lanes(pieces):
        out = pieces[0]
        for i in range(1, BATCH):
            out = jnp.where(segment == i, pieces[i], out)
        return out

    def rolled(value, segments):
        shift = (segments * LEAF) % LANES
        return pltpu.roll(value, shift, axis=1) if shift else value

    for k in range(PANELS):
        rows = slice(k * LEAF, SIZE)
        lanes = slice((k // 4) * LANES, (k // 4 + 1) * LANES)
        a_ref[k, rows, :] = gather_lanes(
            [rolled(gram[b, rows, lanes], b - k % 4) for b in range(BATCH)]
        )
        if k:
            a_ref[k, : k * LEAF, :] = jnp.zeros((k * LEAF, LANES), f32)

    invert_factor(a_ref, x_ref)

    for b in range(BATCH):
        high, low = [
            jnp.concatenate(
                [
                    gather_lanes(
                        [
                            rolled(
                                x_ref[:, k * SIZE + offset : k * SIZE + offset + LANES].astype(f32),
                                k % 4 - b,
                            )
                            for k in range(4 * g, 4 * g + 4)
                        ]
                    )
                    for g in range(2)
                ],
                axis=1,
            ).astype(bf16)
            for offset in (0, LANES)
        ]
        solved = dot(samp[b, 0], high) + (dot(samp[b, 0], low) + dot(samp[b, 1], high))
        scaled_ref[b] = (solved * 16.0).astype(bf16)

    if second:
        scaled_ref[BATCH, lower, :] = carry[...]
    else:
        scaled_ref[BATCH, lower, :] = jnp.zeros((SIZE, SIZE), bf16)
        carry_out[...] = scaled_ref[0, lower, :]

    def deliver(b, loop):
        right_part = lax.dot_general(
            scaled_ref[b], mixed[b], contract_rows, preferred_element_type=f32
        ) * (1.0 / SIZE)
        for s in range(2):
            left_half = scaled_ref[b, upper, :] if s == 0 else scaled_ref[b + 1, lower, :]
            for jb in range(2):
                lines = pl.ds(2 * jb + s, SIZE, stride=4)
                wide_t[lines, :] = left_half[:, jb * LANES : (jb + 1) * LANES].astype(f32)
                start = s * SIZE + jb * LANES
                wide_p[lines, :] = right_part[:, start : start + LANES]
        left_site = wide_t[...]
        right_site = wide_p[...]
        msg[b] = jnp.where(is_right, left_site, right_site).astype(bf16)
        mine[b] = jnp.where(is_right, right_site, left_site).astype(bf16)
        mine_copy(b).start()
        return loop

    def mine_copy(b):
        at = first + b
        return pltpu.make_async_copy(mine.at[b], out.at[at], mine_sem.at[b])

    lax.fori_loop(0, BATCH, deliver, 0)

    if second:
        used = jnp.where(is_right, 0.0, 1.0)
        for jb in range(2):
            value = scaled_ref[0, lower, jb * LANES : (jb + 1) * LANES].astype(f32)
            wide_t[pl.ds(2 * jb, SIZE, stride=4), :] = jnp.zeros((SIZE, LANES), f32)
            wide_t[pl.ds(2 * jb + 1, SIZE, stride=4), :] = value * used
        merge[...] = wide_t[...].astype(bf16)
    for b in range(BATCH):
        mine_copy(b).wait()


def in_hbm(x):
    return pltpu.with_memory_space_constraint(x, pltpu.HBM)


def compute(second, role, gates, kept, own, got, scale, sketch, got_b=None, half=None, carry=None, out=None):
    smem = pl.BlockSpec(memory_space=pltpu.SMEM)
    vmem = pl.BlockSpec(memory_space=pltpu.VMEM)
    hbm = pl.BlockSpec(memory_space=pltpu.HBM)
    own, got, sketch = in_hbm(own), in_hbm(got), in_hbm(sketch)
    if second:
        operands = (role, gates, kept, own, got, in_hbm(got_b), half, scale, sketch, carry, out)
        specs = [smem] * 3 + [hbm] * 3 + [vmem, vmem, hbm, vmem, hbm]
        third = jax.ShapeDtypeStruct((4 * SIZE, LANES), bf16)
    else:
        operands = (role, gates, kept, own, got, scale, sketch)
        specs = [smem] * 3 + [hbm] * 2 + [vmem, hbm]
        third = jax.ShapeDtypeStruct((SIZE, SIZE), bf16)
    part = jax.ShapeDtypeStruct((BATCH, 4 * SIZE, LANES), bf16)
    whole = jax.ShapeDtypeStruct(own.shape, bf16)
    return pl.pallas_call(
        functools.partial(compute_kernel, second),
        out_shape=(part, whole, third),
        in_specs=specs,
        out_specs=(vmem, hbm, vmem),
        scratch_shapes=[
            pltpu.VMEM((6, 2, SIZE, SIZE), bf16),
            pltpu.VMEM((6, 2, SIZE, SIZE), bf16),
            pltpu.VMEM((BATCH, 2 * SIZE, 2 * SIZE), bf16),
            pltpu.VMEM((BATCH, 2, 2 * SIZE, SIZE), bf16),
            pltpu.VMEM((BATCH, SIZE, SIZE), f32),
            pltpu.VMEM((PANELS, SIZE, LANES), f32),
            pltpu.VMEM((SIZE, PANELS * SIZE), bf16),
            pltpu.VMEM((BATCH + 1, 2 * SIZE, SIZE), bf16),
            pltpu.VMEM((4 * SIZE, LANES), f32),
            pltpu.VMEM((4 * SIZE, LANES), f32),
            pltpu.VMEM((6, 4 * SIZE, LANES), bf16),
            pltpu.VMEM((6, 4 * SIZE, LANES), bf16),
            pltpu.VMEM((BATCH, 2 * SIZE, SIZE), bf16),
            pltpu.VMEM((BATCH, 4 * SIZE, LANES), bf16),
            pltpu.SemaphoreType.DMA((6,)),
            pltpu.SemaphoreType.DMA((6,)),
            pltpu.SemaphoreType.DMA,
            pltpu.SemaphoreType.DMA((BATCH,)),
        ],
        input_output_aliases={10: 1} if second else {},
        compiler_params=pltpu.CompilerParams(vmem_limit_bytes=40 * 2**20),
        cost_estimate=pl.CostEstimate(
            flops=20_000_000_000, bytes_accessed=8_000_000, transcendentals=0
        ),
        name="second_half" if second else "first_half",
    )(*operands)


def place_kernel(merged, at, block, *refs):
    if merged:
        merge, _, out, last, sems = refs
    else:
        _, out, sems = refs
    count = block.shape[0]
    copies = []
    for b in range(count):
        source = block.at[b]
        if merged and b == count - 1:
            last[...] = block[b] + merge[...]
            source = last
        copies.append(pltpu.make_async_copy(source, out.at[at[0] + b], sems.at[b]))
        copies[-1].start()
    for copy in copies:
        copy.wait()


def place(out, block, at, merge=None):
    smem = pl.BlockSpec(memory_space=pltpu.SMEM)
    vmem = pl.BlockSpec(memory_space=pltpu.VMEM)
    hbm = pl.BlockSpec(memory_space=pltpu.HBM)
    operands = (jnp.reshape(at, (1,)), block) + (() if merge is None else (merge,)) + (out,)
    scratch = [] if merge is None else [pltpu.VMEM(merge.shape, bf16)]
    return pl.pallas_call(
        functools.partial(place_kernel, merge is not None),
        out_shape=jax.ShapeDtypeStruct(out.shape, out.dtype),
        in_specs=[smem] + [vmem] * (len(operands) - 2) + [hbm],
        out_specs=hbm,
        scratch_shapes=scratch + [pltpu.SemaphoreType.DMA((block.shape[0],))],
        input_output_aliases={len(operands) - 1: 0},
        compiler_params=pltpu.CompilerParams(vmem_limit_bytes=8 * 2**20),
        cost_estimate=pl.CostEstimate(flops=1000000, bytes_accessed=2_000_000, transcendentals=0),
        name="place",
    )(*operands)


def to_lines(x):
    n = x.shape[0]
    return x.reshape(n, SIZE, 2, 2, LANES).transpose(0, 1, 3, 2, 4).reshape(n, 4 * SIZE, LANES)


def from_lines(x):
    n = x.shape[0]
    return x.reshape(n, SIZE, 2, 2, LANES).transpose(0, 1, 3, 2, 4).reshape(n, SIZE, 2, SIZE)


def shards(site_tensors, bond_weights, sector_sizes, kept_ranks, sketches, gate_ends, gate_pair):
    chain = lax.axis_size("chain")
    count = lax.axis_size("group") * chain
    site = lax.axis_index("group") * chain + lax.axis_index("chain")
    is_right = site % 2 == 1

    def swapped(value):
        return lax.ppermute(value, "chain", [(i, i ^ 1) for i in range(chain)])

    def onward(value, by):
        def place(n):
            return n % chain * (count // chain) + n // chain

        pairs = [(place(i), place(i + by)) for i in range(1, count, 2) if i + by < count]
        return lax.ppermute(value, ("chain", "group"), pairs)

    own = to_lines(site_tensors[0, 0])
    sectors = own.shape[0]
    got_a = swapped(lax.dynamic_slice_in_dim(own, jnp.where(is_right, 11, 3), 5, 0))

    column = lax.broadcasted_iota(jnp.int32, (sectors, SIZE), 1)
    lam = bond_weights[0, 0] * (column < sector_sizes[0, 0][:, None]).astype(f32)
    kept_line = jnp.pad(kept_ranks[0, 0].astype(f32)[None, :], ((0, 7), (0, SIZE - sectors)))
    packed = jnp.concatenate([lam, kept_line], axis=0)
    other = swapped(packed)
    before_left = onward(lam, 1)
    before_right = onward(lam, 2)

    got_b = swapped(lax.dynamic_slice_in_dim(own, jnp.where(is_right, 8, 0), 3, 0))
    half = lax.ppermute(
        site_tensors[0, 0, 7, :, 1, :], "chain", [(i, i - 1) for i in range(1, chain, 2)]
    )

    lam_prev = jnp.where(is_right, before_right, before_left)
    lam_prev = jnp.where(site < 2, jnp.ones_like(lam), lam_prev)
    lam_mid = jnp.where(is_right, other[:sectors], lam)
    lam_next = jnp.where(is_right, lam, other[:sectors])
    scale = jnp.pad(jnp.stack([lam_prev, lam_mid, lam_next]), ((0, 0), (1, 7), (0, 0)))
    scale = scale[:, :, None, :]
    kept = jnp.where(is_right, other[sectors, :sectors], kept_line[0, :sectors]).astype(jnp.int32)
    gates = jnp.concatenate([gate_ends, 1.0 + gate_pair[:2], gate_pair[2:]])
    flag = is_right.astype(jnp.int32)
    role_a = jnp.stack([flag, 12 - 8 * flag])
    role_b = jnp.stack([flag, 8 - 8 * flag])

    msg_a, out, carry = compute(False, role_a, gates, kept, own, got_a, scale, sketches)
    back_a = swapped(msg_a)
    msg_b, out, merge = compute(
        True, role_b, gates, kept, own, got_a, scale, sketches, got_b, half, carry, out
    )
    back_b = swapped(msg_b)

    back_at = 8 * flag
    out = place(out, back_a, back_at + 4, merge)
    out = place(out, back_b, back_at)
    return from_lines(out)[None, None]


def solution(mesh):
    return jax.shard_map(
        shards,
        mesh=mesh,
        in_specs=(
            P("group", "chain", None, None, None, None),
            P("group", "chain", None, None),
            P("group", "chain", None),
            P("group", "chain", None),
            P(),
            P(),
            P(),
        ),
        out_specs=P("group", "chain", None, None, None, None),
        check_vma=False,
    )
```

```python
import functools

import jax
import jax.numpy as jnp
from jax import lax
from jax.experimental import pallas as pl
from jax.experimental.pallas import tpu as pltpu
from jax.sharding import PartitionSpec as P

f32 = jnp.float32
bf16 = jnp.bfloat16


BATCH = 4
LEAF = 32
PANELS = 8
LANES = 128
SIZE = 256


def split(x):
    high = x.astype(bf16)
    return high, (x - high.astype(f32)).astype(bf16)


def invert_leaf(d):
    lane = lax.broadcasted_iota(jnp.int32, (8, LANES), 1)
    sub = lax.broadcasted_iota(jnp.int32, (8, LANES), 0)
    segment = (lane // LEAF) * LEAF
    tiles = LEAF // 8
    rows = [d[8 * t : 8 * t + 8, :] for t in range(tiles)]
    cols = [
        [
            jnp.take_along_axis(rows[t], segment + j, axis=1) if t >= j // 8 else None
            for t in range(tiles)
        ]
        for j in range(LEAF)
    ]
    inverse = [((lane - segment) == (sub + 8 * t)).astype(f32) for t in range(tiles)]
    pivots = [jnp.ones((8, LANES), f32) for _ in range(tiles)]

    def row(v, r):
        return jnp.broadcast_to(v[r : r + 1, :], (8, LANES))

    for j in range(LEAF):
        top, r = j // 8, j % 8
        pivot = row(cols[j][top], r)
        reciprocal = 1.0 / pivot
        pivots[top] = jnp.where(sub == r, pivot, pivots[top])
        scaled = {t: cols[j][t] * reciprocal for t in range(top, tiles)}
        for i in range(j + 1, LEAF):
            factor = row(scaled[i // 8], i % 8)
            for t in range(i // 8, tiles):
                cols[i][t] = cols[i][t] - factor * cols[j][t]
        source = row(inverse[top], r)
        for t in range(top, tiles):
            factor = jnp.where(sub > r, scaled[t], 0.0) if t == top else scaled[t]
            inverse[t] = inverse[t] - factor * source
    return jnp.concatenate([inverse[t] * lax.rsqrt(pivots[t]) for t in range(tiles)], axis=0)


def block_weights(high, low, masks):
    high = jnp.concatenate([high * mask for mask in masks], axis=0)
    low = jnp.concatenate([low * mask for mask in masks], axis=0)
    upper = jnp.concatenate([high, high], axis=1)
    lower = jnp.concatenate([low, jnp.zeros_like(low)], axis=1)
    return jnp.concatenate([upper, lower], axis=0)


def times_transposed(x, weights):
    out = lax.dot_general(x, weights, (((1,), (1,)), ((), ())), preferred_element_type=f32)
    return out[:, :LANES] + out[:, LANES:]


def invert_factor(a_ref, x_ref):
    lane = lax.broadcasted_iota(jnp.int32, (LEAF, LANES), 1)
    sub = lax.broadcasted_iota(jnp.int32, (LEAF, LANES), 0)
    eye = ((lane % LEAF) == sub).astype(f32)
    masks = [((lane // LEAF) == b).astype(f32).astype(bf16) for b in range(BATCH)]

    def weights_of(rows, ks):
        return jnp.concatenate(
            [
                block_weights(
                    x_ref[rows, k * SIZE : k * SIZE + LANES],
                    x_ref[rows, k * SIZE + LANES : (k + 1) * SIZE],
                    masks,
                )
                for k in ks
            ],
            axis=1,
        )

    partial = None
    for j in range(PANELS):
        start = j * LEAF
        block = slice(start, start + LEAF)
        col = a_ref[j]
        if j:
            last = slice((j - 1) * SIZE, j * SIZE)
            if partial is not None:
                col = col - partial
            col = col - times_transposed(x_ref[:, last], weights_of(block, [j - 1]))
            x_ref[block, : j * SIZE] = jnp.zeros((LEAF, j * SIZE), bf16)
            if j < PANELS - 1:
                following = slice(start + LEAF, start + 2 * LEAF)
                partial = times_transposed(
                    x_ref[:, : j * SIZE], weights_of(following, range(j))
                )
        inverse = invert_leaf(col[block])
        col = jnp.concatenate(
            [part for part in (col[:start], eye, col[start + LEAF :]) if part.shape[0]], axis=0
        )
        col = times_transposed(
            jnp.concatenate(split(col), axis=1), block_weights(*split(inverse), masks)
        )
        x_ref[:, j * SIZE : (j + 1) * SIZE] = jnp.concatenate(split(col), axis=1)


def compute_kernel(second, *refs):
    (role, gates, kept, own, got, scale, sketch), refs = refs[:7], refs[7:]
    if second:
        carry = refs[0]
        (msg, out, merge), refs = refs[2:5], refs[5:]
    else:
        (msg, out, carry), refs = refs[:3], refs[3:]
    left_w, right_w, mixed, samp, gram, a_ref, x_ref, scaled_ref, wide_t, wide_p = refs[:10]
    got_win, mine, got_sem, mine_sem = refs[10:]
    is_right = role[0] == 1
    first = role[1]
    own_first = role[2]
    g0, g1, p0, p1, p2 = [gates[i] for i in range(5)]

    def got_copy(t):
        return pltpu.make_async_copy(got.at[t], got_win.at[t], got_sem.at[t])

    for t in range(got.shape[0]):
        got_copy(t).start()

    def row_scale(which, q):
        line = scale[which, q + 1]
        return jnp.transpose(jnp.broadcast_to(line, (LANES, SIZE)))

    def weigh(t, loop):
        q = first - 1 + t
        at = jnp.maximum(t - 1, 0) if second else jnp.minimum(t, 4)

        if not (second and isinstance(t, int)):

            @pl.when(True if second else t < 5)
            def _():
                got_copy(at).wait()

        own_wide = own[jnp.clip(q, 0, 15) - own_first].astype(f32)
        got_wide = got_win[at].astype(f32)
        wide_t[...] = jnp.where(is_right, got_wide, own_wide)
        wide_p[...] = jnp.where(is_right, own_wide, got_wide)
        left_rows = row_scale(0, q)
        right_rows = row_scale(1, q)
        for s in range(2):
            col = scale[2, q + s + 1]
            for jb in range(2):
                lines = pl.ds(2 * jb + s, SIZE, stride=4)
                lanes = slice(jb * LANES, (jb + 1) * LANES)
                left_w[t, s, :, lanes] = (wide_t[lines, :] * left_rows).astype(bf16)
                value = (wide_p[lines, :] * right_rows) * col[:, lanes]
                right_w[t, s, :, lanes] = value.astype(bf16)
        return loop

    if second:
        lax.fori_loop(1, 4, weigh, 0)
        weigh(0, 0)
        right_w[0, 1] = carry[6]
        for s in range(2):
            left_w[4, s] = carry[1 + s]
            right_w[4, s] = carry[3 + s]
        right_w[5, 0] = carry[5]
    else:
        lax.fori_loop(0, 6, weigh, 0)
        for s in range(2):
            carry[1 + s] = left_w[0, s]
            carry[3 + s] = right_w[0, s]
        carry[5] = right_w[1, 0]
        q = first - 5
        wide_p[...] = got_win[4].astype(f32)
        right_rows = row_scale(1, q)
        col = scale[2, q + 2]
        for jb in range(2):
            lanes = slice(jb * LANES, (jb + 1) * LANES)
            value = (wide_p[pl.ds(2 * jb + 1, SIZE, stride=4), :] * right_rows) * col[:, lanes]
            carry[6, :, lanes] = value.astype(bf16)

    def dot(a, b):
        return jnp.dot(a, b, preferred_element_type=f32)

    lane256 = lax.broadcasted_iota(jnp.int32, (1, SIZE), 1)
    eye = lax.broadcasted_iota(jnp.int32, (SIZE, SIZE), 0) == lax.broadcasted_iota(
        jnp.int32, (SIZE, SIZE), 1
    )
    upper, lower = slice(0, SIZE), slice(SIZE, 2 * SIZE)
    contract_rows = (((0,), (0,)), ((), ()))

    def sample(b, loop):
        t = b + 1
        left = [left_w[t, 0], left_w[t, 1], left_w[b, 0], left_w[b, 1]]
        right = [right_w[t, 0], right_w[t, 1]]
        mixed[b, upper, upper] = (g0 * dot(left[0], right[0])).astype(bf16)
        mixed[b, upper, lower] = (
            p0 * dot(left[0], right[1]) + p2 * dot(left[1], right_w[t + 1, 0])
        ).astype(bf16)
        mixed[b, lower, upper] = (
            p2 * dot(left[2], right_w[b, 1]) + p1 * dot(left[3], right[0])
        ).astype(bf16)
        mixed[b, lower, lower] = (g1 * dot(left[3], right[1])).astype(bf16)
        keep = lane256 < kept[first + b]
        sampled = jnp.where(keep, dot(mixed[b], sketch[b]), 0.0)
        high, low = split(sampled)
        samp[b, 0] = high
        samp[b, 1] = low
        shift = 0.01 * jnp.sum(sampled * sampled) / SIZE
        hh = lax.dot_general(high, high, contract_rows, preferred_element_type=f32)
        hl = lax.dot_general(high, low, contract_rows, preferred_element_type=f32)
        added = jnp.where(keep, 0.0, 1.0) + shift
        gram[b] = (hh + (hl + jnp.transpose(hl))) + jnp.where(eye, added, 0.0)
        return loop

    lax.fori_loop(0, BATCH, sample, 0, unroll=True)

    segment = lax.broadcasted_iota(jnp.int32, (1, LANES), 1) // LEAF

    def gather_lanes(pieces):
        out = pieces[0]
        for i in range(1, BATCH):
            out = jnp.where(segment == i, pieces[i], out)
        return out

    def rolled(value, segments):
        shift = (segments * LEAF) % LANES
        return pltpu.roll(value, shift, axis=1) if shift else value

    for k in range(PANELS):
        rows = slice(k * LEAF, SIZE)
        lanes = slice((k // 4) * LANES, (k // 4 + 1) * LANES)
        a_ref[k, rows, :] = gather_lanes(
            [rolled(gram[b, rows, lanes], b - k % 4) for b in range(BATCH)]
        )
        if k:
            a_ref[k, : k * LEAF, :] = jnp.zeros((k * LEAF, LANES), f32)

    invert_factor(a_ref, x_ref)

    for b in range(BATCH):
        high, low = [
            jnp.concatenate(
                [
                    gather_lanes(
                        [
                            rolled(
                                x_ref[:, k * SIZE + offset : k * SIZE + offset + LANES].astype(f32),
                                k % 4 - b,
                            )
                            for k in range(4 * g, 4 * g + 4)
                        ]
                    )
                    for g in range(2)
                ],
                axis=1,
            ).astype(bf16)
            for offset in (0, LANES)
        ]
        solved = dot(samp[b, 0], high) + (dot(samp[b, 0], low) + dot(samp[b, 1], high))
        scaled_ref[b] = (solved * 16.0).astype(bf16)

    if second:
        scaled_ref[BATCH, lower, :] = carry[0]
    else:
        scaled_ref[BATCH, lower, :] = jnp.zeros((SIZE, SIZE), bf16)
        carry[0] = scaled_ref[0, lower, :]

    def deliver(b, loop):
        right_part = lax.dot_general(
            scaled_ref[b], mixed[b], contract_rows, preferred_element_type=f32
        ) * (1.0 / SIZE)
        for s in range(2):
            left_half = scaled_ref[b, upper, :] if s == 0 else scaled_ref[b + 1, lower, :]
            for jb in range(2):
                lines = pl.ds(2 * jb + s, SIZE, stride=4)
                wide_t[lines, :] = left_half[:, jb * LANES : (jb + 1) * LANES].astype(f32)
                start = s * SIZE + jb * LANES
                wide_p[lines, :] = right_part[:, start : start + LANES]
        left_site = wide_t[...]
        right_site = wide_p[...]
        msg[b] = jnp.where(is_right, left_site, right_site).astype(bf16)
        mine[b] = jnp.where(is_right, right_site, left_site).astype(bf16)
        mine_copy(b).start()
        return loop

    def mine_copy(b):
        at = first + b
        return pltpu.make_async_copy(mine.at[b], out.at[at], mine_sem.at[b])

    lax.fori_loop(0, BATCH, deliver, 0, unroll=True)

    if second:
        used = jnp.where(is_right, 0.0, 1.0)
        for jb in range(2):
            value = scaled_ref[0, lower, jb * LANES : (jb + 1) * LANES].astype(f32)
            wide_t[pl.ds(2 * jb, SIZE, stride=4), :] = jnp.zeros((SIZE, LANES), f32)
            wide_t[pl.ds(2 * jb + 1, SIZE, stride=4), :] = value * used
        merge[...] = wide_t[...].astype(bf16)
    for b in range(BATCH):
        mine_copy(b).wait()


def in_hbm(x):
    return pltpu.with_memory_space_constraint(x, pltpu.HBM)


def pack_kernel(role, own, out, both, sems):
    flag = role[0]
    bulk = pltpu.make_async_copy(own.at[pl.ds(3 + 8 * flag, 4)], out.at[pl.ds(0, 4)], sems.at[0])
    even = pltpu.make_async_copy(own.at[7 + 8 * flag], both.at[0], sems.at[1])
    odd = pltpu.make_async_copy(own.at[7], both.at[1], sems.at[2])
    even.start()
    odd.start()
    bulk.start()
    even.wait()
    odd.wait()
    is_odd = lax.broadcasted_iota(jnp.int32, (4 * SIZE, LANES), 0) % 2 == 1
    out[4] = jnp.where(is_odd, both[1].astype(f32), both[0].astype(f32)).astype(bf16)
    bulk.wait()


def pack(role, own):
    return pl.pallas_call(
        pack_kernel,
        out_shape=jax.ShapeDtypeStruct((5,) + own.shape[1:], bf16),
        in_specs=[
            pl.BlockSpec(memory_space=pltpu.SMEM),
            pl.BlockSpec(memory_space=pltpu.HBM),
        ],
        out_specs=pl.BlockSpec(memory_space=pltpu.VMEM),
        scratch_shapes=[
            pltpu.VMEM((2,) + own.shape[1:], bf16),
            pltpu.SemaphoreType.DMA((3,)),
        ],
        compiler_params=pltpu.CompilerParams(vmem_limit_bytes=4 * 2**20),
        name="pack",
    )(role, in_hbm(own))


def compute(second, role, gates, kept, own, got, scale, sketch, carry=None, out=None):
    smem = pl.BlockSpec(memory_space=pltpu.SMEM)
    vmem = pl.BlockSpec(memory_space=pltpu.VMEM)
    hbm = pl.BlockSpec(memory_space=pltpu.HBM)
    operands = (role, gates, kept, own, in_hbm(got), scale, sketch)
    specs = [smem] * 3 + [vmem, hbm, vmem, vmem]
    if second:
        operands += (carry, out)
        specs += [vmem, hbm]
        third = jax.ShapeDtypeStruct((4 * SIZE, LANES), bf16)
        whole = jax.ShapeDtypeStruct(out.shape, bf16)
    else:
        third = jax.ShapeDtypeStruct((7, SIZE, SIZE), bf16)
        whole = jax.ShapeDtypeStruct((16, 4 * SIZE, LANES), bf16)
    part = jax.ShapeDtypeStruct((BATCH, 4 * SIZE, LANES), bf16)
    return pl.pallas_call(
        functools.partial(compute_kernel, second),
        out_shape=(part, whole, third),
        in_specs=specs,
        out_specs=(vmem, hbm, vmem),
        scratch_shapes=[
            pltpu.VMEM((6, 2, SIZE, SIZE), bf16),
            pltpu.VMEM((6, 2, SIZE, SIZE), bf16),
            pltpu.VMEM((BATCH, 2 * SIZE, 2 * SIZE), bf16),
            pltpu.VMEM((BATCH, 2, 2 * SIZE, SIZE), bf16),
            pltpu.VMEM((BATCH, SIZE, SIZE), f32),
            pltpu.VMEM((PANELS, SIZE, LANES), f32),
            pltpu.VMEM((SIZE, PANELS * SIZE), bf16),
            pltpu.VMEM((BATCH + 1, 2 * SIZE, SIZE), bf16),
            pltpu.VMEM((4 * SIZE, LANES), f32),
            pltpu.VMEM((4 * SIZE, LANES), f32),
            pltpu.VMEM(got.shape, bf16),
            pltpu.VMEM((BATCH, 4 * SIZE, LANES), bf16),
            pltpu.SemaphoreType.DMA((got.shape[0],)),
            pltpu.SemaphoreType.DMA((BATCH,)),
        ],
        input_output_aliases={8: 1} if second else {},
        compiler_params=pltpu.CompilerParams(vmem_limit_bytes=22 * 2**20),
        cost_estimate=pl.CostEstimate(
            flops=20_000_000_000, bytes_accessed=8_000_000, transcendentals=0
        ),
        name="second_half" if second else "first_half",
    )(*operands)


def place_kernel(merged, at, block, *refs):
    if merged:
        merge, _, out, last, sems = refs
    else:
        _, out, sems = refs
    count = block.shape[0]
    copies = []
    for b in range(count):
        source = block.at[b]
        if merged and b == count - 1:
            last[...] = block[b] + merge[...]
            source = last
        copies.append(pltpu.make_async_copy(source, out.at[at[0] + b], sems.at[b]))
        copies[-1].start()
    for copy in copies:
        copy.wait()


def place(out, block, at, merge=None):
    smem = pl.BlockSpec(memory_space=pltpu.SMEM)
    vmem = pl.BlockSpec(memory_space=pltpu.VMEM)
    hbm = pl.BlockSpec(memory_space=pltpu.HBM)
    operands = (jnp.reshape(at, (1,)), block) + (() if merge is None else (merge,)) + (out,)
    scratch = [] if merge is None else [pltpu.VMEM(merge.shape, bf16)]
    return pl.pallas_call(
        functools.partial(place_kernel, merge is not None),
        out_shape=jax.ShapeDtypeStruct(out.shape, out.dtype),
        in_specs=[smem] + [vmem] * (len(operands) - 2) + [hbm],
        out_specs=hbm,
        scratch_shapes=scratch + [pltpu.SemaphoreType.DMA((block.shape[0],))],
        input_output_aliases={len(operands) - 1: 0},
        compiler_params=pltpu.CompilerParams(vmem_limit_bytes=8 * 2**20),
        cost_estimate=pl.CostEstimate(flops=1000000, bytes_accessed=2_000_000, transcendentals=0),
        name="place",
    )(*operands)


def to_lines(x):
    n = x.shape[0]
    return x.reshape(n, SIZE, 2, 2, LANES).transpose(0, 1, 3, 2, 4).reshape(n, 4 * SIZE, LANES)


def from_lines(x):
    n = x.shape[0]
    return x.reshape(n, SIZE, 2, 2, LANES).transpose(0, 1, 3, 2, 4).reshape(n, SIZE, 2, SIZE)


def shards(site_tensors, bond_weights, sector_sizes, kept_ranks, sketches, gate_ends, gate_pair):
    chain = lax.axis_size("chain")
    count = lax.axis_size("group") * chain
    site = lax.axis_index("group") * chain + lax.axis_index("chain")
    is_right = site % 2 == 1

    def swapped(value):
        return lax.ppermute(value, "chain", [(i, i ^ 1) for i in range(chain)])

    def onward(value, by):
        def place(n):
            return n % chain * (count // chain) + n // chain

        pairs = [(place(i), place(i + by)) for i in range(1, count, 2) if i + by < count]
        return lax.ppermute(value, ("chain", "group"), pairs)

    own = to_lines(site_tensors[0, 0])
    sectors = own.shape[0]
    flag = is_right.astype(jnp.int32)

    def window(array, start, size):
        return lax.dynamic_slice_in_dim(array, start, size, 0)

    got_a = swapped(pack(jnp.reshape(flag, (1,)), own))

    column = lax.broadcasted_iota(jnp.int32, (sectors, SIZE), 1)
    lam = bond_weights[0, 0] * (column < sector_sizes[0, 0][:, None]).astype(f32)
    kept_line = jnp.pad(kept_ranks[0, 0].astype(f32)[None, :], ((0, 7), (0, SIZE - sectors)))
    packed = jnp.concatenate([lam, kept_line], axis=0)
    other = swapped(packed)
    before_left = onward(lam, 1)
    before_right = onward(lam, 2)

    got_b = swapped(window(own, 8 * flag, 3))

    lam_prev = jnp.where(is_right, before_right, before_left)
    lam_prev = jnp.where(site < 2, jnp.ones_like(lam), lam_prev)
    lam_mid = jnp.where(is_right, other[:sectors], lam)
    lam_next = jnp.where(is_right, lam, other[:sectors])
    scale = jnp.pad(jnp.stack([lam_prev, lam_mid, lam_next]), ((0, 0), (1, 7), (0, 0)))
    scale = scale[:, :, None, :]
    kept = jnp.where(is_right, other[sectors, :sectors], kept_line[0, :sectors]).astype(jnp.int32)
    gates = jnp.concatenate([gate_ends, 1.0 + gate_pair[:2], gate_pair[2:]])
    first_a = 12 - 8 * flag
    first_b = 8 - 8 * flag
    own_a = 10 - 7 * flag
    own_b = 7 - 7 * flag
    role_a = jnp.stack([flag, first_a, own_a])
    role_b = jnp.stack([flag, first_b, own_b])

    msg_a, out, carry = compute(
        False, role_a, gates, kept, window(own, own_a, 6), got_a, scale, window(sketches, first_a, 4)
    )
    back_a = swapped(msg_a)
    msg_b, out, merge = compute(
        True,
        role_b,
        gates,
        kept,
        window(own, own_b, 4),
        got_b,
        scale,
        window(sketches, first_b, 4),
        carry,
        out,
    )
    back_b = swapped(msg_b)

    back_at = 8 * flag
    out = place(out, back_a, back_at + 4, merge)
    out = place(out, back_b, back_at)
    return from_lines(out)[None, None]


def solution(mesh):
    return jax.shard_map(
        shards,
        mesh=mesh,
        in_specs=(
            P("group", "chain", None, None, None, None),
            P("group", "chain", None, None),
            P("group", "chain", None),
            P("group", "chain", None),
            P(),
            P(),
            P(),
        ),
        out_specs=P("group", "chain", None, None, None, None),
        check_vma=False,
    )
```

```python
import functools

import jax
import jax.numpy as jnp
from jax import lax
from jax.experimental import pallas as pl
from jax.experimental.pallas import tpu as pltpu
from jax.sharding import PartitionSpec as P

f32 = jnp.float32
bf16 = jnp.bfloat16


BATCH = 4
LEAF = 32
PANELS = 8
LANES = 128
SIZE = 256


def split(x):
    high = x.astype(bf16)
    return high, (x - high.astype(f32)).astype(bf16)


def invert_leaf(d):
    lane = lax.broadcasted_iota(jnp.int32, (8, LANES), 1)
    sub = lax.broadcasted_iota(jnp.int32, (8, LANES), 0)
    segment = (lane // LEAF) * LEAF
    tiles = LEAF // 8
    rows = [d[8 * t : 8 * t + 8, :] for t in range(tiles)]
    cols = [
        [
            jnp.take_along_axis(rows[t], segment + j, axis=1) if t >= j // 8 else None
            for t in range(tiles)
        ]
        for j in range(LEAF)
    ]
    inverse = [((lane - segment) == (sub + 8 * t)).astype(f32) for t in range(tiles)]
    pivots = [jnp.ones((8, LANES), f32) for _ in range(tiles)]

    def row(v, r):
        return jnp.broadcast_to(v[r : r + 1, :], (8, LANES))

    for j in range(LEAF):
        top, r = j // 8, j % 8
        pivot = row(cols[j][top], r)
        reciprocal = 1.0 / pivot
        pivots[top] = jnp.where(sub == r, pivot, pivots[top])
        scaled = {t: cols[j][t] * reciprocal for t in range(top, tiles)}
        for i in range(j + 1, LEAF):
            factor = row(scaled[i // 8], i % 8)
            for t in range(i // 8, tiles):
                cols[i][t] = cols[i][t] - factor * cols[j][t]
        source = row(inverse[top], r)
        for t in range(top, tiles):
            factor = jnp.where(sub > r, scaled[t], 0.0) if t == top else scaled[t]
            inverse[t] = inverse[t] - factor * source
    return jnp.concatenate([inverse[t] * lax.rsqrt(pivots[t]) for t in range(tiles)], axis=0)


def block_weights(high, low, masks):
    high = jnp.concatenate([high * mask for mask in masks], axis=0)
    low = jnp.concatenate([low * mask for mask in masks], axis=0)
    upper = jnp.concatenate([high, high], axis=1)
    lower = jnp.concatenate([low, jnp.zeros_like(low)], axis=1)
    return jnp.concatenate([upper, lower], axis=0)


def times_transposed(x, weights):
    out = lax.dot_general(x, weights, (((1,), (1,)), ((), ())), preferred_element_type=f32)
    return out[:, :LANES] + out[:, LANES:]


def invert_factor(a_ref, x_ref):
    lane = lax.broadcasted_iota(jnp.int32, (LEAF, LANES), 1)
    sub = lax.broadcasted_iota(jnp.int32, (LEAF, LANES), 0)
    eye = ((lane % LEAF) == sub).astype(f32)
    masks = [((lane // LEAF) == b).astype(f32).astype(bf16) for b in range(BATCH)]

    def weights_of(rows, ks):
        return jnp.concatenate(
            [
                block_weights(
                    x_ref[rows, k * SIZE : k * SIZE + LANES],
                    x_ref[rows, k * SIZE + LANES : (k + 1) * SIZE],
                    masks,
                )
                for k in ks
            ],
            axis=1,
        )

    partial = None
    for j in range(PANELS):
        start = j * LEAF
        block = slice(start, start + LEAF)
        col = a_ref[j]
        if j:
            last = slice((j - 1) * SIZE, j * SIZE)
            if partial is not None:
                col = col - partial
            col = col - times_transposed(x_ref[:, last], weights_of(block, [j - 1]))
            x_ref[block, : j * SIZE] = jnp.zeros((LEAF, j * SIZE), bf16)
            if j < PANELS - 1:
                following = slice(start + LEAF, start + 2 * LEAF)
                partial = times_transposed(
                    x_ref[:, : j * SIZE], weights_of(following, range(j))
                )
        inverse = invert_leaf(col[block])
        col = jnp.concatenate(
            [part for part in (col[:start], eye, col[start + LEAF :]) if part.shape[0]], axis=0
        )
        col = times_transposed(
            jnp.concatenate(split(col), axis=1), block_weights(*split(inverse), masks)
        )
        x_ref[:, j * SIZE : (j + 1) * SIZE] = jnp.concatenate(split(col), axis=1)


UPPER, LOWER = slice(0, SIZE), slice(SIZE, 2 * SIZE)
CONTRACT_ROWS = (((0,), (0,)), ((), ()))


def dot(a, b):
    return jnp.dot(a, b, preferred_element_type=f32)


def lines_of(lane_block, s):
    return pl.ds(2 * lane_block + s, SIZE, stride=4)


def lanes_of(lane_block):
    return slice(lane_block * LANES, (lane_block + 1) * LANES)


def column_of(line):
    return jnp.transpose(jnp.broadcast_to(line, (LANES, SIZE)))


def weigh(t, role, own, got, scale, left, right, wide):
    is_right = role[0] == 1
    q = role[1] - 1 + t
    own_wide = own[jnp.clip(q, 0, 15) - role[2]].astype(f32)
    got_wide = got[...].astype(f32)
    wide[0] = jnp.where(is_right, got_wide, own_wide)
    wide[1] = jnp.where(is_right, own_wide, got_wide)
    left_rows = column_of(scale[0, q + 1])
    right_rows = column_of(scale[1, q + 1])
    for s in range(2):
        col = scale[2, q + s + 1]
        for jb in range(2):
            lines, lanes = lines_of(jb, s), lanes_of(jb)
            left[s, :, lanes] = (wide[0, lines, :] * left_rows).astype(bf16)
            right[s, :, lanes] = ((wide[1, lines, :] * right_rows) * col[:, lanes]).astype(bf16)


def sample(gates, kept, sketch, left, before, right, right_before, right_after, mixed, samp, gram):
    g0, g1, p0, p1, p2 = [gates[i] for i in range(5)]
    mixed[UPPER, UPPER] = (g0 * dot(left[0], right[0])).astype(bf16)
    mixed[UPPER, LOWER] = (p0 * dot(left[0], right[1]) + p2 * dot(left[1], right_after)).astype(bf16)
    mixed[LOWER, UPPER] = (
        p2 * dot(before[0], right_before) + p1 * dot(before[1], right[0])
    ).astype(bf16)
    mixed[LOWER, LOWER] = (g1 * dot(before[1], right[1])).astype(bf16)
    keep = lax.broadcasted_iota(jnp.int32, (1, SIZE), 1) < kept
    sampled = jnp.where(keep, dot(mixed[...], sketch), 0.0)
    high, low = split(sampled)
    samp[0] = high
    samp[1] = low
    shift = 0.01 * jnp.sum(sampled * sampled) / SIZE
    hh = lax.dot_general(high, high, CONTRACT_ROWS, preferred_element_type=f32)
    hl = lax.dot_general(high, low, CONTRACT_ROWS, preferred_element_type=f32)
    rows = lax.broadcasted_iota(jnp.int32, (SIZE, SIZE), 0)
    eye = rows == lax.broadcasted_iota(jnp.int32, (SIZE, SIZE), 1)
    added = jnp.where(keep, 0.0, 1.0) + shift
    gram[...] = (hh + (hl + jnp.transpose(hl))) + jnp.where(eye, added, 0.0)


def rolled(value, segments):
    shift = (segments * LEAF) % LANES
    return pltpu.roll(value, shift, axis=1) if shift else value


def gather_lanes(pieces):
    segment = lax.broadcasted_iota(jnp.int32, (1, LANES), 1) // LEAF
    out = pieces[0]
    for i in range(1, BATCH):
        out = jnp.where(segment == i, pieces[i], out)
    return out


def solve(gram, samp, scaled, a_ref, x_ref):
    for k in range(PANELS):
        rows = slice(k * LEAF, SIZE)
        lanes = lanes_of(k // 4)
        a_ref[k, rows, :] = gather_lanes(
            [rolled(gram[b][rows, lanes], b - k % 4) for b in range(BATCH)]
        )
        if k:
            a_ref[k, : k * LEAF, :] = jnp.zeros((k * LEAF, LANES), f32)

    invert_factor(a_ref, x_ref)

    def factor(b, offset):
        halves = []
        for g in range(2):
            panels = [
                rolled(x_ref[:, k * SIZE + offset : k * SIZE + offset + LANES], k % 4 - b)
                for k in range(4 * g, 4 * g + 4)
            ]
            halves.append(gather_lanes(panels))
        return jnp.concatenate(halves, axis=1)

    for b in range(BATCH):
        high, low = factor(b, 0), factor(b, LANES)
        solved = dot(samp[b][0], high) + (dot(samp[b][0], low) + dot(samp[b][1], high))
        scaled[b] = (solved * 16.0).astype(bf16)


def deliver(role, scaled, mixed, wide, ready, msg, out, sems):
    is_right = role[0] == 1
    copies = []
    for b in range(BATCH):
        right_part = lax.dot_general(
            scaled[b], mixed[b][...], CONTRACT_ROWS, preferred_element_type=f32
        ) * (1.0 / SIZE)
        left_wide, right_wide = wide.at[2 * (b % 2)], wide.at[2 * (b % 2) + 1]
        for s in range(2):
            half = scaled[b, UPPER, :] if s == 0 else scaled[b + 1, LOWER, :]
            for jb in range(2):
                lines = lines_of(jb, s)
                left_wide[lines, :] = half[:, lanes_of(jb)].astype(f32)
                right_wide[lines, :] = right_part[:, lanes_of(2 * s + jb)]
        left_site = left_wide[...]
        right_site = right_wide[...]
        ready[0, b] = jnp.where(is_right, left_site, right_site).astype(bf16)
        ready[1, b] = jnp.where(is_right, right_site, left_site).astype(bf16)
        for which, target in enumerate((msg.at[b], out.at[role[1] + b])):
            copies.append(
                pltpu.make_async_copy(ready.at[which, b], target, sems.at[which, b])
            )
            copies[-1].start()
    return copies


def early_kernel(role, gates, kept, own, got, scale, sketch, *refs):
    mixed, samp, gram, edge, left_w, right_w, wide = refs

    def step(t, loop):
        at = jnp.minimum(t - 1, 3)
        weigh(t, role, own, got.at[at], scale, left_w.at[t], right_w.at[t], wide)
        return loop

    lax.fori_loop(1, 6, step, 0)
    for s in range(2):
        edge[s] = left_w[1, s]
        edge[2 + s] = right_w[1, s]
    edge[4] = right_w[2, 0]
    below = role[1] - 5
    wide[0] = got[3].astype(f32)
    rows = column_of(scale[1, below + 1])
    col = scale[2, below + 2]
    for jb in range(2):
        lanes = lanes_of(jb)
        edge[5, :, lanes] = ((wide[0, lines_of(jb, 1), :] * rows) * col[:, lanes]).astype(bf16)
    for b in range(1, BATCH):
        t = b + 1
        sample(
            gates,
            kept[role[1] + b],
            sketch[b],
            (left_w[t, 0], left_w[t, 1]),
            (left_w[t - 1, 0], left_w[t - 1, 1]),
            (right_w[t, 0], right_w[t, 1]),
            right_w[t - 1, 1],
            right_w[t + 1, 0],
            mixed.at[b - 1],
            samp.at[b - 1],
            gram.at[b - 1],
        )


def first_kernel(role, gates, kept, own, got, scale, sketch, *refs):
    (mixed_e, samp_e, gram_e, edge, msg, out, carry), refs = refs[:7], refs[7:]
    mixed, samp, gram, scaled, a_ref, x_ref, wide, ready, sems = refs
    left, right = carry.at[pl.ds(1, 2)], carry.at[pl.ds(3, 2)]
    weigh(0, role, own, got.at[0], scale, left, right, wide)
    sample(
        gates,
        kept[role[1]],
        sketch[0],
        (edge[0], edge[1]),
        (left[0], left[1]),
        (edge[2], edge[3]),
        right[1],
        edge[4],
        mixed,
        samp,
        gram,
    )
    mixed = [mixed] + [mixed_e.at[b] for b in range(BATCH - 1)]
    samp = [samp] + [samp_e.at[b] for b in range(BATCH - 1)]
    gram = [gram] + [gram_e.at[b] for b in range(BATCH - 1)]
    solve(gram, samp, scaled, a_ref, x_ref)
    scaled[BATCH, LOWER, :] = jnp.zeros((SIZE, SIZE), bf16)
    carry[0] = scaled[0, LOWER, :]
    for copy in deliver(role, scaled, mixed, wide, ready, msg, out, sems):
        copy.wait()


def second_kernel(role, gates, kept, own, got, scale, sketch, *refs):
    (edge, carry, _, msg, out, merge), refs = refs[:6], refs[6:]
    left_w, right_w, mixed, samp, gram, scaled, a_ref, x_ref, wide = refs[:9]
    ready, sems = refs[9:]

    def step(t, loop):
        at = jnp.maximum(t - 1, 0)
        weigh(t, role, own, got.at[at], scale, left_w.at[t], right_w.at[t], wide)
        return loop

    lax.fori_loop(0, 4, step, 0)
    right_w[0, 1] = edge[5]
    for s in range(2):
        left_w[4, s] = carry[1 + s]
        right_w[4, s] = carry[3 + s]
    right_w[5, 0] = edge[2]
    for b in range(BATCH):
        t = b + 1
        sample(
            gates,
            kept[role[1] + b],
            sketch[b],
            (left_w[t, 0], left_w[t, 1]),
            (left_w[b, 0], left_w[b, 1]),
            (right_w[t, 0], right_w[t, 1]),
            right_w[b, 1],
            right_w[t + 1, 0],
            mixed.at[b],
            samp.at[b],
            gram.at[b],
        )
    every = range(BATCH)
    solve([gram.at[b] for b in every], [samp.at[b] for b in every], scaled, a_ref, x_ref)
    scaled[BATCH, LOWER, :] = carry[0]
    copies = deliver(
        role, scaled, [mixed.at[b] for b in every], wide, ready, msg, out, sems
    )
    used = jnp.where(role[0] == 1, 0.0, 1.0)
    for jb in range(2):
        value = scaled[0, LOWER, lanes_of(jb)].astype(f32)
        wide[0, lines_of(jb, 0), :] = jnp.zeros((SIZE, LANES), f32)
        wide[0, lines_of(jb, 1), :] = value * used
    merge[...] = wide[0].astype(bf16)
    for copy in copies:
        copy.wait()


def in_hbm(x):
    return pltpu.with_memory_space_constraint(x, pltpu.HBM)


def shaped(*shape, dtype=bf16):
    return jax.ShapeDtypeStruct(shape, dtype)


def run(kernel, operands, specs, outs, out_specs, scratch, aliases=None, mib=20):
    return pl.pallas_call(
        kernel,
        out_shape=outs,
        in_specs=specs,
        out_specs=out_specs,
        scratch_shapes=scratch,
        input_output_aliases=aliases or {},
        compiler_params=pltpu.CompilerParams(vmem_limit_bytes=mib * 2**20),
        cost_estimate=pl.CostEstimate(
            flops=mib * 500_000_000, bytes_accessed=8_000_000, transcendentals=0
        ),
    )(*operands)


SMEM = pl.BlockSpec(memory_space=pltpu.SMEM)
VMEM = pl.BlockSpec(memory_space=pltpu.VMEM)
HBM = pl.BlockSpec(memory_space=pltpu.HBM)
SECTOR = (4 * SIZE, LANES)


def factor_scratch():
    return [
        pltpu.VMEM((BATCH + 1, 2 * SIZE, SIZE), bf16),
        pltpu.VMEM((PANELS, SIZE, LANES), f32),
        pltpu.VMEM((SIZE, PANELS * SIZE), bf16),
        pltpu.VMEM((4, *SECTOR), f32),
    ]


def sample_shapes(make, *lead):
    return [
        make((*lead, 2 * SIZE, 2 * SIZE), bf16),
        make((*lead, 2, 2 * SIZE, SIZE), bf16),
        make((*lead, SIZE, SIZE), f32),
    ]


def early(role, gates, kept, own, got, scale, sketch):
    return run(
        early_kernel,
        (role, gates, kept, own, got, scale, sketch),
        [SMEM] * 3 + [VMEM] * 4,
        sample_shapes(jax.ShapeDtypeStruct, BATCH - 1) + [shaped(6, SIZE, SIZE)],
        [VMEM] * 4,
        [
            pltpu.VMEM((6, 2, SIZE, SIZE), bf16),
            pltpu.VMEM((6, 2, SIZE, SIZE), bf16),
            pltpu.VMEM((2, *SECTOR), f32),
        ],
    )


def first_half(role, gates, kept, own, got, scale, sketch, parts):
    return run(
        first_kernel,
        (role, gates, kept, own, got, scale, sketch, *parts),
        [SMEM] * 3 + [VMEM] * 8,
        [shaped(BATCH, *SECTOR), shaped(16, *SECTOR), shaped(5, SIZE, SIZE)],
        [HBM, HBM, VMEM],
        sample_shapes(pltpu.VMEM)
        + factor_scratch()
        + [pltpu.VMEM((2, BATCH, *SECTOR), bf16), pltpu.SemaphoreType.DMA((2, BATCH))],
    )


def second_half(role, gates, kept, own, got, scale, sketch, edge, carry, out):
    return run(
        second_kernel,
        (role, gates, kept, own, got, scale, sketch, edge, carry, out),
        [SMEM] * 3 + [VMEM] * 6 + [HBM],
        [shaped(BATCH, *SECTOR), shaped(16, *SECTOR), shaped(*SECTOR)],
        [HBM, HBM, VMEM],
        [pltpu.VMEM((6, 2, SIZE, SIZE), bf16), pltpu.VMEM((6, 2, SIZE, SIZE), bf16)]
        + sample_shapes(pltpu.VMEM, BATCH)
        + factor_scratch()
        + [
            pltpu.VMEM((2, BATCH, *SECTOR), bf16),
            pltpu.SemaphoreType.DMA((2, BATCH)),
        ],
        aliases={9: 1},
    )


def pack_kernel(role, sizes, kept, lam, own, out, low, packed, both, sems):
    flag = role[0]
    copies = [
        pltpu.make_async_copy(own.at[7 + 8 * flag], both.at[0], sems.at[0]),
        pltpu.make_async_copy(own.at[7], both.at[1], sems.at[1]),
        pltpu.make_async_copy(own.at[pl.ds(4 + 8 * flag, 3)], out.at[pl.ds(0, 3)], sems.at[2]),
        pltpu.make_async_copy(own.at[3 + 8 * flag], low.at[0], sems.at[3]),
    ]
    for copy in copies:
        copy.start()
    lane = lax.broadcasted_iota(jnp.int32, (1, SIZE), 1)
    line = jnp.zeros((1, SIZE), f32)
    for q in range(16):
        packed[q : q + 1, :] = jnp.where(lane < sizes[q], lam[q : q + 1, :], 0.0)
        line = jnp.where(lane == q, kept[q].astype(f32), line)
    packed[16:24, :] = jnp.broadcast_to(line, (8, SIZE))
    copies[0].wait()
    copies[1].wait()
    is_odd = lax.broadcasted_iota(jnp.int32, SECTOR, 0) % 2 == 1
    out[3] = jnp.where(is_odd, both[1].astype(f32), both[0].astype(f32)).astype(bf16)
    copies[2].wait()
    copies[3].wait()


def pack(role, sizes, kept, lam, own):
    return run(
        pack_kernel,
        (role, sizes, kept, lam, in_hbm(own)),
        [SMEM] * 3 + [VMEM, HBM],
        [shaped(4, *SECTOR), shaped(1, *SECTOR), shaped(24, SIZE, dtype=f32)],
        [VMEM] * 3,
        [pltpu.VMEM((2, *SECTOR), bf16), pltpu.SemaphoreType.DMA((4,))],
        mib=2,
    )


def place_kernel(merged, at, block, *refs):
    if merged:
        merge, _, out, last, sems = refs
    else:
        _, out, sems = refs
    count = block.shape[0]
    copies = []
    for b in range(count):
        source = block.at[b]
        if merged and b == count - 1:
            last[...] = block[b] + merge[...]
            source = last
        copies.append(pltpu.make_async_copy(source, out.at[at[0] + b], sems.at[b]))
        copies[-1].start()
    for copy in copies:
        copy.wait()


def place(out, block, at, merge=None):
    smem = pl.BlockSpec(memory_space=pltpu.SMEM)
    vmem = pl.BlockSpec(memory_space=pltpu.VMEM)
    hbm = pl.BlockSpec(memory_space=pltpu.HBM)
    operands = (jnp.reshape(at, (1,)), block) + (() if merge is None else (merge,)) + (out,)
    scratch = [] if merge is None else [pltpu.VMEM(merge.shape, bf16)]
    return pl.pallas_call(
        functools.partial(place_kernel, merge is not None),
        out_shape=jax.ShapeDtypeStruct(out.shape, out.dtype),
        in_specs=[smem] + [vmem] * (len(operands) - 2) + [hbm],
        out_specs=hbm,
        scratch_shapes=scratch + [pltpu.SemaphoreType.DMA((block.shape[0],))],
        input_output_aliases={len(operands) - 1: 0},
        compiler_params=pltpu.CompilerParams(vmem_limit_bytes=8 * 2**20),
        cost_estimate=pl.CostEstimate(flops=1000000, bytes_accessed=2_000_000, transcendentals=0),
        name="place",
    )(*operands)


def to_lines(x):
    n = x.shape[0]
    return x.reshape(n, SIZE, 2, 2, LANES).transpose(0, 1, 3, 2, 4).reshape(n, 4 * SIZE, LANES)


def from_lines(x):
    n = x.shape[0]
    return x.reshape(n, SIZE, 2, 2, LANES).transpose(0, 1, 3, 2, 4).reshape(n, SIZE, 2, SIZE)


def shards(site_tensors, bond_weights, sector_sizes, kept_ranks, sketches, gate_ends, gate_pair):
    chain = lax.axis_size("chain")
    count = lax.axis_size("group") * chain
    site = lax.axis_index("group") * chain + lax.axis_index("chain")
    is_right = site % 2 == 1

    def swapped(value):
        return lax.ppermute(value, "chain", [(i, i ^ 1) for i in range(chain)])

    def onward(value, by):
        def place(n):
            return n % chain * (count // chain) + n // chain

        pairs = [(place(i), place(i + by)) for i in range(1, count, 2) if i + by < count]
        return lax.ppermute(value, ("chain", "group"), pairs)

    own = to_lines(site_tensors[0, 0])
    sectors = own.shape[0]
    flag = is_right.astype(jnp.int32)

    def window(array, start, size):
        return lax.dynamic_slice_in_dim(array, start, size, 0)

    outgoing, outgoing_low, packed = pack(
        jnp.reshape(flag, (1,)), sector_sizes[0, 0], kept_ranks[0, 0], bond_weights[0, 0], own
    )
    lam = packed[:sectors]
    other = swapped(packed)
    got_a = swapped(outgoing)
    got_low = swapped(outgoing_low)
    before_left = onward(lam, 1)
    before_right = onward(lam, 2)
    got_b = swapped(window(own, 8 * flag, 3))

    lam_prev = jnp.where(is_right, before_right, before_left)
    lam_prev = jnp.where(site < 2, jnp.ones_like(lam), lam_prev)
    lam_mid = jnp.where(is_right, other[:sectors], lam)
    lam_next = jnp.where(is_right, lam, other[:sectors])
    scale = jnp.pad(jnp.stack([lam_prev, lam_mid, lam_next]), ((0, 0), (1, 7), (0, 0)))
    scale = scale[:, :, None, :]
    kept = jnp.where(is_right, other[sectors, :sectors], packed[sectors, :sectors]).astype(jnp.int32)
    gates = jnp.concatenate([gate_ends, 1.0 + gate_pair[:2], gate_pair[2:]])
    first_a = 12 - 8 * flag
    first_b = 8 - 8 * flag
    own_a = 10 - 7 * flag
    own_b = 7 - 7 * flag
    role_a = jnp.stack([flag, first_a, own_a])
    role_b = jnp.stack([flag, first_b, own_b])

    own_win = window(own, own_a, 6)
    sketch_win = window(sketches, first_a, BATCH)
    parts = early(role_a, gates, kept, own_win, got_a, scale, sketch_win)
    msg_a, out, carry = first_half(
        role_a, gates, kept, own_win, got_low, scale, sketch_win, parts
    )
    back_a = swapped(msg_a)
    own_win = window(own, own_b, BATCH)
    sketch_win = window(sketches, first_b, BATCH)
    msg_b, out, merge = second_half(
        role_b, gates, kept, own_win, got_b, scale, sketch_win, parts[3], carry, out
    )
    back_b = swapped(msg_b)

    back_at = 8 * flag
    out = place(out, back_a, back_at + 4, merge)
    out = place(out, back_b, back_at)
    return from_lines(out)[None, None]


def solution(mesh):
    return jax.shard_map(
        shards,
        mesh=mesh,
        in_specs=(
            P("group", "chain", None, None, None, None),
            P("group", "chain", None, None),
            P("group", "chain", None),
            P("group", "chain", None),
            P(),
            P(),
            P(),
        ),
        out_specs=P("group", "chain", None, None, None, None),
        check_vma=False,
    )
```

```python
import functools

import jax
import jax.numpy as jnp
from jax import lax
from jax.experimental import pallas as pl
from jax.experimental.pallas import tpu as pltpu
from jax.sharding import PartitionSpec as P

f32 = jnp.float32
bf16 = jnp.bfloat16


BATCH = 4
LEAF = 32
PANELS = 8
LANES = 128
SIZE = 256


def split(x):
    high = x.astype(bf16)
    return high, (x - high.astype(f32)).astype(bf16)


def invert_leaf(d):
    lane = lax.broadcasted_iota(jnp.int32, (8, LANES), 1)
    sub = lax.broadcasted_iota(jnp.int32, (8, LANES), 0)
    segment = (lane // LEAF) * LEAF
    tiles = LEAF // 8
    rows = [d[8 * t : 8 * t + 8, :] for t in range(tiles)]
    cols = [
        [
            jnp.take_along_axis(rows[t], segment + j, axis=1) if t >= j // 8 else None
            for t in range(tiles)
        ]
        for j in range(LEAF)
    ]
    inverse = [((lane - segment) == (sub + 8 * t)).astype(f32) for t in range(tiles)]
    pivots = [jnp.ones((8, LANES), f32) for _ in range(tiles)]

    def row(v, r):
        return jnp.broadcast_to(v[r : r + 1, :], (8, LANES))

    for j in range(LEAF):
        top, r = j // 8, j % 8
        pivot = row(cols[j][top], r)
        reciprocal = 1.0 / pivot
        pivots[top] = jnp.where(sub == r, pivot, pivots[top])
        scaled = {t: cols[j][t] * reciprocal for t in range(top, tiles)}
        for i in range(j + 1, LEAF):
            factor = row(scaled[i // 8], i % 8)
            for t in range(i // 8, tiles):
                cols[i][t] = cols[i][t] - factor * cols[j][t]
        source = row(inverse[top], r)
        for t in range(top, tiles):
            factor = jnp.where(sub > r, scaled[t], 0.0) if t == top else scaled[t]
            inverse[t] = inverse[t] - factor * source
    return jnp.concatenate([inverse[t] * lax.rsqrt(pivots[t]) for t in range(tiles)], axis=0)


def block_weights(high, low, masks):
    high = jnp.concatenate([high * mask for mask in masks], axis=0)
    low = jnp.concatenate([low * mask for mask in masks], axis=0)
    upper = jnp.concatenate([high, high], axis=1)
    lower = jnp.concatenate([low, jnp.zeros_like(low)], axis=1)
    return jnp.concatenate([upper, lower], axis=0)


def times_transposed(x, weights):
    out = lax.dot_general(x, weights, (((1,), (1,)), ((), ())), preferred_element_type=f32)
    return out[:, :LANES] + out[:, LANES:]


def invert_factor(a_ref, x_ref):
    lane = lax.broadcasted_iota(jnp.int32, (LEAF, LANES), 1)
    sub = lax.broadcasted_iota(jnp.int32, (LEAF, LANES), 0)
    eye = ((lane % LEAF) == sub).astype(f32)
    masks = [((lane // LEAF) == b).astype(f32).astype(bf16) for b in range(BATCH)]

    def weights_of(rows, ks):
        return jnp.concatenate(
            [
                block_weights(
                    x_ref[rows, k * SIZE : k * SIZE + LANES],
                    x_ref[rows, k * SIZE + LANES : (k + 1) * SIZE],
                    masks,
                )
                for k in ks
            ],
            axis=1,
        )

    partial = None
    for j in range(PANELS):
        start = j * LEAF
        block = slice(start, start + LEAF)
        col = a_ref[j]
        if j:
            last = slice((j - 1) * SIZE, j * SIZE)
            if partial is not None:
                col = col - partial
            col = col - times_transposed(x_ref[:, last], weights_of(block, [j - 1]))
            x_ref[block, : j * SIZE] = jnp.zeros((LEAF, j * SIZE), bf16)
            if j < PANELS - 1:
                following = slice(start + LEAF, start + 2 * LEAF)
                partial = times_transposed(
                    x_ref[:, : j * SIZE], weights_of(following, range(j))
                )
        inverse = invert_leaf(col[block])
        col = jnp.concatenate(
            [part for part in (col[:start], eye, col[start + LEAF :]) if part.shape[0]], axis=0
        )
        col = times_transposed(
            jnp.concatenate(split(col), axis=1), block_weights(*split(inverse), masks)
        )
        x_ref[:, j * SIZE : (j + 1) * SIZE] = jnp.concatenate(split(col), axis=1)


UPPER, LOWER = slice(0, SIZE), slice(SIZE, 2 * SIZE)
CONTRACT_ROWS = (((0,), (0,)), ((), ()))


def dot(a, b):
    return jnp.dot(a, b, preferred_element_type=f32)


def lines_of(lane_block, s):
    return pl.ds(2 * lane_block + s, SIZE, stride=4)


def lanes_of(lane_block):
    return slice(lane_block * LANES, (lane_block + 1) * LANES)


def column_of(line):
    return jnp.transpose(jnp.broadcast_to(line, (LANES, SIZE)))


def weigh(t, role, own, got, scale, left, right, wide):
    is_right = role[0] == 1
    q = role[1] - 1 + t
    own_wide = own[jnp.clip(q, 0, 15) - role[2]].astype(f32)
    got_wide = got[...].astype(f32)
    wide[0] = jnp.where(is_right, got_wide, own_wide)
    wide[1] = jnp.where(is_right, own_wide, got_wide)
    left_rows = column_of(scale[0, q + 1])
    right_rows = column_of(scale[1, q + 1])
    for s in range(2):
        col = scale[2, q + s + 1]
        for jb in range(2):
            lines, lanes = lines_of(jb, s), lanes_of(jb)
            left[s, :, lanes] = (wide[0, lines, :] * left_rows).astype(bf16)
            right[s, :, lanes] = ((wide[1, lines, :] * right_rows) * col[:, lanes]).astype(bf16)


def sample(gates, kept, sketch, left, before, right, right_before, right_after, mixed, samp, gram):
    g0, g1, p0, p1, p2 = [gates[i] for i in range(5)]
    mixed[UPPER, UPPER] = (g0 * dot(left[0], right[0])).astype(bf16)
    mixed[UPPER, LOWER] = (p0 * dot(left[0], right[1]) + p2 * dot(left[1], right_after)).astype(bf16)
    mixed[LOWER, UPPER] = (
        p2 * dot(before[0], right_before) + p1 * dot(before[1], right[0])
    ).astype(bf16)
    mixed[LOWER, LOWER] = (g1 * dot(before[1], right[1])).astype(bf16)
    keep = lax.broadcasted_iota(jnp.int32, (1, SIZE), 1) < kept
    sampled = jnp.where(keep, dot(mixed[...], sketch), 0.0)
    high, low = split(sampled)
    samp[0] = high
    samp[1] = low
    shift = 0.01 * jnp.sum(sampled * sampled) / SIZE
    hh = lax.dot_general(high, high, CONTRACT_ROWS, preferred_element_type=f32)
    hl = lax.dot_general(high, low, CONTRACT_ROWS, preferred_element_type=f32)
    rows = lax.broadcasted_iota(jnp.int32, (SIZE, SIZE), 0)
    eye = rows == lax.broadcasted_iota(jnp.int32, (SIZE, SIZE), 1)
    added = jnp.where(keep, 0.0, 1.0) + shift
    gram[...] = (hh + (hl + jnp.transpose(hl))) + jnp.where(eye, added, 0.0)


def rolled(value, segments):
    shift = (segments * LEAF) % LANES
    return pltpu.roll(value, shift, axis=1) if shift else value


def gather_lanes(pieces):
    segment = lax.broadcasted_iota(jnp.int32, (1, LANES), 1) // LEAF
    out = pieces[0]
    for i in range(1, BATCH):
        out = jnp.where(segment == i, pieces[i], out)
    return out


def solve(gram, samp, scaled, a_ref, x_ref):
    for k in range(PANELS):
        rows = slice(k * LEAF, SIZE)
        lanes = lanes_of(k // 4)
        a_ref[k, rows, :] = gather_lanes(
            [rolled(gram[b][rows, lanes], b - k % 4) for b in range(BATCH)]
        )
        if k:
            a_ref[k, : k * LEAF, :] = jnp.zeros((k * LEAF, LANES), f32)

    invert_factor(a_ref, x_ref)

    def factor(b, offset):
        halves = []
        for g in range(2):
            panels = [
                rolled(x_ref[:, k * SIZE + offset : k * SIZE + offset + LANES], k % 4 - b)
                for k in range(4 * g, 4 * g + 4)
            ]
            halves.append(gather_lanes(panels))
        return jnp.concatenate(halves, axis=1)

    for b in range(BATCH):
        high, low = factor(b, 0), factor(b, LANES)
        solved = dot(samp[b][0], high) + (dot(samp[b][0], low) + dot(samp[b][1], high))
        scaled[b] = (solved * 16.0).astype(bf16)


def deliver(role, scaled, mixed, wide, ready, msg, out, sems):
    is_right = role[0] == 1
    copies = []
    for b in range(BATCH):
        right_part = lax.dot_general(
            scaled[b], mixed[b][...], CONTRACT_ROWS, preferred_element_type=f32
        ) * (1.0 / SIZE)
        left_wide, right_wide = wide.at[2 * (b % 2)], wide.at[2 * (b % 2) + 1]
        for s in range(2):
            half = scaled[b, UPPER, :] if s == 0 else scaled[b + 1, LOWER, :]
            for jb in range(2):
                lines = lines_of(jb, s)
                left_wide[lines, :] = half[:, lanes_of(jb)].astype(f32)
                right_wide[lines, :] = right_part[:, lanes_of(2 * s + jb)]
        left_site = left_wide[...]
        right_site = right_wide[...]
        msg[b] = jnp.where(is_right, left_site, right_site).astype(bf16)
        ready[b] = jnp.where(is_right, right_site, left_site).astype(bf16)
        copies.append(pltpu.make_async_copy(ready.at[b], out.at[role[1] + b], sems.at[b]))
        copies[-1].start()
    return copies


def early_kernel(role, gates, kept, own, got_0, got, scale, sketch, *refs):
    mixed, samp, gram, edge, left_w, right_w, wide = refs

    def step(t, loop):
        at = jnp.minimum(t - 2, 2)
        weigh(t, role, own, got.at[at], scale, left_w.at[t], right_w.at[t], wide)
        return loop

    weigh(1, role, own, got_0.at[0], scale, left_w.at[1], right_w.at[1], wide)
    lax.fori_loop(2, 6, step, 0)
    for s in range(2):
        edge[s] = left_w[1, s]
        edge[2 + s] = right_w[1, s]
    edge[4] = right_w[2, 0]
    below = role[1] - 5
    wide[0] = got[2].astype(f32)
    rows = column_of(scale[1, below + 1])
    col = scale[2, below + 2]
    for jb in range(2):
        lanes = lanes_of(jb)
        edge[5, :, lanes] = ((wide[0, lines_of(jb, 1), :] * rows) * col[:, lanes]).astype(bf16)
    for b in range(1, BATCH):
        t = b + 1
        sample(
            gates,
            kept[role[1] + b],
            sketch[b],
            (left_w[t, 0], left_w[t, 1]),
            (left_w[t - 1, 0], left_w[t - 1, 1]),
            (right_w[t, 0], right_w[t, 1]),
            right_w[t - 1, 1],
            right_w[t + 1, 0],
            mixed.at[b - 1],
            samp.at[b - 1],
            gram.at[b - 1],
        )


def first_kernel(role, gates, kept, own, got, scale, sketch, *refs):
    (mixed_e, samp_e, gram_e, edge, msg, out, carry), refs = refs[:7], refs[7:]
    mixed, samp, gram, scaled, a_ref, x_ref, wide, ready, sems = refs
    left, right = carry.at[pl.ds(1, 2)], carry.at[pl.ds(3, 2)]
    weigh(0, role, own, got.at[0], scale, left, right, wide)
    sample(
        gates,
        kept[role[1]],
        sketch[0],
        (edge[0], edge[1]),
        (left[0], left[1]),
        (edge[2], edge[3]),
        right[1],
        edge[4],
        mixed,
        samp,
        gram,
    )
    mixed = [mixed] + [mixed_e.at[b] for b in range(BATCH - 1)]
    samp = [samp] + [samp_e.at[b] for b in range(BATCH - 1)]
    gram = [gram] + [gram_e.at[b] for b in range(BATCH - 1)]
    solve(gram, samp, scaled, a_ref, x_ref)
    scaled[BATCH, LOWER, :] = jnp.zeros((SIZE, SIZE), bf16)
    carry[0] = scaled[0, LOWER, :]
    for copy in deliver(role, scaled, mixed, wide, ready, msg, out, sems):
        copy.wait()


def second_kernel(role, gates, kept, own, got, scale, sketch, *refs):
    (edge, carry, _, msg, out, merge), refs = refs[:6], refs[6:]
    left_w, right_w, mixed, samp, gram, scaled, a_ref, x_ref, wide = refs[:9]
    ready, sems = refs[9:]

    def step(t, loop):
        at = jnp.maximum(t - 1, 0)
        weigh(t, role, own, got.at[at], scale, left_w.at[t], right_w.at[t], wide)
        return loop

    lax.fori_loop(0, 4, step, 0)
    right_w[0, 1] = edge[5]
    for s in range(2):
        left_w[4, s] = carry[1 + s]
        right_w[4, s] = carry[3 + s]
    right_w[5, 0] = edge[2]
    for b in range(BATCH):
        t = b + 1
        sample(
            gates,
            kept[role[1] + b],
            sketch[b],
            (left_w[t, 0], left_w[t, 1]),
            (left_w[b, 0], left_w[b, 1]),
            (right_w[t, 0], right_w[t, 1]),
            right_w[b, 1],
            right_w[t + 1, 0],
            mixed.at[b],
            samp.at[b],
            gram.at[b],
        )
    every = range(BATCH)
    solve([gram.at[b] for b in every], [samp.at[b] for b in every], scaled, a_ref, x_ref)
    scaled[BATCH, LOWER, :] = carry[0]
    copies = deliver(
        role, scaled, [mixed.at[b] for b in every], wide, ready, msg, out, sems
    )
    used = jnp.where(role[0] == 1, 0.0, 1.0)
    for jb in range(2):
        value = scaled[0, LOWER, lanes_of(jb)].astype(f32)
        wide[0, lines_of(jb, 0), :] = jnp.zeros((SIZE, LANES), f32)
        wide[0, lines_of(jb, 1), :] = value * used
    merge[...] = wide[0].astype(bf16)
    for copy in copies:
        copy.wait()


def in_hbm(x):
    return pltpu.with_memory_space_constraint(x, pltpu.HBM)


def shaped(*shape, dtype=bf16):
    return jax.ShapeDtypeStruct(shape, dtype)


def run(kernel, operands, specs, outs, out_specs, scratch, aliases=None, mib=20):
    return pl.pallas_call(
        kernel,
        out_shape=outs,
        in_specs=specs,
        out_specs=out_specs,
        scratch_shapes=scratch,
        input_output_aliases=aliases or {},
        compiler_params=pltpu.CompilerParams(vmem_limit_bytes=mib * 2**20),
        cost_estimate=pl.CostEstimate(
            flops=mib * 500_000_000, bytes_accessed=8_000_000, transcendentals=0
        ),
    )(*operands)


SMEM = pl.BlockSpec(memory_space=pltpu.SMEM)
VMEM = pl.BlockSpec(memory_space=pltpu.VMEM)
HBM = pl.BlockSpec(memory_space=pltpu.HBM)
SECTOR = (4 * SIZE, LANES)


def factor_scratch():
    return [
        pltpu.VMEM((BATCH + 1, 2 * SIZE, SIZE), bf16),
        pltpu.VMEM((PANELS, SIZE, LANES), f32),
        pltpu.VMEM((SIZE, PANELS * SIZE), bf16),
        pltpu.VMEM((4, *SECTOR), f32),
    ]


def sample_shapes(make, *lead):
    return [
        make((*lead, 2 * SIZE, 2 * SIZE), bf16),
        make((*lead, 2, 2 * SIZE, SIZE), bf16),
        make((*lead, SIZE, SIZE), f32),
    ]


def early(role, gates, kept, own, got_0, got, scale, sketch):
    return run(
        early_kernel,
        (role, gates, kept, own, got_0, got, scale, sketch),
        [SMEM] * 3 + [VMEM] * 5,
        sample_shapes(jax.ShapeDtypeStruct, BATCH - 1) + [shaped(6, SIZE, SIZE)],
        [VMEM] * 4,
        [
            pltpu.VMEM((6, 2, SIZE, SIZE), bf16),
            pltpu.VMEM((6, 2, SIZE, SIZE), bf16),
            pltpu.VMEM((2, *SECTOR), f32),
        ],
    )


def first_half(role, gates, kept, own, got, scale, sketch, parts):
    return run(
        first_kernel,
        (role, gates, kept, own, got, scale, sketch, *parts),
        [SMEM] * 3 + [VMEM] * 8,
        [shaped(BATCH, *SECTOR), pltpu.HBM((16, *SECTOR), bf16), shaped(5, SIZE, SIZE)],
        [VMEM, HBM, VMEM],
        sample_shapes(pltpu.VMEM)
        + factor_scratch()
        + [pltpu.VMEM((BATCH, *SECTOR), bf16), pltpu.SemaphoreType.DMA((BATCH,))],
    )


def second_half(role, gates, kept, own, got, scale, sketch, edge, carry, out):
    return run(
        second_kernel,
        (role, gates, kept, own, got, scale, sketch, edge, carry, out),
        [SMEM] * 3 + [VMEM] * 6 + [HBM],
        [shaped(BATCH, *SECTOR), pltpu.HBM((16, *SECTOR), bf16), shaped(*SECTOR)],
        [VMEM, HBM, VMEM],
        [pltpu.VMEM((6, 2, SIZE, SIZE), bf16), pltpu.VMEM((6, 2, SIZE, SIZE), bf16)]
        + sample_shapes(pltpu.VMEM, BATCH)
        + factor_scratch()
        + [
            pltpu.VMEM((BATCH, *SECTOR), bf16),
            pltpu.SemaphoreType.DMA((BATCH,)),
        ],
        aliases={9: 1},
    )


def fetch_kernel(at, own, out, sem):
    copy = pltpu.make_async_copy(own.at[at[0]], out.at[0], sem)
    copy.start()
    copy.wait()


def fetch(at, own):
    return run(
        fetch_kernel,
        (jnp.reshape(at, (1,)), in_hbm(own)),
        [SMEM, HBM],
        [shaped(1, *SECTOR)],
        [VMEM],
        [pltpu.SemaphoreType.DMA],
        mib=1,
    )[0]


def pack_kernel(role, own, out, low, both, sems):
    flag = role[0]
    copies = [
        pltpu.make_async_copy(own.at[7 + 8 * flag], both.at[0], sems.at[0]),
        pltpu.make_async_copy(own.at[7], both.at[1], sems.at[1]),
        pltpu.make_async_copy(own.at[pl.ds(5 + 8 * flag, 2)], out.at[pl.ds(0, 2)], sems.at[2]),
        pltpu.make_async_copy(own.at[3 + 8 * flag], low.at[0], sems.at[3]),
    ]
    for copy in copies:
        copy.start()
    copies[0].wait()
    copies[1].wait()
    is_odd = lax.broadcasted_iota(jnp.int32, SECTOR, 0) % 2 == 1
    out[2] = jnp.where(is_odd, both[1].astype(f32), both[0].astype(f32)).astype(bf16)
    copies[2].wait()
    copies[3].wait()


def pack(role, own):
    return run(
        pack_kernel,
        (role, in_hbm(own)),
        [SMEM, HBM],
        [shaped(3, *SECTOR), shaped(1, *SECTOR)],
        [VMEM] * 2,
        [pltpu.VMEM((2, *SECTOR), bf16), pltpu.SemaphoreType.DMA((4,))],
        mib=2,
    )


def place_kernel(merged, at, block, *refs):
    if merged:
        merge, _, out, last, sems = refs
    else:
        _, out, sems = refs
    count = block.shape[0]
    copies = []
    for b in range(count):
        source = block.at[b]
        if merged and b == count - 1:
            last[...] = block[b] + merge[...]
            source = last
        copies.append(pltpu.make_async_copy(source, out.at[at[0] + b], sems.at[b]))
        copies[-1].start()
    for copy in copies:
        copy.wait()


def place(out, block, at, merge=None):
    smem = pl.BlockSpec(memory_space=pltpu.SMEM)
    vmem = pl.BlockSpec(memory_space=pltpu.VMEM)
    hbm = pl.BlockSpec(memory_space=pltpu.HBM)
    operands = (jnp.reshape(at, (1,)), block) + (() if merge is None else (merge,)) + (out,)
    scratch = [] if merge is None else [pltpu.VMEM(merge.shape, bf16)]
    return pl.pallas_call(
        functools.partial(place_kernel, merge is not None),
        out_shape=pltpu.HBM(out.shape, out.dtype),
        in_specs=[smem] + [vmem] * (len(operands) - 2) + [hbm],
        out_specs=hbm,
        scratch_shapes=scratch + [pltpu.SemaphoreType.DMA((block.shape[0],))],
        input_output_aliases={len(operands) - 1: 0},
        compiler_params=pltpu.CompilerParams(vmem_limit_bytes=8 * 2**20),
        cost_estimate=pl.CostEstimate(flops=1000000, bytes_accessed=2_000_000, transcendentals=0),
        name="place",
    )(*operands)


def to_lines(x):
    n = x.shape[0]
    return x.reshape(n, SIZE, 2, 2, LANES).transpose(0, 1, 3, 2, 4).reshape(n, 4 * SIZE, LANES)


def from_lines(x):
    n = x.shape[0]
    return x.reshape(n, SIZE, 2, 2, LANES).transpose(0, 1, 3, 2, 4).reshape(n, SIZE, 2, SIZE)


def shards(site_tensors, bond_weights, sector_sizes, kept_ranks, sketches, gate_ends, gate_pair):
    chain = lax.axis_size("chain")
    count = lax.axis_size("group") * chain
    site = lax.axis_index("group") * chain + lax.axis_index("chain")
    is_right = site % 2 == 1

    def swapped(value):
        return lax.ppermute(value, "chain", [(i, i ^ 1) for i in range(chain)])

    def onward(value, by):
        def place(n):
            return n % chain * (count // chain) + n // chain

        pairs = [(place(i), place(i + by)) for i in range(1, count, 2) if i + by < count]
        return lax.ppermute(value, ("chain", "group"), pairs)

    own = to_lines(site_tensors[0, 0])
    sectors = own.shape[0]
    flag = is_right.astype(jnp.int32)

    def window(array, start, size):
        return lax.dynamic_slice_in_dim(array, start, size, 0)

    got_0 = swapped(fetch(4 + 8 * flag, own))
    outgoing, outgoing_low = pack(jnp.reshape(flag, (1,)), own)
    got_a = swapped(outgoing)
    got_low = swapped(outgoing_low)

    column = lax.broadcasted_iota(jnp.int32, (sectors, SIZE), 1)
    lam = bond_weights[0, 0] * (column < sector_sizes[0, 0][:, None]).astype(f32)
    kept_line = jnp.pad(kept_ranks[0, 0].astype(f32)[None, :], ((0, 7), (0, SIZE - sectors)))
    packed = jnp.concatenate([lam, kept_line], axis=0)
    other = swapped(packed)
    before_left = onward(lam, 1)
    before_right = onward(lam, 2)
    got_b = swapped(window(own, 8 * flag, 3))

    lam_prev = jnp.where(is_right, before_right, before_left)
    lam_prev = jnp.where(site < 2, jnp.ones_like(lam), lam_prev)
    lam_mid = jnp.where(is_right, other[:sectors], lam)
    lam_next = jnp.where(is_right, lam, other[:sectors])
    scale = jnp.pad(jnp.stack([lam_prev, lam_mid, lam_next]), ((0, 0), (1, 7), (0, 0)))
    scale = scale[:, :, None, :]
    kept = jnp.where(is_right, other[sectors, :sectors], packed[sectors, :sectors]).astype(jnp.int32)
    gates = jnp.concatenate([gate_ends, 1.0 + gate_pair[:2], gate_pair[2:]])
    first_a = 12 - 8 * flag
    first_b = 8 - 8 * flag
    own_a = 10 - 7 * flag
    own_b = 7 - 7 * flag
    role_a = jnp.stack([flag, first_a, own_a])
    role_b = jnp.stack([flag, first_b, own_b])

    own_win = window(own, own_a, 6)
    sketch_win = window(sketches, first_a, BATCH)
    parts = early(role_a, gates, kept, own_win, got_0, got_a, scale, sketch_win)
    msg_a, out, carry = first_half(
        role_a, gates, kept, own_win, got_low, scale, sketch_win, parts
    )
    back_a = swapped(msg_a)
    own_win = window(own, own_b, BATCH)
    sketch_win = window(sketches, first_b, BATCH)
    msg_b, out, merge = second_half(
        role_b, gates, kept, own_win, got_b, scale, sketch_win, parts[3], carry, out
    )
    back_b = swapped(msg_b)

    back_at = 8 * flag
    out = place(out, back_a, back_at + 4, merge)
    out = place(out, back_b, back_at)
    return from_lines(out)[None, None]


def solution(mesh):
    return jax.shard_map(
        shards,
        mesh=mesh,
        in_specs=(
            P("group", "chain", None, None, None, None),
            P("group", "chain", None, None),
            P("group", "chain", None),
            P("group", "chain", None),
            P(),
            P(),
            P(),
        ),
        out_specs=P("group", "chain", None, None, None, None),
        check_vma=False,
    )
```

```python
import functools

import jax
import jax.numpy as jnp
from jax import lax
from jax.experimental import pallas as pl
from jax.experimental.pallas import tpu as pltpu
from jax.sharding import PartitionSpec as P

f32 = jnp.float32
bf16 = jnp.bfloat16


BATCH = 4
LEAF = 32
PANELS = 8
LANES = 128
SIZE = 256


def split(x):
    high = x.astype(bf16)
    return high, (x - high.astype(f32)).astype(bf16)


def invert_leaf(d):
    lane = lax.broadcasted_iota(jnp.int32, (8, LANES), 1)
    sub = lax.broadcasted_iota(jnp.int32, (8, LANES), 0)
    segment = (lane // LEAF) * LEAF
    tiles = LEAF // 8
    rows = [d[8 * t : 8 * t + 8, :] for t in range(tiles)]
    cols = [
        [
            jnp.take_along_axis(rows[t], segment + j, axis=1) if t >= j // 8 else None
            for t in range(tiles)
        ]
        for j in range(LEAF)
    ]
    inverse = [((lane - segment) == (sub + 8 * t)).astype(f32) for t in range(tiles)]
    pivots = [jnp.ones((8, LANES), f32) for _ in range(tiles)]

    def row(v, r):
        return jnp.broadcast_to(v[r : r + 1, :], (8, LANES))

    for j in range(LEAF):
        top, r = j // 8, j % 8
        pivot = row(cols[j][top], r)
        reciprocal = 1.0 / pivot
        pivots[top] = jnp.where(sub == r, pivot, pivots[top])
        scaled = {t: cols[j][t] * reciprocal for t in range(top, tiles)}
        for i in range(j + 1, LEAF):
            factor = row(scaled[i // 8], i % 8)
            for t in range(i // 8, tiles):
                cols[i][t] = cols[i][t] - factor * cols[j][t]
        source = row(inverse[top], r)
        for t in range(top, tiles):
            factor = jnp.where(sub > r, scaled[t], 0.0) if t == top else scaled[t]
            inverse[t] = inverse[t] - factor * source
    return jnp.concatenate([inverse[t] * lax.rsqrt(pivots[t]) for t in range(tiles)], axis=0)


def block_weights(high, low, masks):
    high = jnp.concatenate([high * mask for mask in masks], axis=0)
    low = jnp.concatenate([low * mask for mask in masks], axis=0)
    upper = jnp.concatenate([high, high], axis=1)
    lower = jnp.concatenate([low, jnp.zeros_like(low)], axis=1)
    return jnp.concatenate([upper, lower], axis=0)


def times_transposed(x, weights):
    out = lax.dot_general(x, weights, (((1,), (1,)), ((), ())), preferred_element_type=f32)
    return out[:, :LANES] + out[:, LANES:]


def invert_factor(a_ref, x_ref):
    lane = lax.broadcasted_iota(jnp.int32, (LEAF, LANES), 1)
    sub = lax.broadcasted_iota(jnp.int32, (LEAF, LANES), 0)
    eye = ((lane % LEAF) == sub).astype(f32)
    masks = [((lane // LEAF) == b).astype(f32).astype(bf16) for b in range(BATCH)]

    def weights_of(rows, ks):
        return jnp.concatenate(
            [
                block_weights(
                    x_ref[rows, k * SIZE : k * SIZE + LANES],
                    x_ref[rows, k * SIZE + LANES : (k + 1) * SIZE],
                    masks,
                )
                for k in ks
            ],
            axis=1,
        )

    partial = None
    for j in range(PANELS):
        start = j * LEAF
        block = slice(start, start + LEAF)
        col = a_ref[j]
        if j:
            last = slice((j - 1) * SIZE, j * SIZE)
            if partial is not None:
                col = col - partial
            col = col - times_transposed(x_ref[:, last], weights_of(block, [j - 1]))
            x_ref[block, : j * SIZE] = jnp.zeros((LEAF, j * SIZE), bf16)
            if j < PANELS - 1:
                following = slice(start + LEAF, start + 2 * LEAF)
                partial = times_transposed(
                    x_ref[:, : j * SIZE], weights_of(following, range(j))
                )
        inverse = invert_leaf(col[block])
        col = jnp.concatenate(
            [part for part in (col[:start], eye, col[start + LEAF :]) if part.shape[0]], axis=0
        )
        col = times_transposed(
            jnp.concatenate(split(col), axis=1), block_weights(*split(inverse), masks)
        )
        x_ref[:, j * SIZE : (j + 1) * SIZE] = jnp.concatenate(split(col), axis=1)


UPPER, LOWER = slice(0, SIZE), slice(SIZE, 2 * SIZE)
CONTRACT_ROWS = (((0,), (0,)), ((), ()))


def dot(a, b):
    return jnp.dot(a, b, preferred_element_type=f32)


def lines_of(lane_block, s):
    return pl.ds(2 * lane_block + s, SIZE, stride=4)


def lanes_of(lane_block):
    return slice(lane_block * LANES, (lane_block + 1) * LANES)


def column_of(line):
    return jnp.transpose(jnp.broadcast_to(line, (LANES, SIZE)))


def weigh(t, role, own, got, scale, left, right, wide):
    is_right = role[0] == 1
    q = role[1] - 1 + t
    own_wide = own[jnp.clip(q, 0, 15) - role[2]].astype(f32)
    got_wide = got[...].astype(f32)
    wide[0] = jnp.where(is_right, got_wide, own_wide)
    wide[1] = jnp.where(is_right, own_wide, got_wide)
    left_rows = column_of(scale[0, q + 1])
    right_rows = column_of(scale[1, q + 1])
    for s in range(2):
        col = scale[2, q + s + 1]
        for jb in range(2):
            lines, lanes = lines_of(jb, s), lanes_of(jb)
            left[s, :, lanes] = (wide[0, lines, :] * left_rows).astype(bf16)
            right[s, :, lanes] = ((wide[1, lines, :] * right_rows) * col[:, lanes]).astype(bf16)


def sample(gates, kept, sketch, left, before, right, right_before, right_after, mixed, samp, gram):
    g0, g1, p0, p1, p2 = [gates[i] for i in range(5)]
    mixed[UPPER, UPPER] = (g0 * dot(left[0], right[0])).astype(bf16)
    mixed[UPPER, LOWER] = (p0 * dot(left[0], right[1]) + p2 * dot(left[1], right_after)).astype(bf16)
    mixed[LOWER, UPPER] = (
        p2 * dot(before[0], right_before) + p1 * dot(before[1], right[0])
    ).astype(bf16)
    mixed[LOWER, LOWER] = (g1 * dot(before[1], right[1])).astype(bf16)
    keep = lax.broadcasted_iota(jnp.int32, (1, SIZE), 1) < kept
    sampled = jnp.where(keep, dot(mixed[...], sketch), 0.0)
    high, low = split(sampled)
    samp[0] = high
    samp[1] = low
    shift = 0.01 * jnp.sum(sampled * sampled) / SIZE
    hh = lax.dot_general(high, high, CONTRACT_ROWS, preferred_element_type=f32)
    hl = lax.dot_general(high, low, CONTRACT_ROWS, preferred_element_type=f32)
    rows = lax.broadcasted_iota(jnp.int32, (SIZE, SIZE), 0)
    eye = rows == lax.broadcasted_iota(jnp.int32, (SIZE, SIZE), 1)
    added = jnp.where(keep, 0.0, 1.0) + shift
    gram[...] = (hh + (hl + jnp.transpose(hl))) + jnp.where(eye, added, 0.0)


def rolled(value, segments):
    shift = (segments * LEAF) % LANES
    return pltpu.roll(value, shift, axis=1) if shift else value


def gather_lanes(pieces):
    segment = lax.broadcasted_iota(jnp.int32, (1, LANES), 1) // LEAF
    out = pieces[0]
    for i in range(1, BATCH):
        out = jnp.where(segment == i, pieces[i], out)
    return out


def solve(gram, samp, scaled, a_ref, x_ref):
    for k in range(PANELS):
        rows = slice(k * LEAF, SIZE)
        lanes = lanes_of(k // 4)
        a_ref[k, rows, :] = gather_lanes(
            [rolled(gram[b][rows, lanes], b - k % 4) for b in range(BATCH)]
        )
        if k:
            a_ref[k, : k * LEAF, :] = jnp.zeros((k * LEAF, LANES), f32)

    invert_factor(a_ref, x_ref)

    def factor(b, offset):
        halves = []
        for g in range(2):
            panels = [
                rolled(x_ref[:, k * SIZE + offset : k * SIZE + offset + LANES], k % 4 - b)
                for k in range(4 * g, 4 * g + 4)
            ]
            halves.append(gather_lanes(panels))
        return jnp.concatenate(halves, axis=1)

    for b in range(BATCH):
        high, low = factor(b, 0), factor(b, LANES)
        solved = dot(samp[b][0], high) + (dot(samp[b][0], low) + dot(samp[b][1], high))
        scaled[b] = (solved * 16.0).astype(bf16)


def deliver(role, scaled, mixed, wide, ready, msg, out, sems):
    is_right = role[0] == 1
    copies = []
    for b in range(BATCH):
        right_part = lax.dot_general(
            scaled[b], mixed[b][...], CONTRACT_ROWS, preferred_element_type=f32
        ) * (1.0 / SIZE)
        left_wide, right_wide = wide.at[2 * (b % 2)], wide.at[2 * (b % 2) + 1]
        for s in range(2):
            half = scaled[b, UPPER, :] if s == 0 else scaled[b + 1, LOWER, :]
            for jb in range(2):
                lines = lines_of(jb, s)
                left_wide[lines, :] = half[:, lanes_of(jb)].astype(f32)
                right_wide[lines, :] = right_part[:, lanes_of(2 * s + jb)]
        left_site = left_wide[...]
        right_site = right_wide[...]
        msg[b] = jnp.where(is_right, left_site, right_site).astype(bf16)
        ready[b] = jnp.where(is_right, right_site, left_site).astype(bf16)
        copies.append(pltpu.make_async_copy(ready.at[b], out.at[role[1] + b], sems.at[b]))
        copies[-1].start()
    return copies


def early_kernel(role, gates, kept, own, got_0, got, scale, sketch, *refs):
    mixed, samp, gram, edge, left_w, right_w, wide = refs

    def step(t, loop):
        at = jnp.minimum(t - 3, 1)
        weigh(t, role, own, got.at[at], scale, left_w.at[t], right_w.at[t], wide)
        return loop

    def step_0(t, loop):
        weigh(t, role, own, got_0.at[t - 1], scale, left_w.at[t], right_w.at[t], wide)
        return loop

    lax.fori_loop(1, 3, step_0, 0)
    lax.fori_loop(3, 6, step, 0)
    for s in range(2):
        edge[s] = left_w[1, s]
        edge[2 + s] = right_w[1, s]
    edge[4] = right_w[2, 0]
    below = role[1] - 5
    wide[0] = got[1].astype(f32)
    rows = column_of(scale[1, below + 1])
    col = scale[2, below + 2]
    for jb in range(2):
        lanes = lanes_of(jb)
        edge[5, :, lanes] = ((wide[0, lines_of(jb, 1), :] * rows) * col[:, lanes]).astype(bf16)
    for b in range(1, BATCH):
        t = b + 1
        sample(
            gates,
            kept[role[1] + b],
            sketch[b],
            (left_w[t, 0], left_w[t, 1]),
            (left_w[t - 1, 0], left_w[t - 1, 1]),
            (right_w[t, 0], right_w[t, 1]),
            right_w[t - 1, 1],
            right_w[t + 1, 0],
            mixed.at[b - 1],
            samp.at[b - 1],
            gram.at[b - 1],
        )


def first_kernel(role, gates, kept, own, got, scale, sketch, *refs):
    (mixed_e, samp_e, gram_e, edge, msg, out, carry), refs = refs[:7], refs[7:]
    mixed, samp, gram, scaled, a_ref, x_ref, wide, ready, sems = refs
    left, right = carry.at[pl.ds(1, 2)], carry.at[pl.ds(3, 2)]
    weigh(0, role, own, got.at[0], scale, left, right, wide)
    sample(
        gates,
        kept[role[1]],
        sketch[0],
        (edge[0], edge[1]),
        (left[0], left[1]),
        (edge[2], edge[3]),
        right[1],
        edge[4],
        mixed,
        samp,
        gram,
    )
    mixed = [mixed] + [mixed_e.at[b] for b in range(BATCH - 1)]
    samp = [samp] + [samp_e.at[b] for b in range(BATCH - 1)]
    gram = [gram] + [gram_e.at[b] for b in range(BATCH - 1)]
    solve(gram, samp, scaled, a_ref, x_ref)
    scaled[BATCH, LOWER, :] = jnp.zeros((SIZE, SIZE), bf16)
    carry[0] = scaled[0, LOWER, :]
    for copy in deliver(role, scaled, mixed, wide, ready, msg, out, sems):
        copy.wait()


def second_kernel(role, gates, kept, own, got, scale, sketch, *refs):
    (edge, carry, _, msg, out, merge), refs = refs[:6], refs[6:]
    left_w, right_w, mixed, samp, gram, scaled, a_ref, x_ref, wide = refs[:9]
    ready, sems = refs[9:]

    def step(t, loop):
        at = jnp.maximum(t - 1, 0)
        weigh(t, role, own, got.at[at], scale, left_w.at[t], right_w.at[t], wide)
        return loop

    lax.fori_loop(0, 4, step, 0)
    right_w[0, 1] = edge[5]
    for s in range(2):
        left_w[4, s] = carry[1 + s]
        right_w[4, s] = carry[3 + s]
    right_w[5, 0] = edge[2]
    for b in range(BATCH):
        t = b + 1
        sample(
            gates,
            kept[role[1] + b],
            sketch[b],
            (left_w[t, 0], left_w[t, 1]),
            (left_w[b, 0], left_w[b, 1]),
            (right_w[t, 0], right_w[t, 1]),
            right_w[b, 1],
            right_w[t + 1, 0],
            mixed.at[b],
            samp.at[b],
            gram.at[b],
        )
    every = range(BATCH)
    solve([gram.at[b] for b in every], [samp.at[b] for b in every], scaled, a_ref, x_ref)
    scaled[BATCH, LOWER, :] = carry[0]
    copies = deliver(
        role, scaled, [mixed.at[b] for b in every], wide, ready, msg, out, sems
    )
    used = jnp.where(role[0] == 1, 0.0, 1.0)
    for jb in range(2):
        value = scaled[0, LOWER, lanes_of(jb)].astype(f32)
        wide[0, lines_of(jb, 0), :] = jnp.zeros((SIZE, LANES), f32)
        wide[0, lines_of(jb, 1), :] = value * used
    merge[...] = wide[0].astype(bf16)
    for copy in copies:
        copy.wait()


def in_hbm(x):
    return pltpu.with_memory_space_constraint(x, pltpu.HBM)


def shaped(*shape, dtype=bf16):
    return jax.ShapeDtypeStruct(shape, dtype)


def run(kernel, operands, specs, outs, out_specs, scratch, aliases=None, mib=20):
    return pl.pallas_call(
        kernel,
        out_shape=outs,
        in_specs=specs,
        out_specs=out_specs,
        scratch_shapes=scratch,
        input_output_aliases=aliases or {},
        compiler_params=pltpu.CompilerParams(vmem_limit_bytes=mib * 2**20),
        cost_estimate=pl.CostEstimate(
            flops=mib * 500_000_000, bytes_accessed=8_000_000, transcendentals=0
        ),
    )(*operands)


SMEM = pl.BlockSpec(memory_space=pltpu.SMEM)
VMEM = pl.BlockSpec(memory_space=pltpu.VMEM)
HBM = pl.BlockSpec(memory_space=pltpu.HBM)
SECTOR = (4 * SIZE, LANES)


def factor_scratch():
    return [
        pltpu.VMEM((BATCH + 1, 2 * SIZE, SIZE), bf16),
        pltpu.VMEM((PANELS, SIZE, LANES), f32),
        pltpu.VMEM((SIZE, PANELS * SIZE), bf16),
        pltpu.VMEM((4, *SECTOR), f32),
    ]


def sample_shapes(make, *lead):
    return [
        make((*lead, 2 * SIZE, 2 * SIZE), bf16),
        make((*lead, 2, 2 * SIZE, SIZE), bf16),
        make((*lead, SIZE, SIZE), f32),
    ]


def early(role, gates, kept, own, got_0, got, scale, sketch):
    return run(
        early_kernel,
        (role, gates, kept, own, got_0, got, scale, sketch),
        [SMEM] * 3 + [VMEM] * 5,
        sample_shapes(jax.ShapeDtypeStruct, BATCH - 1) + [shaped(6, SIZE, SIZE)],
        [VMEM] * 4,
        [
            pltpu.VMEM((6, 2, SIZE, SIZE), bf16),
            pltpu.VMEM((6, 2, SIZE, SIZE), bf16),
            pltpu.VMEM((2, *SECTOR), f32),
        ],
    )


def first_half(role, gates, kept, own, got, scale, sketch, parts):
    return run(
        first_kernel,
        (role, gates, kept, own, got, scale, sketch, *parts),
        [SMEM] * 3 + [VMEM] * 8,
        [shaped(BATCH, *SECTOR), pltpu.HBM((16, *SECTOR), bf16), shaped(5, SIZE, SIZE)],
        [VMEM, HBM, VMEM],
        sample_shapes(pltpu.VMEM)
        + factor_scratch()
        + [pltpu.VMEM((BATCH, *SECTOR), bf16), pltpu.SemaphoreType.DMA((BATCH,))],
    )


def second_half(role, gates, kept, own, got, scale, sketch, edge, carry, out):
    return run(
        second_kernel,
        (role, gates, kept, own, got, scale, sketch, edge, carry, out),
        [SMEM] * 3 + [VMEM] * 6 + [HBM],
        [shaped(BATCH, *SECTOR), pltpu.HBM((16, *SECTOR), bf16), shaped(*SECTOR)],
        [VMEM, HBM, VMEM],
        [pltpu.VMEM((6, 2, SIZE, SIZE), bf16), pltpu.VMEM((6, 2, SIZE, SIZE), bf16)]
        + sample_shapes(pltpu.VMEM, BATCH)
        + factor_scratch()
        + [
            pltpu.VMEM((BATCH, *SECTOR), bf16),
            pltpu.SemaphoreType.DMA((BATCH,)),
        ],
        aliases={9: 1},
    )


def fetch_kernel(at, own, out, sem):
    copy = pltpu.make_async_copy(own.at[pl.ds(at[0], out.shape[0])], out, sem)
    copy.start()
    copy.wait()


def fetch(at, own):
    return run(
        fetch_kernel,
        (jnp.reshape(at, (1,)), in_hbm(own)),
        [SMEM, HBM],
        [shaped(2, *SECTOR)],
        [VMEM],
        [pltpu.SemaphoreType.DMA],
        mib=1,
    )[0]


def pack_kernel(role, own, out, low, both, sems):
    flag = role[0]
    copies = [
        pltpu.make_async_copy(own.at[7 + 8 * flag], both.at[0], sems.at[0]),
        pltpu.make_async_copy(own.at[7], both.at[1], sems.at[1]),
        pltpu.make_async_copy(own.at[6 + 8 * flag], out.at[0], sems.at[2]),
        pltpu.make_async_copy(own.at[3 + 8 * flag], low.at[0], sems.at[3]),
    ]
    for copy in copies:
        copy.start()
    copies[0].wait()
    copies[1].wait()
    is_odd = lax.broadcasted_iota(jnp.int32, SECTOR, 0) % 2 == 1
    out[1] = jnp.where(is_odd, both[1].astype(f32), both[0].astype(f32)).astype(bf16)
    copies[2].wait()
    copies[3].wait()


def pack(role, own):
    return run(
        pack_kernel,
        (role, in_hbm(own)),
        [SMEM, HBM],
        [shaped(2, *SECTOR), shaped(1, *SECTOR)],
        [VMEM] * 2,
        [pltpu.VMEM((2, *SECTOR), bf16), pltpu.SemaphoreType.DMA((4,))],
        mib=2,
    )


def place_kernel(merged, at, block, *refs):
    if merged:
        merge, _, out, last, sems = refs
    else:
        _, out, sems = refs
    count = block.shape[0]
    copies = []
    for b in range(count):
        source = block.at[b]
        if merged and b == count - 1:
            last[...] = block[b] + merge[...]
            source = last
        copies.append(pltpu.make_async_copy(source, out.at[at[0] + b], sems.at[b]))
        copies[-1].start()
    for copy in copies:
        copy.wait()


def place(out, block, at, merge=None):
    smem = pl.BlockSpec(memory_space=pltpu.SMEM)
    vmem = pl.BlockSpec(memory_space=pltpu.VMEM)
    hbm = pl.BlockSpec(memory_space=pltpu.HBM)
    operands = (jnp.reshape(at, (1,)), block) + (() if merge is None else (merge,)) + (out,)
    scratch = [] if merge is None else [pltpu.VMEM(merge.shape, bf16)]
    return pl.pallas_call(
        functools.partial(place_kernel, merge is not None),
        out_shape=pltpu.HBM(out.shape, out.dtype),
        in_specs=[smem] + [vmem] * (len(operands) - 2) + [hbm],
        out_specs=hbm,
        scratch_shapes=scratch + [pltpu.SemaphoreType.DMA((block.shape[0],))],
        input_output_aliases={len(operands) - 1: 0},
        compiler_params=pltpu.CompilerParams(vmem_limit_bytes=8 * 2**20),
        cost_estimate=pl.CostEstimate(flops=1000000, bytes_accessed=2_000_000, transcendentals=0),
        name="place",
    )(*operands)


def to_lines(x):
    n = x.shape[0]
    return x.reshape(n, SIZE, 2, 2, LANES).transpose(0, 1, 3, 2, 4).reshape(n, 4 * SIZE, LANES)


def from_lines(x):
    n = x.shape[0]
    return x.reshape(n, SIZE, 2, 2, LANES).transpose(0, 1, 3, 2, 4).reshape(n, SIZE, 2, SIZE)


def shards(site_tensors, bond_weights, sector_sizes, kept_ranks, sketches, gate_ends, gate_pair):
    chain = lax.axis_size("chain")
    count = lax.axis_size("group") * chain
    site = lax.axis_index("group") * chain + lax.axis_index("chain")
    is_right = site % 2 == 1

    def swapped(value):
        return lax.ppermute(value, "chain", [(i, i ^ 1) for i in range(chain)])

    def onward(value):
        def place(n):
            return n % chain * (count // chain) + n // chain

        pairs = [(place(i), place(i + 1)) for i in range(1, count - 1, 2)]
        return lax.ppermute(value, ("chain", "group"), pairs)

    own = to_lines(site_tensors[0, 0])
    sectors = own.shape[0]
    flag = is_right.astype(jnp.int32)

    def window(array, start, size):
        return lax.dynamic_slice_in_dim(array, start, size, 0)

    got_0 = swapped(fetch(4 + 8 * flag, own))
    column = lax.broadcasted_iota(jnp.int32, (sectors, SIZE), 1)
    lam = bond_weights[0, 0] * (column < sector_sizes[0, 0][:, None]).astype(f32)
    before = onward(lam)
    before = jnp.where(site < 2, jnp.ones_like(lam), before)
    kept_line = jnp.pad(kept_ranks[0, 0].astype(f32)[None, :], ((0, 7), (0, SIZE - sectors)))
    packed = jnp.concatenate([lam, before, kept_line], axis=0)
    other = swapped(packed)
    outgoing, outgoing_low = pack(jnp.reshape(flag, (1,)), own)
    got_a = swapped(outgoing)
    got_low = swapped(outgoing_low)
    lam_prev = jnp.where(is_right, other[sectors : 2 * sectors], before)
    lam_mid = jnp.where(is_right, other[:sectors], lam)
    lam_next = jnp.where(is_right, lam, other[:sectors])
    scale = jnp.pad(jnp.stack([lam_prev, lam_mid, lam_next]), ((0, 0), (1, 7), (0, 0)))
    scale = scale[:, :, None, :]
    kept = jnp.where(is_right, other[2 * sectors, :sectors], packed[2 * sectors, :sectors])
    kept = kept.astype(jnp.int32)
    late = jnp.minimum(kept[0], 0)
    got_b = swapped(window(own, 8 * flag + late, 3))
    gates = jnp.concatenate([gate_ends, 1.0 + gate_pair[:2], gate_pair[2:]])
    first_a = 12 - 8 * flag
    first_b = 8 - 8 * flag
    own_a = 10 - 7 * flag
    own_b = 7 - 7 * flag
    role_a = jnp.stack([flag, first_a, own_a])
    role_b = jnp.stack([flag, first_b, own_b])

    own_win = window(own, own_a + late, 6)
    sketch_win = window(sketches, first_a + late, BATCH)
    parts = early(role_a, gates, kept, own_win, got_0, got_a, scale, sketch_win)
    msg_a, out, carry = first_half(
        role_a, gates, kept, own_win, got_low, scale, sketch_win, parts
    )
    back_a = swapped(msg_a)
    own_win = window(own, own_b + late, BATCH)
    sketch_win = window(sketches, first_b + late, BATCH)
    msg_b, out, merge = second_half(
        role_b, gates, kept, own_win, got_b, scale, sketch_win, parts[3], carry, out
    )
    back_b = swapped(msg_b)

    back_at = 8 * flag
    out = place(out, back_a, back_at + 4, merge)
    out = place(out, back_b, back_at)
    return from_lines(out)[None, None]


def solution(mesh):
    return jax.shard_map(
        shards,
        mesh=mesh,
        in_specs=(
            P("group", "chain", None, None, None, None),
            P("group", "chain", None, None),
            P("group", "chain", None),
            P("group", "chain", None),
            P(),
            P(),
            P(),
        ),
        out_specs=P("group", "chain", None, None, None, None),
        check_vma=False,
    )
```

```python
import functools

import jax
import jax.numpy as jnp
from jax import lax
from jax.experimental import pallas as pl
from jax.experimental.pallas import tpu as pltpu
from jax.sharding import PartitionSpec as P

f32 = jnp.float32
bf16 = jnp.bfloat16


BATCH = 4
LEAF = 32
PANELS = 8
LANES = 128
SIZE = 256


def split(x):
    high = x.astype(bf16)
    return high, (x - high.astype(f32)).astype(bf16)


def invert_leaf(d):
    lane = lax.broadcasted_iota(jnp.int32, (8, LANES), 1)
    sub = lax.broadcasted_iota(jnp.int32, (8, LANES), 0)
    segment = (lane // LEAF) * LEAF
    tiles = LEAF // 8
    rows = [d[8 * t : 8 * t + 8, :] for t in range(tiles)]
    cols = [
        [
            jnp.take_along_axis(rows[t], segment + j, axis=1) if t >= j // 8 else None
            for t in range(tiles)
        ]
        for j in range(LEAF)
    ]
    inverse = [((lane - segment) == (sub + 8 * t)).astype(f32) for t in range(tiles)]
    pivots = [jnp.ones((8, LANES), f32) for _ in range(tiles)]

    def row(v, r):
        return jnp.broadcast_to(v[r : r + 1, :], (8, LANES))

    for j in range(LEAF):
        top, r = j // 8, j % 8
        pivot = row(cols[j][top], r)
        reciprocal = 1.0 / pivot
        pivots[top] = jnp.where(sub == r, pivot, pivots[top])
        scaled = {t: cols[j][t] * reciprocal for t in range(top, tiles)}
        for i in range(j + 1, LEAF):
            factor = row(scaled[i // 8], i % 8)
            for t in range(i // 8, tiles):
                cols[i][t] = cols[i][t] - factor * cols[j][t]
        source = row(inverse[top], r)
        for t in range(top, tiles):
            factor = jnp.where(sub > r, scaled[t], 0.0) if t == top else scaled[t]
            inverse[t] = inverse[t] - factor * source
    return jnp.concatenate([inverse[t] * lax.rsqrt(pivots[t]) for t in range(tiles)], axis=0)


def block_weights(high, low, masks):
    high = jnp.concatenate([high * mask for mask in masks], axis=0)
    low = jnp.concatenate([low * mask for mask in masks], axis=0)
    upper = jnp.concatenate([high, high], axis=1)
    lower = jnp.concatenate([low, jnp.zeros_like(low)], axis=1)
    return jnp.concatenate([upper, lower], axis=0)


def times_transposed(x, weights):
    out = lax.dot_general(x, weights, (((1,), (1,)), ((), ())), preferred_element_type=f32)
    return out[:, :LANES] + out[:, LANES:]


def invert_factor(a_ref, x_ref):
    lane = lax.broadcasted_iota(jnp.int32, (LEAF, LANES), 1)
    sub = lax.broadcasted_iota(jnp.int32, (LEAF, LANES), 0)
    eye = ((lane % LEAF) == sub).astype(f32)
    masks = [((lane // LEAF) == b).astype(f32).astype(bf16) for b in range(BATCH)]

    def weights_of(rows, ks):
        return jnp.concatenate(
            [
                block_weights(
                    x_ref[rows, k * SIZE : k * SIZE + LANES],
                    x_ref[rows, k * SIZE + LANES : (k + 1) * SIZE],
                    masks,
                )
                for k in ks
            ],
            axis=1,
        )

    partial = None
    for j in range(PANELS):
        start = j * LEAF
        block = slice(start, start + LEAF)
        col = a_ref[j]
        if j:
            last = slice((j - 1) * SIZE, j * SIZE)
            if partial is not None:
                col = col - partial
            col = col - times_transposed(x_ref[:, last], weights_of(block, [j - 1]))
            x_ref[block, : j * SIZE] = jnp.zeros((LEAF, j * SIZE), bf16)
            if j < PANELS - 1:
                following = slice(start + LEAF, start + 2 * LEAF)
                partial = times_transposed(
                    x_ref[:, : j * SIZE], weights_of(following, range(j))
                )
        inverse = invert_leaf(col[block])
        col = jnp.concatenate(
            [part for part in (col[:start], eye, col[start + LEAF :]) if part.shape[0]], axis=0
        )
        col = times_transposed(
            jnp.concatenate(split(col), axis=1), block_weights(*split(inverse), masks)
        )
        x_ref[:, j * SIZE : (j + 1) * SIZE] = jnp.concatenate(split(col), axis=1)


UPPER, LOWER = slice(0, SIZE), slice(SIZE, 2 * SIZE)
CONTRACT_ROWS = (((0,), (0,)), ((), ()))


def dot(a, b):
    return jnp.dot(a, b, preferred_element_type=f32)


def lines_of(lane_block, s):
    return pl.ds(2 * lane_block + s, SIZE, stride=4)


def lanes_of(lane_block):
    return slice(lane_block * LANES, (lane_block + 1) * LANES)


def column_of(line):
    return jnp.transpose(jnp.broadcast_to(line, (LANES, SIZE)))


def weigh(t, role, own, got, scale, left, right, wide):
    is_right = role[0] == 1
    q = role[1] - 1 + t
    own_wide = own[jnp.clip(q, 0, 15) - role[2]].astype(f32)
    got_wide = got[...].astype(f32)
    wide[0] = jnp.where(is_right, got_wide, own_wide)
    wide[1] = jnp.where(is_right, own_wide, got_wide)
    left_rows = column_of(scale[0, q + 1])
    right_rows = column_of(scale[1, q + 1])
    for s in range(2):
        col = scale[2, q + s + 1]
        for jb in range(2):
            lines, lanes = lines_of(jb, s), lanes_of(jb)
            left[s, :, lanes] = (wide[0, lines, :] * left_rows).astype(bf16)
            right[s, :, lanes] = ((wide[1, lines, :] * right_rows) * col[:, lanes]).astype(bf16)


def sample(gates, kept, sketch, left, before, right, right_before, right_after, mixed, samp, gram):
    g0, g1, p0, p1, p2 = [gates[i] for i in range(5)]
    mixed[UPPER, UPPER] = (g0 * dot(left[0], right[0])).astype(bf16)
    mixed[UPPER, LOWER] = (p0 * dot(left[0], right[1]) + p2 * dot(left[1], right_after)).astype(bf16)
    mixed[LOWER, UPPER] = (
        p2 * dot(before[0], right_before) + p1 * dot(before[1], right[0])
    ).astype(bf16)
    mixed[LOWER, LOWER] = (g1 * dot(before[1], right[1])).astype(bf16)
    keep = lax.broadcasted_iota(jnp.int32, (1, SIZE), 1) < kept
    sampled = jnp.where(keep, dot(mixed[...], sketch), 0.0)
    high, low = split(sampled)
    samp[0] = high
    samp[1] = low
    shift = 0.01 * jnp.sum(sampled * sampled) / SIZE
    hh = lax.dot_general(high, high, CONTRACT_ROWS, preferred_element_type=f32)
    hl = lax.dot_general(high, low, CONTRACT_ROWS, preferred_element_type=f32)
    rows = lax.broadcasted_iota(jnp.int32, (SIZE, SIZE), 0)
    eye = rows == lax.broadcasted_iota(jnp.int32, (SIZE, SIZE), 1)
    added = jnp.where(keep, 0.0, 1.0) + shift
    gram[...] = (hh + (hl + jnp.transpose(hl))) + jnp.where(eye, added, 0.0)


def rolled(value, segments):
    shift = (segments * LEAF) % LANES
    return pltpu.roll(value, shift, axis=1) if shift else value


def gather_lanes(pieces):
    segment = lax.broadcasted_iota(jnp.int32, (1, LANES), 1) // LEAF
    out = pieces[0]
    for i in range(1, BATCH):
        out = jnp.where(segment == i, pieces[i], out)
    return out


def solve(gram, samp, scaled, a_ref, x_ref):
    for k in range(PANELS):
        rows = slice(k * LEAF, SIZE)
        lanes = lanes_of(k // 4)
        a_ref[k, rows, :] = gather_lanes(
            [rolled(gram[b][rows, lanes], b - k % 4) for b in range(BATCH)]
        )
        if k:
            a_ref[k, : k * LEAF, :] = jnp.zeros((k * LEAF, LANES), f32)

    invert_factor(a_ref, x_ref)

    def factor(b, offset):
        halves = []
        for g in range(2):
            panels = [
                rolled(x_ref[:, k * SIZE + offset : k * SIZE + offset + LANES], k % 4 - b)
                for k in range(4 * g, 4 * g + 4)
            ]
            halves.append(gather_lanes(panels))
        return jnp.concatenate(halves, axis=1)

    for b in range(BATCH):
        high, low = factor(b, 0), factor(b, LANES)
        solved = dot(samp[b][0], high) + (dot(samp[b][0], low) + dot(samp[b][1], high))
        scaled[b] = (solved * 16.0).astype(bf16)


def deliver(role, scaled, mixed, wide, ready, msg, out, sems):
    is_right = role[0] == 1
    copies = []
    for b in range(BATCH):
        right_part = lax.dot_general(
            scaled[b], mixed[b][...], CONTRACT_ROWS, preferred_element_type=f32
        ) * (1.0 / SIZE)
        left_wide, right_wide = wide.at[2 * (b % 2)], wide.at[2 * (b % 2) + 1]
        for s in range(2):
            half = scaled[b, UPPER, :] if s == 0 else scaled[b + 1, LOWER, :]
            for jb in range(2):
                lines = lines_of(jb, s)
                left_wide[lines, :] = half[:, lanes_of(jb)].astype(f32)
                right_wide[lines, :] = right_part[:, lanes_of(2 * s + jb)]
        left_site = left_wide[...]
        right_site = right_wide[...]
        msg[b] = jnp.where(is_right, left_site, right_site).astype(bf16)
        ready[b] = jnp.where(is_right, right_site, left_site).astype(bf16)
        copies.append(pltpu.make_async_copy(ready.at[b], out.at[role[1] + b], sems.at[b]))
        copies[-1].start()
    return copies


def early_kernel(role, gates, kept, own, got_0, got, scale, sketch, *refs):
    mixed, samp, gram, edge, left_w, right_w, wide = refs

    def step(t, loop):
        weigh(t, role, own, got.at[0], scale, left_w.at[t], right_w.at[t], wide)
        return loop

    def step_0(t, loop):
        weigh(t, role, own, got_0.at[t - 1], scale, left_w.at[t], right_w.at[t], wide)
        return loop

    lax.fori_loop(1, 4, step_0, 0)
    lax.fori_loop(4, 6, step, 0)
    for s in range(2):
        edge[s] = left_w[1, s]
        edge[2 + s] = right_w[1, s]
    edge[4] = right_w[2, 0]
    below = role[1] - 5
    wide[0] = got[0].astype(f32)
    rows = column_of(scale[1, below + 1])
    col = scale[2, below + 2]
    for jb in range(2):
        lanes = lanes_of(jb)
        edge[5, :, lanes] = ((wide[0, lines_of(jb, 1), :] * rows) * col[:, lanes]).astype(bf16)
    for b in range(1, BATCH):
        t = b + 1
        sample(
            gates,
            kept[role[1] + b],
            sketch[b],
            (left_w[t, 0], left_w[t, 1]),
            (left_w[t - 1, 0], left_w[t - 1, 1]),
            (right_w[t, 0], right_w[t, 1]),
            right_w[t - 1, 1],
            right_w[t + 1, 0],
            mixed.at[b - 1],
            samp.at[b - 1],
            gram.at[b - 1],
        )


def first_kernel(role, gates, kept, own, got, scale, sketch, *refs):
    (mixed_e, samp_e, gram_e, edge, msg, out, carry), refs = refs[:7], refs[7:]
    mixed, samp, gram, scaled, a_ref, x_ref, wide, ready, sems = refs
    left, right = carry.at[pl.ds(1, 2)], carry.at[pl.ds(3, 2)]
    weigh(0, role, own, got.at[0], scale, left, right, wide)
    sample(
        gates,
        kept[role[1]],
        sketch[0],
        (edge[0], edge[1]),
        (left[0], left[1]),
        (edge[2], edge[3]),
        right[1],
        edge[4],
        mixed,
        samp,
        gram,
    )
    mixed = [mixed] + [mixed_e.at[b] for b in range(BATCH - 1)]
    samp = [samp] + [samp_e.at[b] for b in range(BATCH - 1)]
    gram = [gram] + [gram_e.at[b] for b in range(BATCH - 1)]
    solve(gram, samp, scaled, a_ref, x_ref)
    scaled[BATCH, LOWER, :] = jnp.zeros((SIZE, SIZE), bf16)
    carry[0] = scaled[0, LOWER, :]
    for copy in deliver(role, scaled, mixed, wide, ready, msg, out, sems):
        copy.wait()


def second_kernel(role, gates, kept, own, got, scale, sketch, *refs):
    (edge, carry, _, msg, out, merge), refs = refs[:6], refs[6:]
    left_w, right_w, mixed, samp, gram, scaled, a_ref, x_ref, wide = refs[:9]
    ready, sems = refs[9:]

    def step(t, loop):
        at = jnp.maximum(t - 1, 0)
        weigh(t, role, own, got.at[at], scale, left_w.at[t], right_w.at[t], wide)
        return loop

    lax.fori_loop(0, 4, step, 0)
    right_w[0, 1] = edge[5]
    for s in range(2):
        left_w[4, s] = carry[1 + s]
        right_w[4, s] = carry[3 + s]
    right_w[5, 0] = edge[2]
    for b in range(BATCH):
        t = b + 1
        sample(
            gates,
            kept[role[1] + b],
            sketch[b],
            (left_w[t, 0], left_w[t, 1]),
            (left_w[b, 0], left_w[b, 1]),
            (right_w[t, 0], right_w[t, 1]),
            right_w[b, 1],
            right_w[t + 1, 0],
            mixed.at[b],
            samp.at[b],
            gram.at[b],
        )
    every = range(BATCH)
    solve([gram.at[b] for b in every], [samp.at[b] for b in every], scaled, a_ref, x_ref)
    scaled[BATCH, LOWER, :] = carry[0]
    copies = deliver(
        role, scaled, [mixed.at[b] for b in every], wide, ready, msg, out, sems
    )
    used = jnp.where(role[0] == 1, 0.0, 1.0)
    for jb in range(2):
        value = scaled[0, LOWER, lanes_of(jb)].astype(f32)
        wide[0, lines_of(jb, 0), :] = jnp.zeros((SIZE, LANES), f32)
        wide[0, lines_of(jb, 1), :] = value * used
    merge[...] = wide[0].astype(bf16)
    for copy in copies:
        copy.wait()


def in_hbm(x):
    return pltpu.with_memory_space_constraint(x, pltpu.HBM)


def shaped(*shape, dtype=bf16):
    return jax.ShapeDtypeStruct(shape, dtype)


def run(kernel, operands, specs, outs, out_specs, scratch, aliases=None, mib=20):
    return pl.pallas_call(
        kernel,
        out_shape=outs,
        in_specs=specs,
        out_specs=out_specs,
        scratch_shapes=scratch,
        input_output_aliases=aliases or {},
        compiler_params=pltpu.CompilerParams(vmem_limit_bytes=mib * 2**20),
        cost_estimate=pl.CostEstimate(
            flops=mib * 500_000_000, bytes_accessed=8_000_000, transcendentals=0
        ),
    )(*operands)


SMEM = pl.BlockSpec(memory_space=pltpu.SMEM)
VMEM = pl.BlockSpec(memory_space=pltpu.VMEM)
HBM = pl.BlockSpec(memory_space=pltpu.HBM)
SECTOR = (4 * SIZE, LANES)


def factor_scratch():
    return [
        pltpu.VMEM((BATCH + 1, 2 * SIZE, SIZE), bf16),
        pltpu.VMEM((PANELS, SIZE, LANES), f32),
        pltpu.VMEM((SIZE, PANELS * SIZE), bf16),
        pltpu.VMEM((4, *SECTOR), f32),
    ]


def sample_shapes(make, *lead):
    return [
        make((*lead, 2 * SIZE, 2 * SIZE), bf16),
        make((*lead, 2, 2 * SIZE, SIZE), bf16),
        make((*lead, SIZE, SIZE), f32),
    ]


def early(role, gates, kept, own, got_0, got, scale, sketch):
    return run(
        early_kernel,
        (role, gates, kept, own, got_0, got, scale, sketch),
        [SMEM] * 3 + [VMEM] * 5,
        sample_shapes(jax.ShapeDtypeStruct, BATCH - 1) + [shaped(6, SIZE, SIZE)],
        [VMEM] * 4,
        [
            pltpu.VMEM((6, 2, SIZE, SIZE), bf16),
            pltpu.VMEM((6, 2, SIZE, SIZE), bf16),
            pltpu.VMEM((2, *SECTOR), f32),
        ],
    )


def first_half(role, gates, kept, own, got, scale, sketch, parts):
    return run(
        first_kernel,
        (role, gates, kept, own, got, scale, sketch, *parts),
        [SMEM] * 3 + [VMEM] * 8,
        [shaped(BATCH, *SECTOR), pltpu.HBM((16, *SECTOR), bf16), shaped(5, SIZE, SIZE)],
        [VMEM, HBM, VMEM],
        sample_shapes(pltpu.VMEM)
        + factor_scratch()
        + [pltpu.VMEM((BATCH, *SECTOR), bf16), pltpu.SemaphoreType.DMA((BATCH,))],
    )


def second_half(role, gates, kept, own, got, scale, sketch, edge, carry, out):
    return run(
        second_kernel,
        (role, gates, kept, own, got, scale, sketch, edge, carry, out),
        [SMEM] * 3 + [VMEM] * 6 + [HBM],
        [shaped(BATCH, *SECTOR), pltpu.HBM((16, *SECTOR), bf16), shaped(*SECTOR)],
        [VMEM, HBM, VMEM],
        [pltpu.VMEM((6, 2, SIZE, SIZE), bf16), pltpu.VMEM((6, 2, SIZE, SIZE), bf16)]
        + sample_shapes(pltpu.VMEM, BATCH)
        + factor_scratch()
        + [
            pltpu.VMEM((BATCH, *SECTOR), bf16),
            pltpu.SemaphoreType.DMA((BATCH,)),
        ],
        aliases={9: 1},
    )


def fetch_kernel(at, own, out, sem):
    copy = pltpu.make_async_copy(own.at[pl.ds(at[0], out.shape[0])], out, sem)
    copy.start()
    copy.wait()


def fetch(at, own):
    return run(
        fetch_kernel,
        (jnp.reshape(at, (1,)), in_hbm(own)),
        [SMEM, HBM],
        [shaped(3, *SECTOR)],
        [VMEM],
        [pltpu.SemaphoreType.DMA],
        mib=1,
    )[0]


def pack_kernel(role, own, out, low, both, sems):
    flag = role[0]
    copies = [
        pltpu.make_async_copy(own.at[7 + 8 * flag], both.at[0], sems.at[0]),
        pltpu.make_async_copy(own.at[7], both.at[1], sems.at[1]),
        pltpu.make_async_copy(own.at[3 + 8 * flag], low.at[0], sems.at[2]),
    ]
    for copy in copies:
        copy.start()
    copies[0].wait()
    copies[1].wait()
    is_odd = lax.broadcasted_iota(jnp.int32, SECTOR, 0) % 2 == 1
    out[0] = jnp.where(is_odd, both[1].astype(f32), both[0].astype(f32)).astype(bf16)
    copies[2].wait()


def pack(role, own):
    return run(
        pack_kernel,
        (role, in_hbm(own)),
        [SMEM, HBM],
        [shaped(1, *SECTOR)] * 2,
        [VMEM] * 2,
        [pltpu.VMEM((2, *SECTOR), bf16), pltpu.SemaphoreType.DMA((3,))],
        mib=2,
    )


def place_kernel(merged, at, block, *refs):
    if merged:
        merge, _, out, last, sems = refs
    else:
        _, out, sems = refs
    count = block.shape[0]
    copies = []
    for b in range(count):
        source = block.at[b]
        if merged and b == count - 1:
            last[...] = block[b] + merge[...]
            source = last
        copies.append(pltpu.make_async_copy(source, out.at[at[0] + b], sems.at[b]))
        copies[-1].start()
    for copy in copies:
        copy.wait()


def place(out, block, at, merge=None):
    smem = pl.BlockSpec(memory_space=pltpu.SMEM)
    vmem = pl.BlockSpec(memory_space=pltpu.VMEM)
    hbm = pl.BlockSpec(memory_space=pltpu.HBM)
    operands = (jnp.reshape(at, (1,)), block) + (() if merge is None else (merge,)) + (out,)
    scratch = [] if merge is None else [pltpu.VMEM(merge.shape, bf16)]
    return pl.pallas_call(
        functools.partial(place_kernel, merge is not None),
        out_shape=pltpu.HBM(out.shape, out.dtype),
        in_specs=[smem] + [vmem] * (len(operands) - 2) + [hbm],
        out_specs=hbm,
        scratch_shapes=scratch + [pltpu.SemaphoreType.DMA((block.shape[0],))],
        input_output_aliases={len(operands) - 1: 0},
        compiler_params=pltpu.CompilerParams(vmem_limit_bytes=8 * 2**20),
        cost_estimate=pl.CostEstimate(flops=1000000, bytes_accessed=2_000_000, transcendentals=0),
        name="place",
    )(*operands)


def to_lines(x):
    n = x.shape[0]
    return x.reshape(n, SIZE, 2, 2, LANES).transpose(0, 1, 3, 2, 4).reshape(n, 4 * SIZE, LANES)


def from_lines(x):
    n = x.shape[0]
    return x.reshape(n, SIZE, 2, 2, LANES).transpose(0, 1, 3, 2, 4).reshape(n, SIZE, 2, SIZE)


def shards(site_tensors, bond_weights, sector_sizes, kept_ranks, sketches, gate_ends, gate_pair):
    chain = lax.axis_size("chain")
    count = lax.axis_size("group") * chain
    site = lax.axis_index("group") * chain + lax.axis_index("chain")
    is_right = site % 2 == 1

    def swapped(value):
        return lax.ppermute(value, "chain", [(i, i ^ 1) for i in range(chain)])

    def onward(value):
        def place(n):
            return n % chain * (count // chain) + n // chain

        pairs = [(place(i), place(i + 1)) for i in range(1, count - 1, 2)]
        return lax.ppermute(value, ("chain", "group"), pairs)

    own = to_lines(site_tensors[0, 0])
    sectors = own.shape[0]
    flag = is_right.astype(jnp.int32)

    def window(array, start, size):
        return lax.dynamic_slice_in_dim(array, start, size, 0)

    got_0 = swapped(fetch(4 + 8 * flag, own))
    column = lax.broadcasted_iota(jnp.int32, (sectors, SIZE), 1)
    lam = bond_weights[0, 0] * (column < sector_sizes[0, 0][:, None]).astype(f32)
    before = onward(lam)
    before = jnp.where(site < 2, jnp.ones_like(lam), before)
    kept_line = jnp.pad(kept_ranks[0, 0].astype(f32)[None, :], ((0, 7), (0, SIZE - sectors)))
    packed = jnp.concatenate([lam, before, kept_line], axis=0)
    other = swapped(packed)
    outgoing, outgoing_low = pack(jnp.reshape(flag, (1,)), own)
    got_a = swapped(outgoing)
    got_low = swapped(outgoing_low)
    lam_prev = jnp.where(is_right, other[sectors : 2 * sectors], before)
    lam_mid = jnp.where(is_right, other[:sectors], lam)
    lam_next = jnp.where(is_right, lam, other[:sectors])
    scale = jnp.pad(jnp.stack([lam_prev, lam_mid, lam_next]), ((0, 0), (1, 7), (0, 0)))
    scale = scale[:, :, None, :]
    kept = jnp.where(is_right, other[2 * sectors, :sectors], packed[2 * sectors, :sectors])
    kept = kept.astype(jnp.int32)
    late = jnp.minimum(kept[0], 0)
    got_b = swapped(window(own, 8 * flag + late, 3))
    gates = jnp.concatenate([gate_ends, 1.0 + gate_pair[:2], gate_pair[2:]])
    first_a = 12 - 8 * flag
    first_b = 8 - 8 * flag
    own_a = 10 - 7 * flag
    own_b = 7 - 7 * flag
    role_a = jnp.stack([flag, first_a, own_a])
    role_b = jnp.stack([flag, first_b, own_b])

    own_win = window(own, own_a + late, 6)
    sketch_win = window(sketches, first_a + late, BATCH)
    parts = early(role_a, gates, kept, own_win, got_0, got_a, scale, sketch_win)
    msg_a, out, carry = first_half(
        role_a, gates, kept, own_win, got_low, scale, sketch_win, parts
    )
    back_a = swapped(msg_a)
    own_win = window(own, own_b + late, BATCH)
    sketch_win = window(sketches, first_b + late, BATCH)
    msg_b, out, merge = second_half(
        role_b, gates, kept, own_win, got_b, scale, sketch_win, parts[3], carry, out
    )
    back_b = swapped(msg_b)

    back_at = 8 * flag
    out = place(out, back_a, back_at + 4, merge)
    out = place(out, back_b, back_at)
    return from_lines(out)[None, None]


def solution(mesh):
    return jax.shard_map(
        shards,
        mesh=mesh,
        in_specs=(
            P("group", "chain", None, None, None, None),
            P("group", "chain", None, None),
            P("group", "chain", None),
            P("group", "chain", None),
            P(),
            P(),
            P(),
        ),
        out_specs=P("group", "chain", None, None, None, None),
        check_vma=False,
    )
```

```python
import functools

import jax
import jax.numpy as jnp
from jax import lax
from jax.experimental import pallas as pl
from jax.experimental.pallas import tpu as pltpu
from jax.sharding import PartitionSpec as P

f32 = jnp.float32
bf16 = jnp.bfloat16


BATCH = 4
LEAF = 32
PANELS = 8
LANES = 128
SIZE = 256


def split(x):
    high = x.astype(bf16)
    return high, (x - high.astype(f32)).astype(bf16)


def invert_leaf(d):
    lane = lax.broadcasted_iota(jnp.int32, (8, LANES), 1)
    sub = lax.broadcasted_iota(jnp.int32, (8, LANES), 0)
    segment = (lane // LEAF) * LEAF
    tiles = LEAF // 8
    rows = [d[8 * t : 8 * t + 8, :] for t in range(tiles)]
    cols = [
        [
            jnp.take_along_axis(rows[t], segment + j, axis=1) if t >= j // 8 else None
            for t in range(tiles)
        ]
        for j in range(LEAF)
    ]
    inverse = [((lane - segment) == (sub + 8 * t)).astype(f32) for t in range(tiles)]
    pivots = [jnp.ones((8, LANES), f32) for _ in range(tiles)]

    def row(v, r):
        return jnp.broadcast_to(v[r : r + 1, :], (8, LANES))

    for j in range(LEAF):
        top, r = j // 8, j % 8
        pivot = row(cols[j][top], r)
        reciprocal = 1.0 / pivot
        pivots[top] = jnp.where(sub == r, pivot, pivots[top])
        scaled = {t: cols[j][t] * reciprocal for t in range(top, tiles)}
        for i in range(j + 1, LEAF):
            factor = row(scaled[i // 8], i % 8)
            for t in range(i // 8, tiles):
                cols[i][t] = cols[i][t] - factor * cols[j][t]
        source = row(inverse[top], r)
        for t in range(top, tiles):
            factor = jnp.where(sub > r, scaled[t], 0.0) if t == top else scaled[t]
            inverse[t] = inverse[t] - factor * source
    return jnp.concatenate([inverse[t] * lax.rsqrt(pivots[t]) for t in range(tiles)], axis=0)


def block_weights(high, low, masks):
    high = jnp.concatenate([high * mask for mask in masks], axis=0)
    low = jnp.concatenate([low * mask for mask in masks], axis=0)
    upper = jnp.concatenate([high, high], axis=1)
    lower = jnp.concatenate([low, jnp.zeros_like(low)], axis=1)
    return jnp.concatenate([upper, lower], axis=0)


def times_transposed(x, weights):
    out = lax.dot_general(x, weights, (((1,), (1,)), ((), ())), preferred_element_type=f32)
    return out[:, :LANES] + out[:, LANES:]


def invert_factor(a_ref, x_ref):
    lane = lax.broadcasted_iota(jnp.int32, (LEAF, LANES), 1)
    sub = lax.broadcasted_iota(jnp.int32, (LEAF, LANES), 0)
    eye = ((lane % LEAF) == sub).astype(f32)
    masks = [((lane // LEAF) == b).astype(f32).astype(bf16) for b in range(BATCH)]

    def weights_of(rows, ks):
        return jnp.concatenate(
            [
                block_weights(
                    x_ref[rows, k * SIZE : k * SIZE + LANES],
                    x_ref[rows, k * SIZE + LANES : (k + 1) * SIZE],
                    masks,
                )
                for k in ks
            ],
            axis=1,
        )

    partial = None
    for j in range(PANELS):
        start = j * LEAF
        block = slice(start, start + LEAF)
        col = a_ref[j]
        if j:
            last = slice((j - 1) * SIZE, j * SIZE)
            if partial is not None:
                col = col - partial
            col = col - times_transposed(x_ref[:, last], weights_of(block, [j - 1]))
            x_ref[block, : j * SIZE] = jnp.zeros((LEAF, j * SIZE), bf16)
            if j < PANELS - 1:
                following = slice(start + LEAF, start + 2 * LEAF)
                partial = times_transposed(
                    x_ref[:, : j * SIZE], weights_of(following, range(j))
                )
        inverse = invert_leaf(col[block])
        col = jnp.concatenate(
            [part for part in (col[:start], eye, col[start + LEAF :]) if part.shape[0]], axis=0
        )
        col = times_transposed(
            jnp.concatenate(split(col), axis=1), block_weights(*split(inverse), masks)
        )
        x_ref[:, j * SIZE : (j + 1) * SIZE] = jnp.concatenate(split(col), axis=1)


UPPER, LOWER = slice(0, SIZE), slice(SIZE, 2 * SIZE)
CONTRACT_ROWS = (((0,), (0,)), ((), ()))


def dot(a, b):
    return jnp.dot(a, b, preferred_element_type=f32)


def lines_of(lane_block, s):
    return pl.ds(2 * lane_block + s, SIZE, stride=4)


def lanes_of(lane_block):
    return slice(lane_block * LANES, (lane_block + 1) * LANES)


def column_of(line):
    return jnp.transpose(jnp.broadcast_to(line, (LANES, SIZE)))


def weigh(t, role, own, got, scale, left, right, wide):
    is_right = role[0] == 1
    q = role[1] - 1 + t
    own_wide = own[...].astype(f32)
    got_wide = got[...].astype(f32)
    wide[0] = jnp.where(is_right, got_wide, own_wide)
    wide[1] = jnp.where(is_right, own_wide, got_wide)
    left_rows = column_of(scale[0, q + 1])
    right_rows = column_of(scale[1, q + 1])
    for s in range(2):
        col = scale[2, q + s + 1]
        for jb in range(2):
            lines, lanes = lines_of(jb, s), lanes_of(jb)
            left[s, :, lanes] = (wide[0, lines, :] * left_rows).astype(bf16)
            right[s, :, lanes] = ((wide[1, lines, :] * right_rows) * col[:, lanes]).astype(bf16)


def sample(gates, kept, sketch, left, before, right, right_before, right_after, mixed, samp, gram):
    g0, g1, p0, p1, p2 = [gates[i] for i in range(5)]
    mixed[UPPER, UPPER] = (g0 * dot(left[0], right[0])).astype(bf16)
    mixed[UPPER, LOWER] = (p0 * dot(left[0], right[1]) + p2 * dot(left[1], right_after)).astype(bf16)
    mixed[LOWER, UPPER] = (
        p2 * dot(before[0], right_before) + p1 * dot(before[1], right[0])
    ).astype(bf16)
    mixed[LOWER, LOWER] = (g1 * dot(before[1], right[1])).astype(bf16)
    keep = lax.broadcasted_iota(jnp.int32, (1, SIZE), 1) < kept
    sampled = jnp.where(keep, dot(mixed[...], sketch), 0.0)
    high, low = split(sampled)
    samp[0] = high
    samp[1] = low
    shift = 0.01 * jnp.sum(sampled * sampled) / SIZE
    hh = lax.dot_general(high, high, CONTRACT_ROWS, preferred_element_type=f32)
    hl = lax.dot_general(high, low, CONTRACT_ROWS, preferred_element_type=f32)
    rows = lax.broadcasted_iota(jnp.int32, (SIZE, SIZE), 0)
    eye = rows == lax.broadcasted_iota(jnp.int32, (SIZE, SIZE), 1)
    added = jnp.where(keep, 0.0, 1.0) + shift
    gram[...] = (hh + (hl + jnp.transpose(hl))) + jnp.where(eye, added, 0.0)


def rolled(value, segments):
    shift = (segments * LEAF) % LANES
    return pltpu.roll(value, shift, axis=1) if shift else value


def gather_lanes(pieces):
    segment = lax.broadcasted_iota(jnp.int32, (1, LANES), 1) // LEAF
    out = pieces[0]
    for i in range(1, BATCH):
        out = jnp.where(segment == i, pieces[i], out)
    return out


def solve(gram, samp, scaled, a_ref, x_ref):
    for k in range(PANELS):
        rows = slice(k * LEAF, SIZE)
        lanes = lanes_of(k // 4)
        a_ref[k, rows, :] = gather_lanes(
            [rolled(gram[b][rows, lanes], b - k % 4) for b in range(BATCH)]
        )
        if k:
            a_ref[k, : k * LEAF, :] = jnp.zeros((k * LEAF, LANES), f32)

    invert_factor(a_ref, x_ref)

    def factor(b, offset):
        halves = []
        for g in range(2):
            panels = [
                rolled(x_ref[:, k * SIZE + offset : k * SIZE + offset + LANES], k % 4 - b)
                for k in range(4 * g, 4 * g + 4)
            ]
            halves.append(gather_lanes(panels))
        return jnp.concatenate(halves, axis=1)

    for b in range(BATCH):
        high, low = factor(b, 0), factor(b, LANES)
        solved = dot(samp[b][0], high) + (dot(samp[b][0], low) + dot(samp[b][1], high))
        scaled[b] = (solved * 16.0).astype(bf16)


def deliver(role, scaled, mixed, wide, ready, msg, out, sems):
    is_right = role[0] == 1
    copies = []
    for b in range(BATCH):
        right_part = lax.dot_general(
            scaled[b], mixed[b][...], CONTRACT_ROWS, preferred_element_type=f32
        ) * (1.0 / SIZE)
        left_wide, right_wide = wide.at[2 * (b % 2)], wide.at[2 * (b % 2) + 1]
        for s in range(2):
            half = scaled[b, UPPER, :] if s == 0 else scaled[b + 1, LOWER, :]
            for jb in range(2):
                lines = lines_of(jb, s)
                left_wide[lines, :] = half[:, lanes_of(jb)].astype(f32)
                right_wide[lines, :] = right_part[:, lanes_of(2 * s + jb)]
        left_site = left_wide[...]
        right_site = right_wide[...]
        msg[b] = jnp.where(is_right, left_site, right_site).astype(bf16)
        ready[b] = jnp.where(is_right, right_site, left_site).astype(bf16)
        copies.append(pltpu.make_async_copy(ready.at[b], out.at[role[1] + b], sems.at[b]))
        copies[-1].start()
    return copies


def windows(role, own, sketches, own_win, sketch, sems):
    count = own_win.shape[0]

    def own_copy(t):
        at = jnp.clip(role[1] - 1 + t, 0, own.shape[0] - 1)
        return pltpu.make_async_copy(own.at[at], own_win.at[t], sems.at[t])

    sketch_copy = pltpu.make_async_copy(
        sketches.at[pl.ds(role[1], BATCH)], sketch, sems.at[count]
    )
    return own_copy, sketch_copy


def early_kernel(role, gates, kept, own, got_0, got, scale, sketches, *refs):
    mixed, samp, gram, edge, own_low, left_w, right_w, wide, own_win, sketch, sems = refs
    own_copy, sketch_copy = windows(role, own, sketches, own_win, sketch, sems)
    for t in (1, 2, 3, 4, 5, 0):
        own_copy(t).start()
    sketch_copy.start()

    def step(t, loop):
        own_copy(t).wait()
        weigh(t, role, own_win.at[t], got.at[0], scale, left_w.at[t], right_w.at[t], wide)
        return loop

    def step_0(t, loop):
        own_copy(t).wait()
        weigh(t, role, own_win.at[t], got_0.at[t - 1], scale, left_w.at[t], right_w.at[t], wide)
        return loop

    lax.fori_loop(1, 4, step_0, 0)
    lax.fori_loop(4, 6, step, 0)
    for s in range(2):
        edge[s] = left_w[1, s]
        edge[2 + s] = right_w[1, s]
    edge[4] = right_w[2, 0]
    below = role[1] - 5
    wide[0] = got[0].astype(f32)
    rows = column_of(scale[1, below + 1])
    col = scale[2, below + 2]
    for jb in range(2):
        lanes = lanes_of(jb)
        edge[5, :, lanes] = ((wide[0, lines_of(jb, 1), :] * rows) * col[:, lanes]).astype(bf16)
    own_copy(0).wait()
    own_low[...] = own_win[0]
    sketch_copy.wait()
    edge[6] = sketch[0, UPPER]
    edge[7] = sketch[0, LOWER]
    for b in range(1, BATCH):
        t = b + 1
        sample(
            gates,
            kept[role[1] + b],
            sketch[b],
            (left_w[t, 0], left_w[t, 1]),
            (left_w[t - 1, 0], left_w[t - 1, 1]),
            (right_w[t, 0], right_w[t, 1]),
            right_w[t - 1, 1],
            right_w[t + 1, 0],
            mixed.at[b - 1],
            samp.at[b - 1],
            gram.at[b - 1],
        )


def first_kernel(role, gates, kept, got, scale, *refs):
    (mixed_e, samp_e, gram_e, edge, own, msg, out, carry), refs = refs[:8], refs[8:]
    mixed, samp, gram, scaled, a_ref, x_ref, wide, ready, sems = refs
    left, right = carry.at[pl.ds(1, 2)], carry.at[pl.ds(3, 2)]
    weigh(0, role, own, got.at[0], scale, left, right, wide)
    sample(
        gates,
        kept[role[1]],
        jnp.concatenate([edge[6], edge[7]], axis=0),
        (edge[0], edge[1]),
        (left[0], left[1]),
        (edge[2], edge[3]),
        right[1],
        edge[4],
        mixed,
        samp,
        gram,
    )
    mixed = [mixed] + [mixed_e.at[b] for b in range(BATCH - 1)]
    samp = [samp] + [samp_e.at[b] for b in range(BATCH - 1)]
    gram = [gram] + [gram_e.at[b] for b in range(BATCH - 1)]
    solve(gram, samp, scaled, a_ref, x_ref)
    scaled[BATCH, LOWER, :] = jnp.zeros((SIZE, SIZE), bf16)
    carry[0] = scaled[0, LOWER, :]
    for copy in deliver(role, scaled, mixed, wide, ready, msg, out, sems):
        copy.wait()


def second_kernel(role, gates, kept, own, got, scale, sketches, *refs):
    (edge, carry, _, msg, out, merge), refs = refs[:6], refs[6:]
    left_w, right_w, mixed, samp, gram, scaled, a_ref, x_ref, wide = refs[:9]
    ready, sems, own_win, sketch, win_sems = refs[9:]
    own_copy, sketch_copy = windows(role, own, sketches, own_win, sketch, win_sems)
    for t in range(4):
        own_copy(t).start()
    sketch_copy.start()

    def step(t, loop):
        at = jnp.maximum(t - 1, 0)
        own_copy(t).wait()
        weigh(t, role, own_win.at[t], got.at[at], scale, left_w.at[t], right_w.at[t], wide)
        return loop

    lax.fori_loop(0, 4, step, 0)
    right_w[0, 1] = edge[5]
    for s in range(2):
        left_w[4, s] = carry[1 + s]
        right_w[4, s] = carry[3 + s]
    right_w[5, 0] = edge[2]
    sketch_copy.wait()
    for b in range(BATCH):
        t = b + 1
        sample(
            gates,
            kept[role[1] + b],
            sketch[b],
            (left_w[t, 0], left_w[t, 1]),
            (left_w[b, 0], left_w[b, 1]),
            (right_w[t, 0], right_w[t, 1]),
            right_w[b, 1],
            right_w[t + 1, 0],
            mixed.at[b],
            samp.at[b],
            gram.at[b],
        )
    every = range(BATCH)
    solve([gram.at[b] for b in every], [samp.at[b] for b in every], scaled, a_ref, x_ref)
    scaled[BATCH, LOWER, :] = carry[0]
    copies = deliver(
        role, scaled, [mixed.at[b] for b in every], wide, ready, msg, out, sems
    )
    used = jnp.where(role[0] == 1, 0.0, 1.0)
    for jb in range(2):
        value = scaled[0, LOWER, lanes_of(jb)].astype(f32)
        wide[0, lines_of(jb, 0), :] = jnp.zeros((SIZE, LANES), f32)
        wide[0, lines_of(jb, 1), :] = value * used
    merge[...] = wide[0].astype(bf16)
    for copy in copies:
        copy.wait()


def in_hbm(x):
    return pltpu.with_memory_space_constraint(x, pltpu.HBM)


def shaped(*shape, dtype=bf16):
    return jax.ShapeDtypeStruct(shape, dtype)


def run(kernel, operands, specs, outs, out_specs, scratch, aliases=None, mib=20):
    return pl.pallas_call(
        kernel,
        out_shape=outs,
        in_specs=specs,
        out_specs=out_specs,
        scratch_shapes=scratch,
        input_output_aliases=aliases or {},
        compiler_params=pltpu.CompilerParams(vmem_limit_bytes=mib * 2**20),
        cost_estimate=pl.CostEstimate(
            flops=mib * 500_000_000, bytes_accessed=8_000_000, transcendentals=0
        ),
    )(*operands)


SMEM = pl.BlockSpec(memory_space=pltpu.SMEM)
VMEM = pl.BlockSpec(memory_space=pltpu.VMEM)
HBM = pl.BlockSpec(memory_space=pltpu.HBM)
SECTOR = (4 * SIZE, LANES)


def factor_scratch():
    return [
        pltpu.VMEM((BATCH + 1, 2 * SIZE, SIZE), bf16),
        pltpu.VMEM((PANELS, SIZE, LANES), f32),
        pltpu.VMEM((SIZE, PANELS * SIZE), bf16),
        pltpu.VMEM((4, *SECTOR), f32),
    ]


def sample_shapes(make, *lead):
    return [
        make((*lead, 2 * SIZE, 2 * SIZE), bf16),
        make((*lead, 2, 2 * SIZE, SIZE), bf16),
        make((*lead, SIZE, SIZE), f32),
    ]


def window_scratch(count):
    return [
        pltpu.VMEM((count, *SECTOR), bf16),
        pltpu.VMEM((BATCH, 2 * SIZE, SIZE), bf16),
        pltpu.SemaphoreType.DMA((count + 1,)),
    ]


def early(role, gates, kept, own, got_0, got, scale, sketches):
    return run(
        early_kernel,
        (role, gates, kept, in_hbm(own), got_0, got, scale, in_hbm(sketches)),
        [SMEM] * 3 + [HBM, VMEM, VMEM, VMEM, HBM],
        sample_shapes(jax.ShapeDtypeStruct, BATCH - 1) + [shaped(8, SIZE, SIZE), shaped(*SECTOR)],
        [VMEM] * 5,
        [
            pltpu.VMEM((6, 2, SIZE, SIZE), bf16),
            pltpu.VMEM((6, 2, SIZE, SIZE), bf16),
            pltpu.VMEM((2, *SECTOR), f32),
        ]
        + window_scratch(6),
    )


def first_half(role, gates, kept, got, scale, parts):
    return run(
        first_kernel,
        (role, gates, kept, got, scale, *parts),
        [SMEM] * 3 + [VMEM] * 7,
        [shaped(BATCH, *SECTOR), pltpu.HBM((16, *SECTOR), bf16), shaped(5, SIZE, SIZE)],
        [VMEM, HBM, VMEM],
        sample_shapes(pltpu.VMEM)
        + factor_scratch()
        + [pltpu.VMEM((BATCH, *SECTOR), bf16), pltpu.SemaphoreType.DMA((BATCH,))],
    )


def second_half(role, gates, kept, own, got, scale, sketches, edge, carry, out):
    return run(
        second_kernel,
        (role, gates, kept, in_hbm(own), got, scale, in_hbm(sketches), edge, carry, out),
        [SMEM] * 3 + [HBM, VMEM, VMEM, HBM, VMEM, VMEM, HBM],
        [shaped(BATCH, *SECTOR), pltpu.HBM((16, *SECTOR), bf16), shaped(*SECTOR)],
        [VMEM, HBM, VMEM],
        [pltpu.VMEM((6, 2, SIZE, SIZE), bf16), pltpu.VMEM((6, 2, SIZE, SIZE), bf16)]
        + sample_shapes(pltpu.VMEM, BATCH)
        + factor_scratch()
        + [
            pltpu.VMEM((BATCH, *SECTOR), bf16),
            pltpu.SemaphoreType.DMA((BATCH,)),
        ]
        + window_scratch(4),
        aliases={9: 1},
    )


def fetch_kernel(at, own, out, sem):
    copy = pltpu.make_async_copy(own.at[pl.ds(at[0], out.shape[0])], out, sem)
    copy.start()
    copy.wait()


def fetch(at, own):
    return run(
        fetch_kernel,
        (jnp.reshape(at, (1,)), in_hbm(own)),
        [SMEM, HBM],
        [shaped(3, *SECTOR)],
        [VMEM],
        [pltpu.SemaphoreType.DMA],
        mib=1,
    )[0]


def pack_kernel(role, own, out, low, rest, both, sems):
    flag = role[0]
    copies = [
        pltpu.make_async_copy(own.at[7 + 8 * flag], both.at[0], sems.at[0]),
        pltpu.make_async_copy(own.at[7], both.at[1], sems.at[1]),
        pltpu.make_async_copy(own.at[3 + 8 * flag], low.at[0], sems.at[2]),
        pltpu.make_async_copy(own.at[pl.ds(8 * flag, 3)], rest, sems.at[3]),
    ]
    for copy in copies:
        copy.start()
    copies[0].wait()
    copies[1].wait()
    is_odd = lax.broadcasted_iota(jnp.int32, SECTOR, 0) % 2 == 1
    out[0] = jnp.where(is_odd, both[1].astype(f32), both[0].astype(f32)).astype(bf16)
    copies[2].wait()
    copies[3].wait()


def pack(role, own):
    return run(
        pack_kernel,
        (role, in_hbm(own)),
        [SMEM, HBM],
        [shaped(1, *SECTOR), shaped(1, *SECTOR), shaped(3, *SECTOR)],
        [VMEM] * 3,
        [pltpu.VMEM((2, *SECTOR), bf16), pltpu.SemaphoreType.DMA((4,))],
        mib=2,
    )


def place_kernel(merged, at, block, *refs):
    if merged:
        merge, _, out, last, sems = refs
    else:
        _, out, sems = refs
    count = block.shape[0]
    copies = []
    for b in range(count):
        source = block.at[b]
        if merged and b == count - 1:
            last[...] = block[b] + merge[...]
            source = last
        copies.append(pltpu.make_async_copy(source, out.at[at[0] + b], sems.at[b]))
        copies[-1].start()
    for copy in copies:
        copy.wait()


def place(out, block, at, merge=None):
    smem = pl.BlockSpec(memory_space=pltpu.SMEM)
    vmem = pl.BlockSpec(memory_space=pltpu.VMEM)
    hbm = pl.BlockSpec(memory_space=pltpu.HBM)
    operands = (jnp.reshape(at, (1,)), block) + (() if merge is None else (merge,)) + (out,)
    scratch = [] if merge is None else [pltpu.VMEM(merge.shape, bf16)]
    return pl.pallas_call(
        functools.partial(place_kernel, merge is not None),
        out_shape=pltpu.HBM(out.shape, out.dtype),
        in_specs=[smem] + [vmem] * (len(operands) - 2) + [hbm],
        out_specs=hbm,
        scratch_shapes=scratch + [pltpu.SemaphoreType.DMA((block.shape[0],))],
        input_output_aliases={len(operands) - 1: 0},
        compiler_params=pltpu.CompilerParams(vmem_limit_bytes=8 * 2**20),
        cost_estimate=pl.CostEstimate(flops=1000000, bytes_accessed=2_000_000, transcendentals=0),
        name="place",
    )(*operands)


def to_lines(x):
    n = x.shape[0]
    return x.reshape(n, SIZE, 2, 2, LANES).transpose(0, 1, 3, 2, 4).reshape(n, 4 * SIZE, LANES)


def from_lines(x):
    n = x.shape[0]
    return x.reshape(n, SIZE, 2, 2, LANES).transpose(0, 1, 3, 2, 4).reshape(n, SIZE, 2, SIZE)


def shards(site_tensors, bond_weights, sector_sizes, kept_ranks, sketches, gate_ends, gate_pair):
    chain = lax.axis_size("chain")
    count = lax.axis_size("group") * chain
    site = lax.axis_index("group") * chain + lax.axis_index("chain")
    is_right = site % 2 == 1

    def swapped(value):
        return lax.ppermute(value, "chain", [(i, i ^ 1) for i in range(chain)])

    def onward(value):
        def place(n):
            return n % chain * (count // chain) + n // chain

        pairs = [(place(i), place(i + 1)) for i in range(1, count - 1, 2)]
        return lax.ppermute(value, ("chain", "group"), pairs)

    own = to_lines(site_tensors[0, 0])
    sectors = own.shape[0]
    flag = is_right.astype(jnp.int32)

    got_0 = swapped(fetch(4 + 8 * flag, own))
    column = lax.broadcasted_iota(jnp.int32, (sectors, SIZE), 1)
    lam = bond_weights[0, 0] * (column < sector_sizes[0, 0][:, None]).astype(f32)
    before = onward(lam)
    before = jnp.where(site < 2, jnp.ones_like(lam), before)
    kept_line = jnp.pad(kept_ranks[0, 0].astype(f32)[None, :], ((0, 7), (0, SIZE - sectors)))
    packed = jnp.concatenate([lam, before, kept_line], axis=0)
    other = swapped(packed)
    outgoing, outgoing_low, outgoing_b = pack(jnp.reshape(flag, (1,)), own)
    got_a = swapped(outgoing)
    got_low = swapped(outgoing_low)
    lam_prev = jnp.where(is_right, other[sectors : 2 * sectors], before)
    lam_mid = jnp.where(is_right, other[:sectors], lam)
    lam_next = jnp.where(is_right, lam, other[:sectors])
    scale = jnp.pad(jnp.stack([lam_prev, lam_mid, lam_next]), ((0, 0), (1, 7), (0, 0)))
    scale = scale[:, :, None, :]
    kept = jnp.where(is_right, other[2 * sectors, :sectors], packed[2 * sectors, :sectors])
    kept = kept.astype(jnp.int32)
    got_b = swapped(outgoing_b)
    gates = jnp.concatenate([gate_ends, 1.0 + gate_pair[:2], gate_pair[2:]])
    first_a = 12 - 8 * flag
    first_b = 8 - 8 * flag
    role_a = jnp.stack([flag, first_a])
    role_b = jnp.stack([flag, first_b])

    parts = early(role_a, gates, kept, own, got_0, got_a, scale, sketches)
    msg_a, out, carry = first_half(role_a, gates, kept, got_low, scale, parts)
    back_a = swapped(msg_a)
    msg_b, out, merge = second_half(
        role_b, gates, kept, own, got_b, scale, sketches, parts[3], carry, out
    )
    back_b = swapped(msg_b)

    back_at = 8 * flag
    out = place(out, back_a, back_at + 4, merge)
    out = place(out, back_b, back_at)
    return from_lines(out)[None, None]


def solution(mesh):
    return jax.shard_map(
        shards,
        mesh=mesh,
        in_specs=(
            P("group", "chain", None, None, None, None),
            P("group", "chain", None, None),
            P("group", "chain", None),
            P("group", "chain", None),
            P(),
            P(),
            P(),
        ),
        out_specs=P("group", "chain", None, None, None, None),
        check_vma=False,
    )
```

```python
import jax
import jax.numpy as jnp
from jax import lax
from jax.experimental import pallas as pl
from jax.experimental.pallas import tpu as pltpu
from jax.sharding import PartitionSpec as P

f32 = jnp.float32
bf16 = jnp.bfloat16


BATCH = 4
LEAF = 32
PANELS = 8
LANES = 128
SIZE = 256


def split(x):
    high = x.astype(bf16)
    return high, (x - high.astype(f32)).astype(bf16)


def invert_leaf(d):
    lane = lax.broadcasted_iota(jnp.int32, (8, LANES), 1)
    sub = lax.broadcasted_iota(jnp.int32, (8, LANES), 0)
    segment = (lane // LEAF) * LEAF
    tiles = LEAF // 8
    rows = [d[8 * t : 8 * t + 8, :] for t in range(tiles)]
    cols = [
        [
            jnp.take_along_axis(rows[t], segment + j, axis=1) if t >= j // 8 else None
            for t in range(tiles)
        ]
        for j in range(LEAF)
    ]
    inverse = [((lane - segment) == (sub + 8 * t)).astype(f32) for t in range(tiles)]
    pivots = [jnp.ones((8, LANES), f32) for _ in range(tiles)]

    def row(v, r):
        return jnp.broadcast_to(v[r : r + 1, :], (8, LANES))

    for j in range(LEAF):
        top, r = j // 8, j % 8
        pivot = row(cols[j][top], r)
        reciprocal = 1.0 / pivot
        pivots[top] = jnp.where(sub == r, pivot, pivots[top])
        scaled = {t: cols[j][t] * reciprocal for t in range(top, tiles)}
        for i in range(j + 1, LEAF):
            factor = row(scaled[i // 8], i % 8)
            for t in range(i // 8, tiles):
                cols[i][t] = cols[i][t] - factor * cols[j][t]
        source = row(inverse[top], r)
        for t in range(top, tiles):
            factor = jnp.where(sub > r, scaled[t], 0.0) if t == top else scaled[t]
            inverse[t] = inverse[t] - factor * source
    return jnp.concatenate([inverse[t] * lax.rsqrt(pivots[t]) for t in range(tiles)], axis=0)


def block_weights(high, low, masks):
    high = jnp.concatenate([high * mask for mask in masks], axis=0)
    low = jnp.concatenate([low * mask for mask in masks], axis=0)
    upper = jnp.concatenate([high, high], axis=1)
    lower = jnp.concatenate([low, jnp.zeros_like(low)], axis=1)
    return jnp.concatenate([upper, lower], axis=0)


def times_transposed(x, weights):
    out = lax.dot_general(x, weights, (((1,), (1,)), ((), ())), preferred_element_type=f32)
    return out[:, :LANES] + out[:, LANES:]


def invert_factor(a_ref, x_ref):
    lane = lax.broadcasted_iota(jnp.int32, (LEAF, LANES), 1)
    sub = lax.broadcasted_iota(jnp.int32, (LEAF, LANES), 0)
    eye = ((lane % LEAF) == sub).astype(f32)
    masks = [((lane // LEAF) == b).astype(f32).astype(bf16) for b in range(BATCH)]

    def weights_of(rows, ks):
        return jnp.concatenate(
            [
                block_weights(
                    x_ref[rows, k * SIZE : k * SIZE + LANES],
                    x_ref[rows, k * SIZE + LANES : (k + 1) * SIZE],
                    masks,
                )
                for k in ks
            ],
            axis=1,
        )

    partial = None
    for j in range(PANELS):
        start = j * LEAF
        block = slice(start, start + LEAF)
        col = a_ref[j]
        if j:
            last = slice((j - 1) * SIZE, j * SIZE)
            if partial is not None:
                col = col - partial
            col = col - times_transposed(x_ref[:, last], weights_of(block, [j - 1]))
            x_ref[block, : j * SIZE] = jnp.zeros((LEAF, j * SIZE), bf16)
            if j < PANELS - 1:
                following = slice(start + LEAF, start + 2 * LEAF)
                partial = times_transposed(
                    x_ref[:, : j * SIZE], weights_of(following, range(j))
                )
        inverse = invert_leaf(col[block])
        col = jnp.concatenate(
            [part for part in (col[:start], eye, col[start + LEAF :]) if part.shape[0]], axis=0
        )
        col = times_transposed(
            jnp.concatenate(split(col), axis=1), block_weights(*split(inverse), masks)
        )
        x_ref[:, j * SIZE : (j + 1) * SIZE] = jnp.concatenate(split(col), axis=1)


UPPER, LOWER = slice(0, SIZE), slice(SIZE, 2 * SIZE)
CONTRACT_ROWS = (((0,), (0,)), ((), ()))


def dot(a, b):
    return jnp.dot(a, b, preferred_element_type=f32)


def lines_of(lane_block, s):
    return pl.ds(2 * lane_block + s, SIZE, stride=4)


def lanes_of(lane_block):
    return slice(lane_block * LANES, (lane_block + 1) * LANES)


def column_of(line):
    return jnp.transpose(jnp.broadcast_to(line, (LANES, SIZE)))


def weigh(t, role, own, got, scale, left, right, wide):
    is_right = role[0] == 1
    q = role[1] - 1 + t
    own_wide = own[...].astype(f32)
    got_wide = got[...].astype(f32)
    wide[0] = jnp.where(is_right, got_wide, own_wide)
    wide[1] = jnp.where(is_right, own_wide, got_wide)
    left_rows = column_of(scale[0, q + 1])
    right_rows = column_of(scale[1, q + 1])
    for s in range(2):
        col = scale[2, q + s + 1]
        for jb in range(2):
            lines, lanes = lines_of(jb, s), lanes_of(jb)
            left[s, :, lanes] = (wide[0, lines, :] * left_rows).astype(bf16)
            right[s, :, lanes] = ((wide[1, lines, :] * right_rows) * col[:, lanes]).astype(bf16)


def sample(gates, kept, sketch, left, before, right, right_before, right_after, mixed, samp, gram):
    g0, g1, p0, p1, p2 = [gates[i] for i in range(5)]
    mixed[UPPER, UPPER] = (g0 * dot(left[0], right[0])).astype(bf16)
    mixed[UPPER, LOWER] = (p0 * dot(left[0], right[1]) + p2 * dot(left[1], right_after)).astype(bf16)
    mixed[LOWER, UPPER] = (
        p2 * dot(before[0], right_before) + p1 * dot(before[1], right[0])
    ).astype(bf16)
    mixed[LOWER, LOWER] = (g1 * dot(before[1], right[1])).astype(bf16)
    keep = lax.broadcasted_iota(jnp.int32, (1, SIZE), 1) < kept
    sampled = jnp.where(keep, dot(mixed[...], sketch), 0.0)
    high, low = split(sampled)
    samp[0] = high
    samp[1] = low
    shift = 0.01 * jnp.sum(sampled * sampled) / SIZE
    hh = lax.dot_general(high, high, CONTRACT_ROWS, preferred_element_type=f32)
    hl = lax.dot_general(high, low, CONTRACT_ROWS, preferred_element_type=f32)
    rows = lax.broadcasted_iota(jnp.int32, (SIZE, SIZE), 0)
    eye = rows == lax.broadcasted_iota(jnp.int32, (SIZE, SIZE), 1)
    added = jnp.where(keep, 0.0, 1.0) + shift
    gram[...] = (hh + (hl + jnp.transpose(hl))) + jnp.where(eye, added, 0.0)


def rolled(value, segments):
    shift = (segments * LEAF) % LANES
    return pltpu.roll(value, shift, axis=1) if shift else value


def gather_lanes(pieces):
    segment = lax.broadcasted_iota(jnp.int32, (1, LANES), 1) // LEAF
    out = pieces[0]
    for i in range(1, BATCH):
        out = jnp.where(segment == i, pieces[i], out)
    return out


def solve(gram, samp, scaled, a_ref, x_ref):
    for k in range(PANELS):
        rows = slice(k * LEAF, SIZE)
        lanes = lanes_of(k // 4)
        a_ref[k, rows, :] = gather_lanes(
            [rolled(gram[b][rows, lanes], b - k % 4) for b in range(BATCH)]
        )
        if k:
            a_ref[k, : k * LEAF, :] = jnp.zeros((k * LEAF, LANES), f32)

    invert_factor(a_ref, x_ref)

    def factor(b, offset):
        halves = []
        for g in range(2):
            panels = [
                rolled(x_ref[:, k * SIZE + offset : k * SIZE + offset + LANES], k % 4 - b)
                for k in range(4 * g, 4 * g + 4)
            ]
            halves.append(gather_lanes(panels))
        return jnp.concatenate(halves, axis=1)

    for b in range(BATCH):
        high, low = factor(b, 0), factor(b, LANES)
        solved = dot(samp[b][0], high) + (dot(samp[b][0], low) + dot(samp[b][1], high))
        scaled[b] = (solved * 16.0).astype(bf16)


def deliver(role, scaled, mixed, wide, ready, msg, out, sems, halved):
    is_right = role[0] == 1
    copies = []
    for b in range(BATCH):
        right_part = lax.dot_general(
            scaled[b], mixed[b][...], CONTRACT_ROWS, preferred_element_type=f32
        ) * (1.0 / SIZE)
        left_wide, right_wide = wide.at[2 * (b % 2)], wide.at[2 * (b % 2) + 1]
        for s in range(2):
            half = scaled[b, UPPER, :] if s == 0 else scaled[b + 1, LOWER, :]
            for jb in range(2):
                lines = lines_of(jb, s)
                left_wide[lines, :] = half[:, lanes_of(jb)].astype(f32)
                right_wide[lines, :] = right_part[:, lanes_of(2 * s + jb)]
        left_site = left_wide[...]
        right_site = right_wide[...]
        if not halved:
            msg[b] = jnp.where(is_right, left_site, right_site).astype(bf16)
        elif b + 1 < BATCH:
            lines = slice(b * 4 * SIZE, (b + 1) * 4 * SIZE)
            msg[lines, :] = jnp.where(is_right, left_site, right_site).astype(bf16)
        else:
            for jb in range(2):
                lines = slice((12 + jb) * SIZE, (13 + jb) * SIZE)
                half = scaled[b, UPPER, lanes_of(jb)].astype(f32)
                msg[lines, :] = jnp.where(is_right, half, right_part[:, lanes_of(jb)]).astype(bf16)
        ready[b] = jnp.where(is_right, right_site, left_site).astype(bf16)
        copies.append(pltpu.make_async_copy(ready.at[b], out.at[role[1] + b], sems.at[b]))
        copies[-1].start()
    return copies


def windows(first, own, sketches, own_win, sketch, sems):
    count = own_win.shape[0]

    def own_copy(t):
        at = jnp.clip(first - 1 + t, 0, own.shape[0] - 1)
        return pltpu.make_async_copy(own.at[at], own_win.at[t], sems.at[t])

    sketch_copy = pltpu.make_async_copy(sketches.at[pl.ds(first, BATCH)], sketch, sems.at[count])
    return own_copy, sketch_copy


def early_kernel(role, gates, kept, own, got_0, got, scale, sketches, *refs):
    mixed, samp, gram, edge, own_low, left_w, right_w, wide, own_win, sketch, sems = refs
    own_copy, sketch_copy = windows(role[1], own, sketches, own_win, sketch, sems)
    for t in (1, 2, 3, 4, 5, 0):
        own_copy(t).start()
    sketch_copy.start()

    def step(t, loop):
        own_copy(t).wait()
        weigh(t, role, own_win.at[t], got.at[0], scale, left_w.at[t], right_w.at[t], wide)
        return loop

    def step_0(t, loop):
        own_copy(t).wait()
        weigh(t, role, own_win.at[t], got_0.at[t - 1], scale, left_w.at[t], right_w.at[t], wide)
        return loop

    lax.fori_loop(1, 4, step_0, 0)
    lax.fori_loop(4, 6, step, 0)
    for s in range(2):
        edge[s] = left_w[1, s]
        edge[2 + s] = right_w[1, s]
    edge[4] = right_w[2, 0]
    below = role[1] - 5
    wide[0] = got[0].astype(f32)
    rows = column_of(scale[1, below + 1])
    col = scale[2, below + 2]
    for jb in range(2):
        lanes = lanes_of(jb)
        edge[5, :, lanes] = ((wide[0, lines_of(jb, 1), :] * rows) * col[:, lanes]).astype(bf16)
    own_copy(0).wait()
    own_low[...] = own_win[0]
    sketch_copy.wait()
    edge[6] = sketch[0, UPPER]
    edge[7] = sketch[0, LOWER]
    for b in range(1, BATCH):
        t = b + 1
        sample(
            gates,
            kept[role[1] + b],
            sketch[b],
            (left_w[t, 0], left_w[t, 1]),
            (left_w[t - 1, 0], left_w[t - 1, 1]),
            (right_w[t, 0], right_w[t, 1]),
            right_w[t - 1, 1],
            right_w[t + 1, 0],
            mixed.at[b - 1],
            samp.at[b - 1],
            gram.at[b - 1],
        )


def first_kernel(role, gates, kept, got, scale, all_own, sketches, *refs):
    (mixed_e, samp_e, gram_e, edge, own), refs = refs[:5], refs[5:]
    (msg, out, carry, own_next, sketch_next), refs = refs[:5], refs[5:]
    mixed, samp, gram, scaled, a_ref, x_ref, wide, ready, sems, next_sems = refs
    own_copy, sketch_copy = windows(
        role[1] - BATCH, all_own, sketches, own_next, sketch_next, next_sems
    )
    for t in range(4):
        own_copy(t).start()
    sketch_copy.start()
    left, right = carry.at[pl.ds(1, 2)], carry.at[pl.ds(3, 2)]
    weigh(0, role, own, got.at[0], scale, left, right, wide)
    sample(
        gates,
        kept[role[1]],
        jnp.concatenate([edge[6], edge[7]], axis=0),
        (edge[0], edge[1]),
        (left[0], left[1]),
        (edge[2], edge[3]),
        right[1],
        edge[4],
        mixed,
        samp,
        gram,
    )
    mixed = [mixed] + [mixed_e.at[b] for b in range(BATCH - 1)]
    samp = [samp] + [samp_e.at[b] for b in range(BATCH - 1)]
    gram = [gram] + [gram_e.at[b] for b in range(BATCH - 1)]
    solve(gram, samp, scaled, a_ref, x_ref)
    scaled[BATCH, LOWER, :] = jnp.zeros((SIZE, SIZE), bf16)
    carry[0] = scaled[0, LOWER, :]
    for copy in deliver(role, scaled, mixed, wide, ready, msg, out, sems, True):
        copy.wait()
    for t in range(4):
        own_copy(t).wait()
    sketch_copy.wait()


def second_kernel(role, gates, kept, own, got, scale, sketch, *refs):
    (edge, carry, _, msg, out, merge), refs = refs[:6], refs[6:]
    left_w, right_w, mixed, samp, gram, scaled, a_ref, x_ref, wide = refs[:9]
    ready, sems = refs[9:]

    def step(t, loop):
        at = jnp.maximum(t - 1, 0)
        weigh(t, role, own.at[t], got.at[at], scale, left_w.at[t], right_w.at[t], wide)
        return loop

    lax.fori_loop(0, 4, step, 0)
    right_w[0, 1] = edge[5]
    for s in range(2):
        left_w[4, s] = carry[1 + s]
        right_w[4, s] = carry[3 + s]
    right_w[5, 0] = edge[2]
    for b in range(BATCH):
        t = b + 1
        sample(
            gates,
            kept[role[1] + b],
            sketch[b],
            (left_w[t, 0], left_w[t, 1]),
            (left_w[b, 0], left_w[b, 1]),
            (right_w[t, 0], right_w[t, 1]),
            right_w[b, 1],
            right_w[t + 1, 0],
            mixed.at[b],
            samp.at[b],
            gram.at[b],
        )
    every = range(BATCH)
    solve([gram.at[b] for b in every], [samp.at[b] for b in every], scaled, a_ref, x_ref)
    scaled[BATCH, LOWER, :] = carry[0]
    copies = deliver(
        role, scaled, [mixed.at[b] for b in every], wide, ready, msg, out, sems, False
    )
    used = jnp.where(role[0] == 1, 0.0, 1.0)
    for jb in range(2):
        value = scaled[0, LOWER, lanes_of(jb)].astype(f32)
        wide[0, lines_of(jb, 0), :] = jnp.zeros((SIZE, LANES), f32)
        wide[0, lines_of(jb, 1), :] = value * used
    merge[...] = wide[0].astype(bf16)
    for copy in copies:
        copy.wait()


def in_hbm(x):
    return pltpu.with_memory_space_constraint(x, pltpu.HBM)


def shaped(*shape, dtype=bf16):
    return jax.ShapeDtypeStruct(shape, dtype)


def run(kernel, operands, specs, outs, out_specs, scratch, aliases=None, mib=20):
    return pl.pallas_call(
        kernel,
        out_shape=outs,
        in_specs=specs,
        out_specs=out_specs,
        scratch_shapes=scratch,
        input_output_aliases=aliases or {},
        compiler_params=pltpu.CompilerParams(vmem_limit_bytes=mib * 2**20),
        cost_estimate=pl.CostEstimate(
            flops=mib * 500_000_000, bytes_accessed=8_000_000, transcendentals=0
        ),
    )(*operands)


SMEM = pl.BlockSpec(memory_space=pltpu.SMEM)
VMEM = pl.BlockSpec(memory_space=pltpu.VMEM)
HBM = pl.BlockSpec(memory_space=pltpu.HBM)
SECTOR = (4 * SIZE, LANES)


def factor_scratch():
    return [
        pltpu.VMEM((BATCH + 1, 2 * SIZE, SIZE), bf16),
        pltpu.VMEM((PANELS, SIZE, LANES), f32),
        pltpu.VMEM((SIZE, PANELS * SIZE), bf16),
        pltpu.VMEM((4, *SECTOR), f32),
    ]


def sample_shapes(make, *lead):
    return [
        make((*lead, 2 * SIZE, 2 * SIZE), bf16),
        make((*lead, 2, 2 * SIZE, SIZE), bf16),
        make((*lead, SIZE, SIZE), f32),
    ]


def window_scratch(count):
    return [
        pltpu.VMEM((count, *SECTOR), bf16),
        pltpu.VMEM((BATCH, 2 * SIZE, SIZE), bf16),
        pltpu.SemaphoreType.DMA((count + 1,)),
    ]


def early(role, gates, kept, own, got_0, got, scale, sketches):
    return run(
        early_kernel,
        (role, gates, kept, in_hbm(own), got_0, got, scale, in_hbm(sketches)),
        [SMEM] * 3 + [HBM, VMEM, VMEM, VMEM, HBM],
        sample_shapes(jax.ShapeDtypeStruct, BATCH - 1) + [shaped(8, SIZE, SIZE), shaped(*SECTOR)],
        [VMEM] * 5,
        [
            pltpu.VMEM((6, 2, SIZE, SIZE), bf16),
            pltpu.VMEM((6, 2, SIZE, SIZE), bf16),
            pltpu.VMEM((2, *SECTOR), f32),
        ]
        + window_scratch(6),
    )


def first_half(role, gates, kept, got, scale, own, sketches, parts):
    return run(
        first_kernel,
        (role, gates, kept, got, scale, in_hbm(own), in_hbm(sketches), *parts),
        [SMEM] * 3 + [VMEM, VMEM, HBM, HBM] + [VMEM] * 5,
        [
            shaped(14 * SIZE, LANES),
            pltpu.HBM((16, *SECTOR), bf16),
            shaped(5, SIZE, SIZE),
            shaped(4, *SECTOR),
            shaped(BATCH, 2 * SIZE, SIZE),
        ],
        [VMEM, HBM, VMEM, VMEM, VMEM],
        sample_shapes(pltpu.VMEM)
        + factor_scratch()
        + [
            pltpu.VMEM((BATCH, *SECTOR), bf16),
            pltpu.SemaphoreType.DMA((BATCH,)),
            pltpu.SemaphoreType.DMA((5,)),
        ],
    )


def second_half(role, gates, kept, own, got, scale, sketch, edge, carry, out):
    return run(
        second_kernel,
        (role, gates, kept, own, got, scale, sketch, edge, carry, out),
        [SMEM] * 3 + [VMEM] * 6 + [HBM],
        [shaped(BATCH, *SECTOR), pltpu.HBM((16, *SECTOR), bf16), shaped(*SECTOR)],
        [VMEM, HBM, VMEM],
        [pltpu.VMEM((6, 2, SIZE, SIZE), bf16), pltpu.VMEM((6, 2, SIZE, SIZE), bf16)]
        + sample_shapes(pltpu.VMEM, BATCH)
        + factor_scratch()
        + [
            pltpu.VMEM((BATCH, *SECTOR), bf16),
            pltpu.SemaphoreType.DMA((BATCH,)),
        ],
        aliases={9: 1},
    )


def fetch_kernel(at, own, out, sem):
    copy = pltpu.make_async_copy(own.at[pl.ds(at[0], out.shape[0])], out, sem)
    copy.start()
    copy.wait()


def fetch(at, own):
    return run(
        fetch_kernel,
        (jnp.reshape(at, (1,)), in_hbm(own)),
        [SMEM, HBM],
        [shaped(3, *SECTOR)],
        [VMEM],
        [pltpu.SemaphoreType.DMA],
        mib=1,
    )[0]


def pack_kernel(role, own, out, low, rest, both, sems):
    flag = role[0]
    copies = [
        pltpu.make_async_copy(own.at[7 + 8 * flag], both.at[0], sems.at[0]),
        pltpu.make_async_copy(own.at[7], both.at[1], sems.at[1]),
        pltpu.make_async_copy(own.at[3 + 8 * flag], low.at[0], sems.at[2]),
        pltpu.make_async_copy(own.at[pl.ds(8 * flag, 3)], rest, sems.at[3]),
    ]
    for copy in copies:
        copy.start()
    copies[0].wait()
    copies[1].wait()
    is_odd = lax.broadcasted_iota(jnp.int32, SECTOR, 0) % 2 == 1
    out[0] = jnp.where(is_odd, both[1].astype(f32), both[0].astype(f32)).astype(bf16)
    copies[2].wait()
    copies[3].wait()


def pack(role, own):
    return run(
        pack_kernel,
        (role, in_hbm(own)),
        [SMEM, HBM],
        [shaped(1, *SECTOR), shaped(1, *SECTOR), shaped(3, *SECTOR)],
        [VMEM] * 3,
        [pltpu.VMEM((2, *SECTOR), bf16), pltpu.SemaphoreType.DMA((4,))],
        mib=2,
    )


def place_kernel(at, block, _, out, sems):
    copies = []
    for b in range(block.shape[0]):
        copies.append(pltpu.make_async_copy(block.at[b], out.at[at[0] + b], sems.at[b]))
        copies[-1].start()
    for copy in copies:
        copy.wait()


def place_halved_kernel(at, block, merge, _, out, last, wide, sems):
    copies = []
    for b in range(3):
        lines = pl.ds(b * 4 * SIZE, 4 * SIZE)
        copies.append(pltpu.make_async_copy(block.at[lines], out.at[at[0] + b], sems.at[b]))
        copies[-1].start()
    for jb in range(2):
        half = block[(12 + jb) * SIZE : (13 + jb) * SIZE, :]
        wide[lines_of(jb, 0), :] = half.astype(f32)
        wide[lines_of(jb, 1), :] = jnp.zeros((SIZE, LANES), f32)
    last[...] = (wide[...] + merge[...].astype(f32)).astype(bf16)
    copies.append(pltpu.make_async_copy(last, out.at[at[0] + 3], sems.at[3]))
    copies[-1].start()
    for copy in copies:
        copy.wait()


def place(out, block, at, merge=None):
    operands = (jnp.reshape(at, (1,)), block) + (() if merge is None else (merge,)) + (out,)
    scratch = [pltpu.VMEM(SECTOR, bf16), pltpu.VMEM(SECTOR, f32)] if merge is not None else []
    return run(
        place_kernel if merge is None else place_halved_kernel,
        operands,
        [SMEM] + [VMEM] * (len(operands) - 2) + [HBM],
        [pltpu.HBM(out.shape, out.dtype)],
        [HBM],
        scratch + [pltpu.SemaphoreType.DMA((4,))],
        aliases={len(operands) - 1: 0},
        mib=4,
    )[0]


def to_lines(x):
    n = x.shape[0]
    return x.reshape(n, SIZE, 2, 2, LANES).transpose(0, 1, 3, 2, 4).reshape(n, 4 * SIZE, LANES)


def from_lines(x):
    n = x.shape[0]
    return x.reshape(n, SIZE, 2, 2, LANES).transpose(0, 1, 3, 2, 4).reshape(n, SIZE, 2, SIZE)


def shards(site_tensors, bond_weights, sector_sizes, kept_ranks, sketches, gate_ends, gate_pair):
    chain = lax.axis_size("chain")
    count = lax.axis_size("group") * chain
    site = lax.axis_index("group") * chain + lax.axis_index("chain")
    is_right = site % 2 == 1

    def swapped(value):
        return lax.ppermute(value, "chain", [(i, i ^ 1) for i in range(chain)])

    def onward(value):
        def place(n):
            return n % chain * (count // chain) + n // chain

        pairs = [(place(i), place(i + 1)) for i in range(1, count - 1, 2)]
        return lax.ppermute(value, ("chain", "group"), pairs)

    own = to_lines(site_tensors[0, 0])
    sectors = own.shape[0]
    flag = is_right.astype(jnp.int32)

    got_0 = swapped(fetch(4 + 8 * flag, own))
    column = lax.broadcasted_iota(jnp.int32, (sectors, SIZE), 1)
    lam = bond_weights[0, 0] * (column < sector_sizes[0, 0][:, None]).astype(f32)
    before = onward(lam)
    before = jnp.where(site < 2, jnp.ones_like(lam), before)
    kept_line = jnp.pad(kept_ranks[0, 0].astype(f32)[None, :], ((0, 7), (0, SIZE - sectors)))
    packed = jnp.concatenate([lam, before, kept_line], axis=0)
    other = swapped(packed)
    outgoing, outgoing_low, outgoing_b = pack(jnp.reshape(flag, (1,)), own)
    got_a = swapped(outgoing)
    got_low = swapped(outgoing_low)
    lam_prev = jnp.where(is_right, other[sectors : 2 * sectors], before)
    lam_mid = jnp.where(is_right, other[:sectors], lam)
    lam_next = jnp.where(is_right, lam, other[:sectors])
    scale = jnp.pad(jnp.stack([lam_prev, lam_mid, lam_next]), ((0, 0), (1, 7), (0, 0)))
    scale = scale[:, :, None, :]
    kept = jnp.where(is_right, other[2 * sectors, :sectors], packed[2 * sectors, :sectors])
    kept = kept.astype(jnp.int32)
    got_b = swapped(outgoing_b)
    gates = jnp.concatenate([gate_ends, 1.0 + gate_pair[:2], gate_pair[2:]])
    first_a = 12 - 8 * flag
    first_b = 8 - 8 * flag
    role_a = jnp.stack([flag, first_a])
    role_b = jnp.stack([flag, first_b])

    parts = early(role_a, gates, kept, own, got_0, got_a, scale, sketches)
    msg_a, out, carry, own_b, sketch_b = first_half(
        role_a, gates, kept, got_low, scale, own, sketches, parts
    )
    back_a = swapped(msg_a)
    msg_b, out, merge = second_half(
        role_b, gates, kept, own_b, got_b, scale, sketch_b, parts[3], carry, out
    )
    back_b = swapped(msg_b)

    back_at = 8 * flag
    out = place(out, back_a, back_at + 4, merge)
    out = place(out, back_b, back_at)
    return from_lines(out)[None, None]


def solution(mesh):
    return jax.shard_map(
        shards,
        mesh=mesh,
        in_specs=(
            P("group", "chain", None, None, None, None),
            P("group", "chain", None, None),
            P("group", "chain", None),
            P("group", "chain", None),
            P(),
            P(),
            P(),
        ),
        out_specs=P("group", "chain", None, None, None, None),
        check_vma=False,
    )
```

```python
import jax
import jax.numpy as jnp
from jax import lax
from jax.experimental import pallas as pl
from jax.experimental.pallas import tpu as pltpu
from jax.sharding import PartitionSpec as P

f32 = jnp.float32
bf16 = jnp.bfloat16


BATCH = 4
LEAF = 32
PANELS = 8
LANES = 128
SIZE = 256


def split(x):
    high = x.astype(bf16)
    return high, (x - high.astype(f32)).astype(bf16)


def invert_leaf(d):
    lane = lax.broadcasted_iota(jnp.int32, (8, LANES), 1)
    sub = lax.broadcasted_iota(jnp.int32, (8, LANES), 0)
    segment = (lane // LEAF) * LEAF
    tiles = LEAF // 8
    rows = [d[8 * t : 8 * t + 8, :] for t in range(tiles)]
    cols = [
        [
            jnp.take_along_axis(rows[t], segment + j, axis=1) if t >= j // 8 else None
            for t in range(tiles)
        ]
        for j in range(LEAF)
    ]
    inverse = [((lane - segment) == (sub + 8 * t)).astype(f32) for t in range(tiles)]
    pivots = [jnp.ones((8, LANES), f32) for _ in range(tiles)]

    def row(v, r):
        return jnp.broadcast_to(v[r : r + 1, :], (8, LANES))

    for j in range(LEAF):
        top, r = j // 8, j % 8
        pivot = row(cols[j][top], r)
        reciprocal = 1.0 / pivot
        pivots[top] = jnp.where(sub == r, pivot, pivots[top])
        scaled = {t: cols[j][t] * reciprocal for t in range(top, tiles)}
        for i in range(j + 1, LEAF):
            factor = row(scaled[i // 8], i % 8)
            for t in range(i // 8, tiles):
                cols[i][t] = cols[i][t] - factor * cols[j][t]
        source = row(inverse[top], r)
        for t in range(top, tiles):
            factor = jnp.where(sub > r, scaled[t], 0.0) if t == top else scaled[t]
            inverse[t] = inverse[t] - factor * source
    return jnp.concatenate([inverse[t] * lax.rsqrt(pivots[t]) for t in range(tiles)], axis=0)


def block_weights(high, low, masks):
    high = jnp.concatenate([high * mask for mask in masks], axis=0)
    low = jnp.concatenate([low * mask for mask in masks], axis=0)
    upper = jnp.concatenate([high, high], axis=1)
    lower = jnp.concatenate([low, jnp.zeros_like(low)], axis=1)
    return jnp.concatenate([upper, lower], axis=0)


def times_transposed(x, weights):
    out = lax.dot_general(x, weights, (((1,), (1,)), ((), ())), preferred_element_type=f32)
    return out[:, :LANES] + out[:, LANES:]


def invert_factor(a_ref, x_ref):
    lane = lax.broadcasted_iota(jnp.int32, (LEAF, LANES), 1)
    sub = lax.broadcasted_iota(jnp.int32, (LEAF, LANES), 0)
    eye = ((lane % LEAF) == sub).astype(f32)
    masks = [((lane // LEAF) == b).astype(f32).astype(bf16) for b in range(BATCH)]

    def weights_of(rows, ks):
        return jnp.concatenate(
            [
                block_weights(
                    x_ref[rows, k * SIZE : k * SIZE + LANES],
                    x_ref[rows, k * SIZE + LANES : (k + 1) * SIZE],
                    masks,
                )
                for k in ks
            ],
            axis=1,
        )

    partial = None
    for j in range(PANELS):
        start = j * LEAF
        block = slice(start, start + LEAF)
        col = a_ref[j]
        if j:
            last = slice((j - 1) * SIZE, j * SIZE)
            if partial is not None:
                col = col - partial
            col = col - times_transposed(x_ref[:, last], weights_of(block, [j - 1]))
            x_ref[block, : j * SIZE] = jnp.zeros((LEAF, j * SIZE), bf16)
            if j < PANELS - 1:
                following = slice(start + LEAF, start + 2 * LEAF)
                partial = times_transposed(
                    x_ref[:, : j * SIZE], weights_of(following, range(j))
                )
        inverse = invert_leaf(col[block])
        col = jnp.concatenate(
            [part for part in (col[:start], eye, col[start + LEAF :]) if part.shape[0]], axis=0
        )
        col = times_transposed(
            jnp.concatenate(split(col), axis=1), block_weights(*split(inverse), masks)
        )
        x_ref[:, j * SIZE : (j + 1) * SIZE] = jnp.concatenate(split(col), axis=1)


UPPER, LOWER = slice(0, SIZE), slice(SIZE, 2 * SIZE)
CONTRACT_ROWS = (((0,), (0,)), ((), ()))


def dot(a, b):
    return jnp.dot(a, b, preferred_element_type=f32)


def lines_of(lane_block, s):
    return pl.ds(2 * lane_block + s, SIZE, stride=4)


def lanes_of(lane_block):
    return slice(lane_block * LANES, (lane_block + 1) * LANES)


def column_of(line):
    return jnp.transpose(jnp.broadcast_to(line, (LANES, SIZE)))


def weigh(t, role, own, got, scale, left, right, wide):
    is_right = role[0] == 1
    q = role[1] - 1 + t
    own_wide = own[...].astype(f32)
    got_wide = got[...].astype(f32)
    wide[0] = jnp.where(is_right, got_wide, own_wide)
    wide[1] = jnp.where(is_right, own_wide, got_wide)
    left_rows = column_of(scale[0, q + 1])
    right_rows = column_of(scale[1, q + 1])
    for s in range(2):
        col = scale[2, q + s + 1]
        for jb in range(2):
            lines, lanes = lines_of(jb, s), lanes_of(jb)
            left[s, :, lanes] = (wide[0, lines, :] * left_rows).astype(bf16)
            right[s, :, lanes] = ((wide[1, lines, :] * right_rows) * col[:, lanes]).astype(bf16)


def sample(gates, kept, sketch, left, before, right, right_before, right_after, mixed, samp, gram):
    g0, g1, p0, p1, p2 = [gates[i] for i in range(5)]
    mixed[UPPER, UPPER] = (g0 * dot(left[0], right[0])).astype(bf16)
    mixed[UPPER, LOWER] = (p0 * dot(left[0], right[1]) + p2 * dot(left[1], right_after)).astype(bf16)
    mixed[LOWER, UPPER] = (
        p2 * dot(before[0], right_before) + p1 * dot(before[1], right[0])
    ).astype(bf16)
    mixed[LOWER, LOWER] = (g1 * dot(before[1], right[1])).astype(bf16)
    keep = lax.broadcasted_iota(jnp.int32, (1, SIZE), 1) < kept
    sampled = jnp.where(keep, dot(mixed[...], sketch), 0.0)
    high, low = split(sampled)
    samp[0] = high
    samp[1] = low
    shift = 0.01 * jnp.sum(sampled * sampled) / SIZE
    hh = lax.dot_general(high, high, CONTRACT_ROWS, preferred_element_type=f32)
    hl = lax.dot_general(high, low, CONTRACT_ROWS, preferred_element_type=f32)
    rows = lax.broadcasted_iota(jnp.int32, (SIZE, SIZE), 0)
    eye = rows == lax.broadcasted_iota(jnp.int32, (SIZE, SIZE), 1)
    added = jnp.where(keep, 0.0, 1.0) + shift
    gram[...] = (hh + (hl + jnp.transpose(hl))) + jnp.where(eye, added, 0.0)


def rolled(value, segments):
    shift = (segments * LEAF) % LANES
    return pltpu.roll(value, shift, axis=1) if shift else value


def gather_lanes(pieces):
    segment = lax.broadcasted_iota(jnp.int32, (1, LANES), 1) // LEAF
    out = pieces[0]
    for i in range(1, BATCH):
        out = jnp.where(segment == i, pieces[i], out)
    return out


def solve(gram, samp, scaled, a_ref, x_ref):
    for k in range(PANELS):
        rows = slice(k * LEAF, SIZE)
        lanes = lanes_of(k // 4)
        a_ref[k, rows, :] = gather_lanes(
            [rolled(gram[b][rows, lanes], b - k % 4) for b in range(BATCH)]
        )
        if k:
            a_ref[k, : k * LEAF, :] = jnp.zeros((k * LEAF, LANES), f32)

    invert_factor(a_ref, x_ref)

    def factor(b, offset):
        halves = []
        for g in range(2):
            panels = [
                rolled(x_ref[:, k * SIZE + offset : k * SIZE + offset + LANES], k % 4 - b)
                for k in range(4 * g, 4 * g + 4)
            ]
            halves.append(gather_lanes(panels))
        return jnp.concatenate(halves, axis=1)

    for b in range(BATCH):
        high, low = factor(b, 0), factor(b, LANES)
        solved = dot(samp[b][0], high) + (dot(samp[b][0], low) + dot(samp[b][1], high))
        scaled[b] = (solved * 16.0).astype(bf16)


def deliver(role, scaled, mixed, wide, ready, msg, out, sems, halved):
    is_right = role[0] == 1
    copies = []
    for b in range(BATCH):
        right_part = lax.dot_general(
            scaled[b], mixed[b][...], CONTRACT_ROWS, preferred_element_type=f32
        ) * (1.0 / SIZE)
        left_wide, right_wide = wide.at[2 * (b % 2)], wide.at[2 * (b % 2) + 1]
        for s in range(2):
            half = scaled[b, UPPER, :] if s == 0 else scaled[b + 1, LOWER, :]
            for jb in range(2):
                lines = lines_of(jb, s)
                left_wide[lines, :] = half[:, lanes_of(jb)].astype(f32)
                right_wide[lines, :] = right_part[:, lanes_of(2 * s + jb)]
        left_site = left_wide[...]
        right_site = right_wide[...]
        if not halved:
            msg[b] = jnp.where(is_right, left_site, right_site).astype(bf16)
        elif b + 1 < BATCH:
            lines = slice(b * 4 * SIZE, (b + 1) * 4 * SIZE)
            msg[lines, :] = jnp.where(is_right, left_site, right_site).astype(bf16)
        else:
            for jb in range(2):
                lines = slice((12 + jb) * SIZE, (13 + jb) * SIZE)
                half = scaled[b, UPPER, lanes_of(jb)].astype(f32)
                msg[lines, :] = jnp.where(is_right, half, right_part[:, lanes_of(jb)]).astype(bf16)
        ready[b] = jnp.where(is_right, right_site, left_site).astype(bf16)
        copies.append(pltpu.make_async_copy(ready.at[b], out.at[role[1] + b], sems.at[b]))
        copies[-1].start()
    return copies


def windows(first, own, sketches, own_win, sketch, sems):
    count = own_win.shape[0]

    def own_copy(t):
        at = jnp.clip(first - 1 + t, 0, own.shape[0] - 1)
        return pltpu.make_async_copy(own.at[at], own_win.at[t], sems.at[t])

    sketch_copy = pltpu.make_async_copy(sketches.at[pl.ds(first, BATCH)], sketch, sems.at[count])
    return own_copy, sketch_copy


def early_kernel(role, gates, kept, own, got_0, got, scale, sketch, *refs):
    mixed, samp, gram, edge, left_w, right_w, wide = refs

    def step(t, loop):
        weigh(t, role, own.at[t], got.at[0], scale, left_w.at[t], right_w.at[t], wide)
        return loop

    def step_0(t, loop):
        weigh(t, role, own.at[t], got_0.at[t - 1], scale, left_w.at[t], right_w.at[t], wide)
        return loop

    lax.fori_loop(1, 4, step_0, 0)
    lax.fori_loop(4, 6, step, 0)
    for s in range(2):
        edge[s] = left_w[1, s]
        edge[2 + s] = right_w[1, s]
    edge[4] = right_w[2, 0]
    below = role[1] - 5
    wide[0] = got[0].astype(f32)
    rows = column_of(scale[1, below + 1])
    col = scale[2, below + 2]
    for jb in range(2):
        lanes = lanes_of(jb)
        edge[5, :, lanes] = ((wide[0, lines_of(jb, 1), :] * rows) * col[:, lanes]).astype(bf16)
    for b in range(1, BATCH):
        t = b + 1
        sample(
            gates,
            kept[role[1] + b],
            sketch[b],
            (left_w[t, 0], left_w[t, 1]),
            (left_w[t - 1, 0], left_w[t - 1, 1]),
            (right_w[t, 0], right_w[t, 1]),
            right_w[t - 1, 1],
            right_w[t + 1, 0],
            mixed.at[b - 1],
            samp.at[b - 1],
            gram.at[b - 1],
        )


def first_kernel(role, gates, kept, own, got, scale, sketch, *refs):
    (mixed_e, samp_e, gram_e, edge, msg, out, carry), refs = refs[:7], refs[7:]
    mixed, samp, gram, scaled, a_ref, x_ref, wide, ready, sems = refs
    left, right = carry.at[pl.ds(1, 2)], carry.at[pl.ds(3, 2)]
    weigh(0, role, own.at[0], got.at[0], scale, left, right, wide)
    sample(
        gates,
        kept[role[1]],
        sketch[0],
        (edge[0], edge[1]),
        (left[0], left[1]),
        (edge[2], edge[3]),
        right[1],
        edge[4],
        mixed,
        samp,
        gram,
    )
    mixed = [mixed] + [mixed_e.at[b] for b in range(BATCH - 1)]
    samp = [samp] + [samp_e.at[b] for b in range(BATCH - 1)]
    gram = [gram] + [gram_e.at[b] for b in range(BATCH - 1)]
    solve(gram, samp, scaled, a_ref, x_ref)
    scaled[BATCH, LOWER, :] = jnp.zeros((SIZE, SIZE), bf16)
    carry[0] = scaled[0, LOWER, :]
    for copy in deliver(role, scaled, mixed, wide, ready, msg, out, sems, True):
        copy.wait()


def second_kernel(role, gates, kept, own, got, scale, sketch, *refs):
    (edge, carry, _, msg, out, merge), refs = refs[:6], refs[6:]
    left_w, right_w, mixed, samp, gram, scaled, a_ref, x_ref, wide = refs[:9]
    ready, sems = refs[9:]

    def step(t, loop):
        at = jnp.maximum(t - 1, 0)
        weigh(t, role, own.at[t], got.at[at], scale, left_w.at[t], right_w.at[t], wide)
        return loop

    lax.fori_loop(0, 4, step, 0)
    right_w[0, 1] = edge[5]
    for s in range(2):
        left_w[4, s] = carry[1 + s]
        right_w[4, s] = carry[3 + s]
    right_w[5, 0] = edge[2]
    for b in range(BATCH):
        t = b + 1
        sample(
            gates,
            kept[role[1] + b],
            sketch[b],
            (left_w[t, 0], left_w[t, 1]),
            (left_w[b, 0], left_w[b, 1]),
            (right_w[t, 0], right_w[t, 1]),
            right_w[b, 1],
            right_w[t + 1, 0],
            mixed.at[b],
            samp.at[b],
            gram.at[b],
        )
    every = range(BATCH)
    solve([gram.at[b] for b in every], [samp.at[b] for b in every], scaled, a_ref, x_ref)
    scaled[BATCH, LOWER, :] = carry[0]
    copies = deliver(
        role, scaled, [mixed.at[b] for b in every], wide, ready, msg, out, sems, False
    )
    used = jnp.where(role[0] == 1, 0.0, 1.0)
    for jb in range(2):
        value = scaled[0, LOWER, lanes_of(jb)].astype(f32)
        wide[0, lines_of(jb, 0), :] = jnp.zeros((SIZE, LANES), f32)
        wide[0, lines_of(jb, 1), :] = value * used
    merge[...] = wide[0].astype(bf16)
    for copy in copies:
        copy.wait()


def in_hbm(x):
    return pltpu.with_memory_space_constraint(x, pltpu.HBM)


def shaped(*shape, dtype=bf16):
    return jax.ShapeDtypeStruct(shape, dtype)


def run(kernel, operands, specs, outs, out_specs, scratch, aliases=None, mib=20):
    return pl.pallas_call(
        kernel,
        out_shape=outs,
        in_specs=specs,
        out_specs=out_specs,
        scratch_shapes=scratch,
        input_output_aliases=aliases or {},
        compiler_params=pltpu.CompilerParams(vmem_limit_bytes=mib * 2**20),
        cost_estimate=pl.CostEstimate(
            flops=mib * 500_000_000, bytes_accessed=8_000_000, transcendentals=0
        ),
    )(*operands)


SMEM = pl.BlockSpec(memory_space=pltpu.SMEM)
VMEM = pl.BlockSpec(memory_space=pltpu.VMEM)
HBM = pl.BlockSpec(memory_space=pltpu.HBM)
SECTOR = (4 * SIZE, LANES)


def factor_scratch():
    return [
        pltpu.VMEM((BATCH + 1, 2 * SIZE, SIZE), bf16),
        pltpu.VMEM((PANELS, SIZE, LANES), f32),
        pltpu.VMEM((SIZE, PANELS * SIZE), bf16),
        pltpu.VMEM((4, *SECTOR), f32),
    ]


def sample_shapes(make, *lead):
    return [
        make((*lead, 2 * SIZE, 2 * SIZE), bf16),
        make((*lead, 2, 2 * SIZE, SIZE), bf16),
        make((*lead, SIZE, SIZE), f32),
    ]


def early(role, gates, kept, own, got_0, got, scale, sketch):
    return run(
        early_kernel,
        (role, gates, kept, own, got_0, got, scale, sketch),
        [SMEM] * 3 + [VMEM] * 5,
        sample_shapes(jax.ShapeDtypeStruct, BATCH - 1) + [shaped(6, SIZE, SIZE)],
        [VMEM] * 4,
        [
            pltpu.VMEM((6, 2, SIZE, SIZE), bf16),
            pltpu.VMEM((6, 2, SIZE, SIZE), bf16),
            pltpu.VMEM((2, *SECTOR), f32),
        ],
    )


def first_half(role, gates, kept, own, got, scale, sketch, parts):
    return run(
        first_kernel,
        (role, gates, kept, own, got, scale, sketch, *parts),
        [SMEM] * 3 + [VMEM] * 8,
        [shaped(14 * SIZE, LANES), pltpu.HBM((16, *SECTOR), bf16), shaped(5, SIZE, SIZE)],
        [VMEM, HBM, VMEM],
        sample_shapes(pltpu.VMEM)
        + factor_scratch()
        + [pltpu.VMEM((BATCH, *SECTOR), bf16), pltpu.SemaphoreType.DMA((BATCH,))],
    )


def second_half(role, gates, kept, own, got, scale, sketch, edge, carry, out):
    return run(
        second_kernel,
        (role, gates, kept, own, got, scale, sketch, edge, carry, out),
        [SMEM] * 3 + [VMEM] * 6 + [HBM],
        [shaped(BATCH, *SECTOR), pltpu.HBM((16, *SECTOR), bf16), shaped(*SECTOR)],
        [VMEM, HBM, VMEM],
        [pltpu.VMEM((6, 2, SIZE, SIZE), bf16), pltpu.VMEM((6, 2, SIZE, SIZE), bf16)]
        + sample_shapes(pltpu.VMEM, BATCH)
        + factor_scratch()
        + [
            pltpu.VMEM((BATCH, *SECTOR), bf16),
            pltpu.SemaphoreType.DMA((BATCH,)),
        ],
        aliases={9: 1},
    )


def fetch_kernel(at, own, out, sem):
    copy = pltpu.make_async_copy(own.at[pl.ds(at[0], out.shape[0])], out, sem)
    copy.start()
    copy.wait()


def fetch(at, own):
    return run(
        fetch_kernel,
        (jnp.reshape(at, (1,)), in_hbm(own)),
        [SMEM, HBM],
        [shaped(3, *SECTOR)],
        [VMEM],
        [pltpu.SemaphoreType.DMA],
        mib=1,
    )[0]


def pack_kernel(role, own, sketches, out, low, rest, *refs):
    own_a, sketch_a, own_b, sketch_b, both, sems, sems_a, sems_b = refs
    flag = role[0]
    copies = [
        pltpu.make_async_copy(own.at[7 + 8 * flag], both.at[0], sems.at[0]),
        pltpu.make_async_copy(own.at[7], both.at[1], sems.at[1]),
        pltpu.make_async_copy(own.at[3 + 8 * flag], low.at[0], sems.at[2]),
        pltpu.make_async_copy(own.at[pl.ds(8 * flag, 3)], rest, sems.at[3]),
    ]
    first = 12 - 8 * flag
    for start, own_win, sketch, win_sems in (
        (first, own_a, sketch_a, sems_a),
        (first - BATCH, own_b, sketch_b, sems_b),
    ):
        own_copy, sketch_copy = windows(start, own, sketches, own_win, sketch, win_sems)
        copies += [own_copy(t) for t in range(own_win.shape[0])] + [sketch_copy]
    for copy in copies:
        copy.start()
    copies[0].wait()
    copies[1].wait()
    is_odd = lax.broadcasted_iota(jnp.int32, SECTOR, 0) % 2 == 1
    out[0] = jnp.where(is_odd, both[1].astype(f32), both[0].astype(f32)).astype(bf16)
    for copy in copies[2:]:
        copy.wait()


def pack(role, own, sketches):
    sketch = shaped(BATCH, 2 * SIZE, SIZE)
    return run(
        pack_kernel,
        (role, in_hbm(own), in_hbm(sketches)),
        [SMEM, HBM, HBM],
        [shaped(count, *SECTOR) for count in (1, 1, 3)]
        + [shaped(6, *SECTOR), sketch, shaped(4, *SECTOR), sketch],
        [VMEM] * 7,
        [
            pltpu.VMEM((2, *SECTOR), bf16),
            pltpu.SemaphoreType.DMA((4,)),
            pltpu.SemaphoreType.DMA((7,)),
            pltpu.SemaphoreType.DMA((5,)),
        ],
        mib=2,
    )


def place_kernel(at, block, _, out, sems):
    copies = []
    for b in range(block.shape[0]):
        copies.append(pltpu.make_async_copy(block.at[b], out.at[at[0] + b], sems.at[b]))
        copies[-1].start()
    for copy in copies:
        copy.wait()


def place_halved_kernel(at, block, merge, _, out, last, wide, sems):
    copies = []
    for b in range(3):
        lines = pl.ds(b * 4 * SIZE, 4 * SIZE)
        copies.append(pltpu.make_async_copy(block.at[lines], out.at[at[0] + b], sems.at[b]))
        copies[-1].start()
    for jb in range(2):
        half = block[(12 + jb) * SIZE : (13 + jb) * SIZE, :]
        wide[lines_of(jb, 0), :] = half.astype(f32)
        wide[lines_of(jb, 1), :] = jnp.zeros((SIZE, LANES), f32)
    last[...] = (wide[...] + merge[...].astype(f32)).astype(bf16)
    copies.append(pltpu.make_async_copy(last, out.at[at[0] + 3], sems.at[3]))
    copies[-1].start()
    for copy in copies:
        copy.wait()


def place(out, block, at, merge=None):
    operands = (jnp.reshape(at, (1,)), block) + (() if merge is None else (merge,)) + (out,)
    scratch = [pltpu.VMEM(SECTOR, bf16), pltpu.VMEM(SECTOR, f32)] if merge is not None else []
    return run(
        place_kernel if merge is None else place_halved_kernel,
        operands,
        [SMEM] + [VMEM] * (len(operands) - 2) + [HBM],
        [pltpu.HBM(out.shape, out.dtype)],
        [HBM],
        scratch + [pltpu.SemaphoreType.DMA((4,))],
        aliases={len(operands) - 1: 0},
        mib=4,
    )[0]


def to_lines(x):
    n = x.shape[0]
    return x.reshape(n, SIZE, 2, 2, LANES).transpose(0, 1, 3, 2, 4).reshape(n, 4 * SIZE, LANES)


def from_lines(x):
    n = x.shape[0]
    return x.reshape(n, SIZE, 2, 2, LANES).transpose(0, 1, 3, 2, 4).reshape(n, SIZE, 2, SIZE)


def shards(site_tensors, bond_weights, sector_sizes, kept_ranks, sketches, gate_ends, gate_pair):
    chain = lax.axis_size("chain")
    count = lax.axis_size("group") * chain
    site = lax.axis_index("group") * chain + lax.axis_index("chain")
    is_right = site % 2 == 1

    def swapped(value):
        return lax.ppermute(value, "chain", [(i, i ^ 1) for i in range(chain)])

    def onward(value):
        def place(n):
            return n % chain * (count // chain) + n // chain

        pairs = [(place(i), place(i + 1)) for i in range(1, count - 1, 2)]
        return lax.ppermute(value, ("chain", "group"), pairs)

    own = to_lines(site_tensors[0, 0])
    sectors = own.shape[0]
    flag = is_right.astype(jnp.int32)

    got_0 = swapped(fetch(4 + 8 * flag, own))
    column = lax.broadcasted_iota(jnp.int32, (sectors, SIZE), 1)
    lam = bond_weights[0, 0] * (column < sector_sizes[0, 0][:, None]).astype(f32)
    before = onward(lam)
    before = jnp.where(site < 2, jnp.ones_like(lam), before)
    kept_line = jnp.pad(kept_ranks[0, 0].astype(f32)[None, :], ((0, 7), (0, SIZE - sectors)))
    packed = jnp.concatenate([lam, before, kept_line], axis=0)
    other = swapped(packed)
    outgoing, outgoing_low, outgoing_b, own_a, sketch_a, own_b, sketch_b = pack(
        jnp.reshape(flag, (1,)), own, sketches
    )
    got_a = swapped(outgoing)
    got_low = swapped(outgoing_low)
    lam_prev = jnp.where(is_right, other[sectors : 2 * sectors], before)
    lam_mid = jnp.where(is_right, other[:sectors], lam)
    lam_next = jnp.where(is_right, lam, other[:sectors])
    scale = jnp.pad(jnp.stack([lam_prev, lam_mid, lam_next]), ((0, 0), (1, 7), (0, 0)))
    scale = scale[:, :, None, :]
    kept = jnp.where(is_right, other[2 * sectors, :sectors], packed[2 * sectors, :sectors])
    kept = kept.astype(jnp.int32)
    got_b = swapped(outgoing_b)
    gates = jnp.concatenate([gate_ends, 1.0 + gate_pair[:2], gate_pair[2:]])
    first_a = 12 - 8 * flag
    first_b = 8 - 8 * flag
    role_a = jnp.stack([flag, first_a])
    role_b = jnp.stack([flag, first_b])

    parts = early(role_a, gates, kept, own_a, got_0, got_a, scale, sketch_a)
    msg_a, out, carry = first_half(role_a, gates, kept, own_a, got_low, scale, sketch_a, parts)
    back_a = swapped(msg_a)
    msg_b, out, merge = second_half(
        role_b, gates, kept, own_b, got_b, scale, sketch_b, parts[3], carry, out
    )
    back_b = swapped(msg_b)

    back_at = 8 * flag
    out = place(out, back_a, back_at + 4, merge)
    out = place(out, back_b, back_at)
    return from_lines(out)[None, None]


def solution(mesh):
    return jax.shard_map(
        shards,
        mesh=mesh,
        in_specs=(
            P("group", "chain", None, None, None, None),
            P("group", "chain", None, None),
            P("group", "chain", None),
            P("group", "chain", None),
            P(),
            P(),
            P(),
        ),
        out_specs=P("group", "chain", None, None, None, None),
        check_vma=False,
    )
```

```python
import jax
import jax.numpy as jnp
from jax import lax
from jax.experimental import pallas as pl
from jax.experimental.pallas import tpu as pltpu
from jax.sharding import PartitionSpec as P

f32 = jnp.float32
bf16 = jnp.bfloat16


BATCH = 4
LEAF = 32
PANELS = 8
LANES = 128
SIZE = 256


def split(x):
    high = x.astype(bf16)
    return high, (x - high.astype(f32)).astype(bf16)


def invert_leaf(d):
    lane = lax.broadcasted_iota(jnp.int32, (8, LANES), 1)
    sub = lax.broadcasted_iota(jnp.int32, (8, LANES), 0)
    segment = (lane // LEAF) * LEAF
    tiles = LEAF // 8
    rows = [d[8 * t : 8 * t + 8, :] for t in range(tiles)]
    cols = [
        [
            jnp.take_along_axis(rows[t], segment + j, axis=1) if t >= j // 8 else None
            for t in range(tiles)
        ]
        for j in range(LEAF)
    ]
    inverse = [((lane - segment) == (sub + 8 * t)).astype(f32) for t in range(tiles)]
    pivots = [jnp.ones((8, LANES), f32) for _ in range(tiles)]

    def row(v, r):
        return jnp.broadcast_to(v[r : r + 1, :], (8, LANES))

    for j in range(LEAF):
        top, r = j // 8, j % 8
        pivot = row(cols[j][top], r)
        reciprocal = 1.0 / pivot
        pivots[top] = jnp.where(sub == r, pivot, pivots[top])
        scaled = {t: cols[j][t] * reciprocal for t in range(top, tiles)}
        for i in range(j + 1, LEAF):
            factor = row(scaled[i // 8], i % 8)
            for t in range(i // 8, tiles):
                cols[i][t] = cols[i][t] - factor * cols[j][t]
        source = row(inverse[top], r)
        for t in range(top, tiles):
            factor = jnp.where(sub > r, scaled[t], 0.0) if t == top else scaled[t]
            inverse[t] = inverse[t] - factor * source
    return jnp.concatenate([inverse[t] * lax.rsqrt(pivots[t]) for t in range(tiles)], axis=0)


def block_weights(high, low, masks):
    high = jnp.concatenate([high * mask for mask in masks], axis=0)
    low = jnp.concatenate([low * mask for mask in masks], axis=0)
    upper = jnp.concatenate([high, high], axis=1)
    lower = jnp.concatenate([low, jnp.zeros_like(low)], axis=1)
    return jnp.concatenate([upper, lower], axis=0)


def times_transposed(x, weights):
    out = lax.dot_general(x, weights, (((1,), (1,)), ((), ())), preferred_element_type=f32)
    return out[:, :LANES] + out[:, LANES:]


def invert_factor(a_ref, x_ref):
    lane = lax.broadcasted_iota(jnp.int32, (LEAF, LANES), 1)
    sub = lax.broadcasted_iota(jnp.int32, (LEAF, LANES), 0)
    eye = ((lane % LEAF) == sub).astype(f32)
    masks = [((lane // LEAF) == b).astype(f32).astype(bf16) for b in range(BATCH)]

    def weights_of(rows, ks):
        return jnp.concatenate(
            [
                block_weights(
                    x_ref[rows, k * SIZE : k * SIZE + LANES],
                    x_ref[rows, k * SIZE + LANES : (k + 1) * SIZE],
                    masks,
                )
                for k in ks
            ],
            axis=1,
        )

    partial = None
    for j in range(PANELS):
        start = j * LEAF
        block = slice(start, start + LEAF)
        col = a_ref[j]
        if j:
            last = slice((j - 1) * SIZE, j * SIZE)
            if partial is not None:
                col = col - partial
            col = col - times_transposed(x_ref[:, last], weights_of(block, [j - 1]))
            x_ref[block, : j * SIZE] = jnp.zeros((LEAF, j * SIZE), bf16)
            if j < PANELS - 1:
                following = slice(start + LEAF, start + 2 * LEAF)
                partial = times_transposed(
                    x_ref[:, : j * SIZE], weights_of(following, range(j))
                )
        inverse = invert_leaf(col[block])
        col = jnp.concatenate(
            [part for part in (col[:start], eye, col[start + LEAF :]) if part.shape[0]], axis=0
        )
        col = times_transposed(
            jnp.concatenate(split(col), axis=1), block_weights(*split(inverse), masks)
        )
        x_ref[:, j * SIZE : (j + 1) * SIZE] = jnp.concatenate(split(col), axis=1)


UPPER, LOWER = slice(0, SIZE), slice(SIZE, 2 * SIZE)
CONTRACT_ROWS = (((0,), (0,)), ((), ()))


def dot(a, b):
    return jnp.dot(a, b, preferred_element_type=f32)


def lines_of(lane_block, s):
    return pl.ds(2 * lane_block + s, SIZE, stride=4)


def lanes_of(lane_block):
    return slice(lane_block * LANES, (lane_block + 1) * LANES)


def column_of(line):
    return jnp.transpose(jnp.broadcast_to(line, (LANES, SIZE)))


def weigh(t, role, own, got, scale, left, right, wide):
    is_right = role[0] == 1
    q = role[1] - 1 + t
    own_wide = own[...].astype(f32)
    got_wide = got[...].astype(f32)
    wide[0] = jnp.where(is_right, got_wide, own_wide)
    wide[1] = jnp.where(is_right, own_wide, got_wide)
    left_rows = column_of(scale[0, q + 1])
    right_rows = column_of(scale[1, q + 1])
    for s in range(2):
        col = scale[2, q + s + 1]
        for jb in range(2):
            lines, lanes = lines_of(jb, s), lanes_of(jb)
            left[s, :, lanes] = (wide[0, lines, :] * left_rows).astype(bf16)
            right[s, :, lanes] = ((wide[1, lines, :] * right_rows) * col[:, lanes]).astype(bf16)


def sample(gates, kept, sketch, left, before, right, right_before, right_after, mixed, samp, gram):
    g0, g1, p0, p1, p2 = [gates[i] for i in range(5)]
    mixed[UPPER, UPPER] = (g0 * dot(left[0], right[0])).astype(bf16)
    mixed[UPPER, LOWER] = (p0 * dot(left[0], right[1]) + p2 * dot(left[1], right_after)).astype(bf16)
    mixed[LOWER, UPPER] = (
        p2 * dot(before[0], right_before) + p1 * dot(before[1], right[0])
    ).astype(bf16)
    mixed[LOWER, LOWER] = (g1 * dot(before[1], right[1])).astype(bf16)
    keep = lax.broadcasted_iota(jnp.int32, (1, SIZE), 1) < kept
    sampled = jnp.where(keep, dot(mixed[...], sketch), 0.0)
    high, low = split(sampled)
    samp[0] = high
    samp[1] = low
    shift = 0.01 * jnp.sum(sampled * sampled) / SIZE
    hh = lax.dot_general(high, high, CONTRACT_ROWS, preferred_element_type=f32)
    hl = lax.dot_general(high, low, CONTRACT_ROWS, preferred_element_type=f32)
    rows = lax.broadcasted_iota(jnp.int32, (SIZE, SIZE), 0)
    eye = rows == lax.broadcasted_iota(jnp.int32, (SIZE, SIZE), 1)
    added = jnp.where(keep, 0.0, 1.0) + shift
    gram[...] = (hh + (hl + jnp.transpose(hl))) + jnp.where(eye, added, 0.0)


def rolled(value, segments):
    shift = (segments * LEAF) % LANES
    return pltpu.roll(value, shift, axis=1) if shift else value


def gather_lanes(pieces):
    segment = lax.broadcasted_iota(jnp.int32, (1, LANES), 1) // LEAF
    out = pieces[0]
    for i in range(1, BATCH):
        out = jnp.where(segment == i, pieces[i], out)
    return out


def solve(gram, samp, scaled, a_ref, x_ref):
    for k in range(PANELS):
        rows = slice(k * LEAF, SIZE)
        lanes = lanes_of(k // 4)
        a_ref[k, rows, :] = gather_lanes(
            [rolled(gram[b][rows, lanes], b - k % 4) for b in range(BATCH)]
        )
        if k:
            a_ref[k, : k * LEAF, :] = jnp.zeros((k * LEAF, LANES), f32)

    invert_factor(a_ref, x_ref)

    def factor(b, offset):
        halves = []
        for g in range(2):
            panels = [
                rolled(x_ref[:, k * SIZE + offset : k * SIZE + offset + LANES], k % 4 - b)
                for k in range(4 * g, 4 * g + 4)
            ]
            halves.append(gather_lanes(panels))
        return jnp.concatenate(halves, axis=1)

    for b in range(BATCH):
        high, low = factor(b, 0), factor(b, LANES)
        solved = dot(samp[b][0], high) + (dot(samp[b][0], low) + dot(samp[b][1], high))
        scaled[b] = (solved * 16.0).astype(bf16)


def deliver(role, scaled, mixed, wide, ready, msg, out, sems, halved):
    is_right = role[0] == 1
    copies = []
    for b in range(BATCH):
        right_part = lax.dot_general(
            scaled[b], mixed[b][...], CONTRACT_ROWS, preferred_element_type=f32
        ) * (1.0 / SIZE)
        left_wide, right_wide = wide.at[2 * (b % 2)], wide.at[2 * (b % 2) + 1]
        for s in range(2):
            half = scaled[b, UPPER, :] if s == 0 else scaled[b + 1, LOWER, :]
            for jb in range(2):
                lines = lines_of(jb, s)
                left_wide[lines, :] = half[:, lanes_of(jb)].astype(f32)
                right_wide[lines, :] = right_part[:, lanes_of(2 * s + jb)]
        left_site = left_wide[...]
        right_site = right_wide[...]
        if not halved:
            target = msg[0].at[b] if b + 1 < BATCH else msg[1].at[0]
            target[...] = jnp.where(is_right, left_site, right_site).astype(bf16)
        elif b + 1 < BATCH:
            lines = slice(b * 4 * SIZE, (b + 1) * 4 * SIZE)
            msg[lines, :] = jnp.where(is_right, left_site, right_site).astype(bf16)
        else:
            for jb in range(2):
                lines = slice((12 + jb) * SIZE, (13 + jb) * SIZE)
                half = scaled[b, UPPER, lanes_of(jb)].astype(f32)
                msg[lines, :] = jnp.where(is_right, half, right_part[:, lanes_of(jb)]).astype(bf16)
        ready[b] = jnp.where(is_right, right_site, left_site).astype(bf16)
        copies.append(pltpu.make_async_copy(ready.at[b], out.at[role[1] + b], sems.at[b]))
        copies[-1].start()
    return copies


def windows(first, own, sketches, own_win, sketch, sems):
    count = own_win.shape[0]

    def own_copy(t):
        at = jnp.clip(first - 1 + t, 0, own.shape[0] - 1)
        return pltpu.make_async_copy(own.at[at], own_win.at[t], sems.at[t])

    sketch_copy = pltpu.make_async_copy(sketches.at[pl.ds(first, BATCH)], sketch, sems.at[count])
    return own_copy, sketch_copy


def early_kernel(role, gates, kept, own, got_0, got, scale, sketch, *refs):
    mixed, samp, gram, edge, left_w, right_w, wide = refs

    def step(t, loop):
        weigh(t, role, own.at[t], got.at[0], scale, left_w.at[t], right_w.at[t], wide)
        return loop

    def step_0(t, loop):
        weigh(t, role, own.at[t], got_0.at[t - 1], scale, left_w.at[t], right_w.at[t], wide)
        return loop

    lax.fori_loop(1, 4, step_0, 0)
    lax.fori_loop(4, 6, step, 0)
    for s in range(2):
        edge[s] = left_w[1, s]
        edge[2 + s] = right_w[1, s]
    edge[4] = right_w[2, 0]
    below = role[1] - 5
    wide[0] = got[0].astype(f32)
    rows = column_of(scale[1, below + 1])
    col = scale[2, below + 2]
    for jb in range(2):
        lanes = lanes_of(jb)
        edge[5, :, lanes] = ((wide[0, lines_of(jb, 1), :] * rows) * col[:, lanes]).astype(bf16)
    for b in range(1, BATCH):
        t = b + 1
        sample(
            gates,
            kept[role[1] + b],
            sketch[b],
            (left_w[t, 0], left_w[t, 1]),
            (left_w[t - 1, 0], left_w[t - 1, 1]),
            (right_w[t, 0], right_w[t, 1]),
            right_w[t - 1, 1],
            right_w[t + 1, 0],
            mixed.at[b - 1],
            samp.at[b - 1],
            gram.at[b - 1],
        )


def first_kernel(role, gates, kept, own, got, scale, sketch, *refs):
    (mixed_e, samp_e, gram_e, edge, msg, out, carry), refs = refs[:7], refs[7:]
    mixed, samp, gram, scaled, a_ref, x_ref, wide, ready, sems = refs
    left, right = carry.at[pl.ds(1, 2)], carry.at[pl.ds(3, 2)]
    weigh(0, role, own.at[0], got.at[0], scale, left, right, wide)
    sample(
        gates,
        kept[role[1]],
        sketch[0],
        (edge[0], edge[1]),
        (left[0], left[1]),
        (edge[2], edge[3]),
        right[1],
        edge[4],
        mixed,
        samp,
        gram,
    )
    mixed = [mixed] + [mixed_e.at[b] for b in range(BATCH - 1)]
    samp = [samp] + [samp_e.at[b] for b in range(BATCH - 1)]
    gram = [gram] + [gram_e.at[b] for b in range(BATCH - 1)]
    solve(gram, samp, scaled, a_ref, x_ref)
    scaled[BATCH, LOWER, :] = jnp.zeros((SIZE, SIZE), bf16)
    carry[0] = scaled[0, LOWER, :]
    for copy in deliver(role, scaled, mixed, wide, ready, msg, out, sems, True):
        copy.wait()


def second_kernel(role, gates, kept, own, got, scale, sketch, *refs):
    (edge, carry, _, msg, msg_last, out, merge), refs = refs[:7], refs[7:]
    left_w, right_w, mixed, samp, gram, scaled, a_ref, x_ref, wide = refs[:9]
    ready, sems = refs[9:]

    def step(t, loop):
        at = jnp.maximum(t - 1, 0)
        weigh(t, role, own.at[t], got.at[at], scale, left_w.at[t], right_w.at[t], wide)
        return loop

    lax.fori_loop(0, 4, step, 0)
    right_w[0, 1] = edge[5]
    for s in range(2):
        left_w[4, s] = carry[1 + s]
        right_w[4, s] = carry[3 + s]
    right_w[5, 0] = edge[2]
    for b in range(BATCH):
        t = b + 1
        sample(
            gates,
            kept[role[1] + b],
            sketch[b],
            (left_w[t, 0], left_w[t, 1]),
            (left_w[b, 0], left_w[b, 1]),
            (right_w[t, 0], right_w[t, 1]),
            right_w[b, 1],
            right_w[t + 1, 0],
            mixed.at[b],
            samp.at[b],
            gram.at[b],
        )
    every = range(BATCH)
    solve([gram.at[b] for b in every], [samp.at[b] for b in every], scaled, a_ref, x_ref)
    scaled[BATCH, LOWER, :] = carry[0]
    copies = deliver(
        role,
        scaled,
        [mixed.at[b] for b in every],
        wide,
        ready,
        (msg, msg_last),
        out,
        sems,
        False,
    )
    used = jnp.where(role[0] == 1, 0.0, 1.0)
    for jb in range(2):
        value = scaled[0, LOWER, lanes_of(jb)].astype(f32)
        wide[0, lines_of(jb, 0), :] = jnp.zeros((SIZE, LANES), f32)
        wide[0, lines_of(jb, 1), :] = value * used
    merge[...] = wide[0].astype(bf16)
    for copy in copies:
        copy.wait()


def in_hbm(x):
    return pltpu.with_memory_space_constraint(x, pltpu.HBM)


def shaped(*shape, dtype=bf16):
    return jax.ShapeDtypeStruct(shape, dtype)


def run(kernel, operands, specs, outs, out_specs, scratch, aliases=None, mib=20):
    return pl.pallas_call(
        kernel,
        out_shape=outs,
        in_specs=specs,
        out_specs=out_specs,
        scratch_shapes=scratch,
        input_output_aliases=aliases or {},
        compiler_params=pltpu.CompilerParams(vmem_limit_bytes=mib * 2**20),
        cost_estimate=pl.CostEstimate(
            flops=mib * 500_000_000, bytes_accessed=8_000_000, transcendentals=0
        ),
    )(*operands)


SMEM = pl.BlockSpec(memory_space=pltpu.SMEM)
VMEM = pl.BlockSpec(memory_space=pltpu.VMEM)
HBM = pl.BlockSpec(memory_space=pltpu.HBM)
SECTOR = (4 * SIZE, LANES)


def factor_scratch():
    return [
        pltpu.VMEM((BATCH + 1, 2 * SIZE, SIZE), bf16),
        pltpu.VMEM((PANELS, SIZE, LANES), f32),
        pltpu.VMEM((SIZE, PANELS * SIZE), bf16),
        pltpu.VMEM((4, *SECTOR), f32),
    ]


def sample_shapes(make, *lead):
    return [
        make((*lead, 2 * SIZE, 2 * SIZE), bf16),
        make((*lead, 2, 2 * SIZE, SIZE), bf16),
        make((*lead, SIZE, SIZE), f32),
    ]


def early(role, gates, kept, own, got_0, got, scale, sketch):
    return run(
        early_kernel,
        (role, gates, kept, own, got_0, got, scale, sketch),
        [SMEM] * 3 + [VMEM] * 5,
        sample_shapes(jax.ShapeDtypeStruct, BATCH - 1) + [shaped(6, SIZE, SIZE)],
        [VMEM] * 4,
        [
            pltpu.VMEM((6, 2, SIZE, SIZE), bf16),
            pltpu.VMEM((6, 2, SIZE, SIZE), bf16),
            pltpu.VMEM((2, *SECTOR), f32),
        ],
    )


def first_half(role, gates, kept, own, got, scale, sketch, parts):
    return run(
        first_kernel,
        (role, gates, kept, own, got, scale, sketch, *parts),
        [SMEM] * 3 + [VMEM] * 8,
        [shaped(14 * SIZE, LANES), pltpu.HBM((16, *SECTOR), bf16), shaped(5, SIZE, SIZE)],
        [VMEM, HBM, VMEM],
        sample_shapes(pltpu.VMEM)
        + factor_scratch()
        + [pltpu.VMEM((BATCH, *SECTOR), bf16), pltpu.SemaphoreType.DMA((BATCH,))],
    )


def second_half(role, gates, kept, own, got, scale, sketch, edge, carry, out):
    return run(
        second_kernel,
        (role, gates, kept, own, got, scale, sketch, edge, carry, out),
        [SMEM] * 3 + [VMEM] * 6 + [HBM],
        [
            shaped(BATCH - 1, *SECTOR),
            shaped(1, *SECTOR),
            pltpu.HBM((16, *SECTOR), bf16),
            shaped(*SECTOR),
        ],
        [VMEM, VMEM, HBM, VMEM],
        [pltpu.VMEM((6, 2, SIZE, SIZE), bf16), pltpu.VMEM((6, 2, SIZE, SIZE), bf16)]
        + sample_shapes(pltpu.VMEM, BATCH)
        + factor_scratch()
        + [
            pltpu.VMEM((BATCH, *SECTOR), bf16),
            pltpu.SemaphoreType.DMA((BATCH,)),
        ],
        aliases={9: 2},
    )


def fetch_kernel(at, own, out, sem):
    copy = pltpu.make_async_copy(own.at[pl.ds(at[0], out.shape[0])], out, sem)
    copy.start()
    copy.wait()


def fetch(at, own):
    return run(
        fetch_kernel,
        (jnp.reshape(at, (1,)), in_hbm(own)),
        [SMEM, HBM],
        [shaped(3, *SECTOR)],
        [VMEM],
        [pltpu.SemaphoreType.DMA],
        mib=1,
    )[0]


def pack_kernel(role, own, sketches, out, low, rest, *refs):
    own_a, sketch_a, own_b, sketch_b, both, sems, sems_a, sems_b = refs
    flag = role[0]
    copies = [
        pltpu.make_async_copy(own.at[7 + 8 * flag], both.at[0], sems.at[0]),
        pltpu.make_async_copy(own.at[7], both.at[1], sems.at[1]),
        pltpu.make_async_copy(own.at[3 + 8 * flag], low.at[0], sems.at[2]),
        pltpu.make_async_copy(own.at[pl.ds(8 * flag, 3)], rest, sems.at[3]),
    ]
    first = 12 - 8 * flag
    for start, own_win, sketch, win_sems in (
        (first, own_a, sketch_a, sems_a),
        (first - BATCH, own_b, sketch_b, sems_b),
    ):
        own_copy, sketch_copy = windows(start, own, sketches, own_win, sketch, win_sems)
        copies += [own_copy(t) for t in range(own_win.shape[0])] + [sketch_copy]
    for copy in copies:
        copy.start()
    copies[0].wait()
    copies[1].wait()
    is_odd = lax.broadcasted_iota(jnp.int32, SECTOR, 0) % 2 == 1
    out[0] = jnp.where(is_odd, both[1].astype(f32), both[0].astype(f32)).astype(bf16)
    for copy in copies[2:]:
        copy.wait()


def pack(role, own, sketches):
    sketch = shaped(BATCH, 2 * SIZE, SIZE)
    return run(
        pack_kernel,
        (role, in_hbm(own), in_hbm(sketches)),
        [SMEM, HBM, HBM],
        [shaped(count, *SECTOR) for count in (1, 1, 3)]
        + [shaped(6, *SECTOR), sketch, shaped(4, *SECTOR), sketch],
        [VMEM] * 7,
        [
            pltpu.VMEM((2, *SECTOR), bf16),
            pltpu.SemaphoreType.DMA((4,)),
            pltpu.SemaphoreType.DMA((7,)),
            pltpu.SemaphoreType.DMA((5,)),
        ],
        mib=2,
    )


def place_kernel(at, block, _, out, sems):
    copies = []
    for b in range(block.shape[0]):
        copies.append(pltpu.make_async_copy(block.at[b], out.at[at[0] + b], sems.at[b]))
        copies[-1].start()
    for copy in copies:
        copy.wait()


def place_halved_kernel(at, block, merge, _, out, last, wide, sems):
    copies = []
    for b in range(3):
        lines = pl.ds(b * 4 * SIZE, 4 * SIZE)
        copies.append(pltpu.make_async_copy(block.at[lines], out.at[at[0] + b], sems.at[b]))
        copies[-1].start()
    for jb in range(2):
        half = block[(12 + jb) * SIZE : (13 + jb) * SIZE, :]
        wide[lines_of(jb, 0), :] = half.astype(f32)
        wide[lines_of(jb, 1), :] = jnp.zeros((SIZE, LANES), f32)
    last[...] = (wide[...] + merge[...].astype(f32)).astype(bf16)
    copies.append(pltpu.make_async_copy(last, out.at[at[0] + 3], sems.at[3]))
    copies[-1].start()
    for copy in copies:
        copy.wait()


def place(out, block, at, merge=None):
    operands = (jnp.reshape(at, (1,)), block) + (() if merge is None else (merge,)) + (out,)
    scratch = [pltpu.VMEM(SECTOR, bf16), pltpu.VMEM(SECTOR, f32)] if merge is not None else []
    return run(
        place_kernel if merge is None else place_halved_kernel,
        operands,
        [SMEM] + [VMEM] * (len(operands) - 2) + [HBM],
        [pltpu.HBM(out.shape, out.dtype)],
        [HBM],
        scratch + [pltpu.SemaphoreType.DMA((4,))],
        aliases={len(operands) - 1: 0},
        mib=4,
    )[0]


def to_lines(x):
    n = x.shape[0]
    return x.reshape(n, SIZE, 2, 2, LANES).transpose(0, 1, 3, 2, 4).reshape(n, 4 * SIZE, LANES)


def from_lines(x):
    n = x.shape[0]
    return x.reshape(n, SIZE, 2, 2, LANES).transpose(0, 1, 3, 2, 4).reshape(n, SIZE, 2, SIZE)


def shards(site_tensors, bond_weights, sector_sizes, kept_ranks, sketches, gate_ends, gate_pair):
    chain = lax.axis_size("chain")
    count = lax.axis_size("group") * chain
    site = lax.axis_index("group") * chain + lax.axis_index("chain")
    is_right = site % 2 == 1

    def swapped(value):
        return lax.ppermute(value, "chain", [(i, i ^ 1) for i in range(chain)])

    def onward(value):
        def place(n):
            return n % chain * (count // chain) + n // chain

        pairs = [(place(i), place(i + 1)) for i in range(1, count - 1, 2)]
        return lax.ppermute(value, ("chain", "group"), pairs)

    own = to_lines(site_tensors[0, 0])
    sectors = own.shape[0]
    flag = is_right.astype(jnp.int32)

    got_0 = swapped(fetch(4 + 8 * flag, own))
    column = lax.broadcasted_iota(jnp.int32, (sectors, SIZE), 1)
    lam = bond_weights[0, 0] * (column < sector_sizes[0, 0][:, None]).astype(f32)
    before = onward(lam)
    before = jnp.where(site < 2, jnp.ones_like(lam), before)
    kept_line = jnp.pad(kept_ranks[0, 0].astype(f32)[None, :], ((0, 7), (0, SIZE - sectors)))
    packed = jnp.concatenate([lam, before, kept_line], axis=0)
    other = swapped(packed)
    outgoing, outgoing_low, outgoing_b, own_a, sketch_a, own_b, sketch_b = pack(
        jnp.reshape(flag, (1,)), own, sketches
    )
    got_a = swapped(outgoing)
    got_low = swapped(outgoing_low)
    lam_prev = jnp.where(is_right, other[sectors : 2 * sectors], before)
    lam_mid = jnp.where(is_right, other[:sectors], lam)
    lam_next = jnp.where(is_right, lam, other[:sectors])
    scale = jnp.pad(jnp.stack([lam_prev, lam_mid, lam_next]), ((0, 0), (1, 7), (0, 0)))
    scale = scale[:, :, None, :]
    kept = jnp.where(is_right, other[2 * sectors, :sectors], packed[2 * sectors, :sectors])
    kept = kept.astype(jnp.int32)
    got_b = swapped(outgoing_b)
    gates = jnp.concatenate([gate_ends, 1.0 + gate_pair[:2], gate_pair[2:]])
    first_a = 12 - 8 * flag
    first_b = 8 - 8 * flag
    role_a = jnp.stack([flag, first_a])
    role_b = jnp.stack([flag, first_b])

    parts = early(role_a, gates, kept, own_a, got_0, got_a, scale, sketch_a)
    msg_a, out, carry = first_half(role_a, gates, kept, own_a, got_low, scale, sketch_a, parts)
    back_a = swapped(msg_a)
    msg_b, msg_last, out, merge = second_half(
        role_b, gates, kept, own_b, got_b, scale, sketch_b, parts[3], carry, out
    )
    back_b = swapped(msg_b)
    back_last = swapped(msg_last)

    back_at = 8 * flag
    out = place(out, back_a, back_at + 4, merge)
    out = place(out, back_b, back_at)
    out = place(out, back_last, back_at + BATCH - 1)
    return from_lines(out)[None, None]


def solution(mesh):
    return jax.shard_map(
        shards,
        mesh=mesh,
        in_specs=(
            P("group", "chain", None, None, None, None),
            P("group", "chain", None, None),
            P("group", "chain", None),
            P("group", "chain", None),
            P(),
            P(),
            P(),
        ),
        out_specs=P("group", "chain", None, None, None, None),
        check_vma=False,
    )
```
